64 devices in a mesh: tp: 4 (over x, y), cp: 16 (over z, core).
Axes of the slice: x: 2, y: 2, z: 8, core: 2. Of those that a mesh axis runs over, the one named last changes fastest.
The devices are a block of a 4x4x8 slice.
Arguments:
- query: bfloat16 [16, 512, 32, 128], P(None, 'cp', 'tp'), parts along dimension 2
- out_act: bfloat16 [16, 512, 32, 128], P(None, 'cp', 'tp'), parts along dimension 2
- out_grad: bfloat16 [16, 512, 32, 128], P(None, 'cp', 'tp'), parts along dimension 2
- row_lse: float32 [16, 512, 32], P(None, 'cp', 'tp'), parts along dimension 2
- key_act: bfloat16 [10240, 8, 128], P('cp', 'tp'), parts along dimension 1
- value_act: bfloat16 [10240, 8, 128], P('cp', 'tp'), parts along dimension 1
- doc_ids: int32 [10240], replicated
Outputs:
- output 1: bfloat16 [16, 512, 32, 128], P(None, 'cp', 'tp'), parts along dimension 2
- output 2: float32 [10240, 8, 128], P('cp', 'tp'), parts along dimension 1
- output 3: float32 [10240, 8, 128], P('cp', 'tp'), parts along dimension 1
There are 4 independent parts. The reference program is written for one: setup_inputs(seed, part) draws one part's arguments, and reference() takes and returns one part's arrays. A program takes and returns all parts, laid end to end along the dimension named above; an argument that names none is the same for every part.
All inputs are finite; a program needn't handle non-finite values.
Results may differ from the reference program's by a relative error of at most 0.00747609.
Values are sent between devices in bfloat16 or wider.
A program may use at most 768 MiB of HBM per device.

```python
import jax
import jax.numpy as jnp
from jax import lax

SLICES = 16
SUB_LEN = 512
PRE_LEN = 2048
Q_HEADS = 8
KV_HEADS = 2
HEAD_DIM = 128
SPLITS = 16

PREFIX = PRE_LEN + SLICES * SUB_LEN
GROUP_SIZE = Q_HEADS // KV_HEADS
BLOCK_LEN = SUB_LEN // SPLITS
SCORE_SCALE = HEAD_DIM ** -0.5
GRAD_SCALE = (PREFIX // 8) ** 0.5
DOC_MEAN = PREFIX // 8


def masked_scores(q_blk, key_act, doc_ids, first_pos):
    block_len = q_blk.shape[0]
    scores = jnp.einsum('qhgd,khd->qhgk', q_blk.astype(jnp.float32), key_act.astype(jnp.float32)) * SCORE_SCALE
    q_pos = first_pos + jnp.arange(block_len)
    k_pos = jnp.arange(key_act.shape[0])
    q_doc = lax.dynamic_slice(doc_ids, (first_pos,), (block_len,))
    allowed = (k_pos[None, :] <= q_pos[:, None]) & (doc_ids[None, :] == q_doc[:, None])
    return scores, allowed[:, None, None, :]


def forward_lse(query, key_act, doc_ids):
    n_blocks = SLICES * SPLITS
    q_blocks = query.reshape(n_blocks, BLOCK_LEN, KV_HEADS, GROUP_SIZE, HEAD_DIM)
    firsts = PRE_LEN + jnp.arange(n_blocks) * BLOCK_LEN

    def block_lse(xs_blk):
        q_blk, first_pos = xs_blk
        scores, allowed = masked_scores(q_blk, key_act, doc_ids, first_pos)
        return jax.nn.logsumexp(jnp.where(allowed, scores, -1e30), axis=-1)

    return lax.map(block_lse, (q_blocks, firsts)).reshape(SLICES, SUB_LEN, Q_HEADS)


def setup_inputs(seed: int = 0, part: int = 0) -> dict:
    root_key = jax.random.key(seed)
    part_keys = jax.random.split(jax.random.fold_in(root_key, part), 5)
    doc_key = jax.random.key(seed + 17)
    starts = (jax.random.randint(doc_key, (PREFIX,), 0, DOC_MEAN) == 0) & (jnp.arange(PREFIX) > 0)
    doc_ids = jnp.cumsum(starts.astype(jnp.int32)).astype(jnp.int32)
    q_shape = (SLICES, SUB_LEN, Q_HEADS, HEAD_DIM)
    query = jax.random.normal(part_keys[0], q_shape, jnp.float32).astype(jnp.bfloat16)
    key_act = jax.random.normal(part_keys[1], (PREFIX, KV_HEADS, HEAD_DIM), jnp.float32).astype(jnp.bfloat16)
    value_act = jax.random.normal(part_keys[2], (PREFIX, KV_HEADS, HEAD_DIM), jnp.float32).astype(jnp.bfloat16)
    grad_dir = jax.random.normal(part_keys[3], q_shape, jnp.float32)
    out_noise = jax.random.normal(part_keys[4], q_shape, jnp.float32)
    out_grad = (GRAD_SCALE * grad_dir).astype(jnp.bfloat16)
    out_act = (0.125 * (grad_dir + out_noise)).astype(jnp.bfloat16)
    row_lse = forward_lse(query, key_act, doc_ids)
    return {'query': query, 'out_act': out_act, 'out_grad': out_grad, 'row_lse': row_lse, 'key_act': key_act, 'value_act': value_act, 'doc_ids': doc_ids}


def reference(query, out_act, out_grad, row_lse, key_act, value_act, doc_ids):
    n_blocks = SLICES * SPLITS
    blk_shape = (n_blocks, BLOCK_LEN, KV_HEADS, GROUP_SIZE, HEAD_DIM)
    key_f32 = key_act.astype(jnp.float32)
    value_f32 = value_act.astype(jnp.float32)
    xs_all = (query.reshape(blk_shape), out_act.reshape(blk_shape), out_grad.reshape(blk_shape), row_lse.reshape(n_blocks, BLOCK_LEN, KV_HEADS, GROUP_SIZE), PRE_LEN + jnp.arange(n_blocks) * BLOCK_LEN)

    def block_step(carry_in, xs_blk):
        dk_acc, dv_acc = carry_in
        q_blk, o_blk, do_blk, lse_blk, first_pos = xs_blk
        scores, allowed = masked_scores(q_blk, key_act, doc_ids, first_pos)
        p_full = jnp.where(allowed, jnp.exp(scores - lse_blk[..., None]), 0.0)
        p_half = p_full.astype(jnp.bfloat16).astype(jnp.float32)
        grad_f32 = do_blk.astype(jnp.float32)
        row_delta = jnp.sum(grad_f32 * o_blk.astype(jnp.float32), axis=-1)
        dv_acc = dv_acc + jnp.einsum('qhgk,qhgd->khd', p_half, grad_f32)
        d_prob = jnp.einsum('qhgd,khd->qhgk', grad_f32, value_f32)
        d_score = (p_full * (d_prob - row_delta[..., None])).astype(jnp.bfloat16).astype(jnp.float32)
        dq_blk = (jnp.einsum('qhgk,khd->qhgd', d_score, key_f32) * SCORE_SCALE).astype(jnp.bfloat16)
        dk_acc = dk_acc + jnp.einsum('qhgk,qhgd->khd', d_score, q_blk.astype(jnp.float32)) * SCORE_SCALE
        return (dk_acc, dv_acc), dq_blk

    zero_acc = jnp.zeros((PREFIX, KV_HEADS, HEAD_DIM), jnp.float32)
    (d_key, d_value), dq_blocks = lax.scan(block_step, (zero_acc, zero_acc), xs_all)
    return dq_blocks.reshape(SLICES, SUB_LEN, Q_HEADS, HEAD_DIM), d_key, d_value
```

```python
import functools
import math

import jax
import jax.numpy as jnp
from jax import lax
from jax.experimental import pallas as pl
from jax.experimental.pallas import tpu as pltpu
from jax.sharding import PartitionSpec as P

MESH = pl.DeviceIdType.MESH
CORES = 2
F32 = jnp.float32
BF16 = jnp.bfloat16


def ring_kernel(cp_size, sub_start, local_len, scale, kv_in, q_in, qt_in, do_in, dot_in, st_in, dq_out, dkv_out,
                kvb, acc, rsb, qn, qt, don, dot, st, dqa, dqr, dqo,
                ag_send, ag_recv, rs_send, rs_recv, x_send, x_recv, loc_sem, out_sem):
    n_chip = cp_size // CORES
    n_hop = n_chip - 1
    n_kv, n_sub, rows = q_in.shape[0], q_in.shape[1], q_in.shape[2]
    key_tile = kv_in.shape[2]
    head_dim = kv_in.shape[3] // 2
    span = local_len * CORES
    sub_len = local_len * cp_size
    keys_local = 2 * key_tile
    own = 2 * n_hop

    me = lax.axis_index('cp')
    chip, core = me // CORES, lax.rem(me, CORES)
    right = lax.rem(me + CORES, cp_size)
    left = lax.rem(me + cp_size - CORES, cp_size)
    sibling = me + 1 - 2 * core
    nbr = (right, left)

    barrier = pltpu.get_barrier_semaphore()
    for peer in (right, left, sibling):
        pl.semaphore_signal(barrier, inc=1, device_id={'cp': peer}, device_id_type=MESH)
    pl.semaphore_wait(barrier, 3)

    def remote(src, dst, send, recv, peer):
        return pltpu.make_async_remote_copy(src_ref=src, dst_ref=dst, send_sem=send, recv_sem=recv,
                                            device_id={'cp': peer}, device_id_type=MESH)

    def half_of(way, k):
        return (k + way) % 2

    def gather(way, j):
        src = kv_in.at[half_of(way, j)] if j < 2 else kvb.at[way * n_hop + j - 2]
        i = way * n_hop + j
        return remote(src, kvb.at[i], ag_send.at[i], ag_recv.at[i], nbr[way])

    def reduce_copy(way, k):
        i = way * n_hop + k
        return remote(acc.at[i], rsb.at[i], rs_send.at[i], rs_recv.at[i], nbr[1 - way])

    pairs = ((q_in, qn), (qt_in, qt), (do_in, don), (dot_in, dot), (st_in, st))

    def part_of(ref, which):
        cut = pl.ds(which * rows, rows)
        return ref.at[:, :, cut, :] if ref.shape[2] == CORES * rows and ref.shape[3] == head_dim else ref.at[:, :, :, cut]

    share = [remote(a, part_of(b, 1), x_send.at[i], x_recv.at[i], sibling) for i, (a, b) in enumerate(pairs)]
    local = [pltpu.make_async_copy(a, part_of(b, 0), loc_sem.at[i]) for i, (a, b) in enumerate(pairs)]
    local.append(pltpu.make_async_copy(kv_in, kvb.at[pl.ds(own, 2)], loc_sem.at[len(pairs)]))
    for j in range(2):
        for way in range(2):
            gather(way, j).start()
    for c in share + local:
        c.start()

    @pl.loop(0, n_kv * n_sub)
    def _(i):
        dqa[i // n_sub, lax.rem(i, n_sub)] = jnp.zeros(dqa.shape[2:], F32)

    for c in local:
        c.wait()
    for c in share:
        c.wait()

    exp_scale = scale * math.log2(math.e)
    k_iota = lax.broadcasted_iota(jnp.int32, (key_tile, CORES * rows), 0).astype(F32)

    def chunk(slot, key_chip, half, head):
        pos0 = (key_chip * CORES + core) * keys_local + half * key_tile
        t = pos0 - sub_start - span * chip - span + sub_len
        s_lo = jnp.minimum(jnp.maximum(t, 0) // sub_len, n_sub)
        pos_f = pos0.astype(F32)
        k = kvb[slot, head, :, :head_dim]
        v = kvb[slot, head, :, head_dim:]
        acc[slot, head] = jnp.zeros(acc.shape[2:], F32)

        @pl.loop(s_lo, n_sub)
        def _(s):
            lse, delta = st[head, s, 0:1, :], st[head, s, 1:2, :]
            lo, hi = st[head, s, 2:3, :] - pos_f, st[head, s, 3:4, :] - pos_f
            s_t = jnp.dot(k, qt[head, s], preferred_element_type=F32)
            dp_t = jnp.dot(v, dot[head, s], preferred_element_type=F32)
            ok = (k_iota >= lo) & (k_iota <= hi)
            p = jnp.where(ok, jnp.exp2(s_t * exp_scale - lse), 0.0)
            ds = (p * (dp_t - delta)).astype(BF16)
            acc[slot, head, :, head_dim:] += jnp.dot(p.astype(BF16), don[head, s], preferred_element_type=F32)
            acc[slot, head, :, :head_dim] += jnp.dot(ds, qn[head, s], preferred_element_type=F32)
            dqa[head, s] += lax.dot_general(ds, k, (((0,), (0,)), ((), ())), preferred_element_type=F32)

    def unit(way, k):
        if way is None:
            slot, key_chip, half = own + k, chip, k
        else:
            hop = k // 2 + 1
            slot, half = way * n_hop + k, half_of(way, k)
            key_chip = lax.rem(chip + (hop if way else n_chip - hop), n_chip)
        for head in range(n_kv):
            chunk(slot, key_chip, half, head)

    def event(k):
        for way in range(2):
            gather(way, k).wait_recv()
            if k + 2 < n_hop:
                gather(way, k + 2).start()

    def add(dst, src):
        steps = n_kv * 4
        cut = key_tile // 4

        @pl.loop(0, steps)
        def _(i):
            h, r = i // 4, pl.ds(pl.multiple_of(lax.rem(i, 4) * cut, 8), cut)
            acc[dst, h, r, :] += rsb[src, h, r, :]

    units = [(None, 0), (None, 1)] + [(way, k) for k in range(n_hop) for way in range(2)]
    done = units[:n_hop]
    for k in range(n_hop):
        unit(*done[k])
        event(k)
    for k in reversed(range(n_hop)):
        for way in range(2):
            if (way, k) not in done:
                unit(way, k)
            if k + 2 < n_hop:
                reduce_copy(way, k + 2).wait_recv()
                add(way * n_hop + k, way * n_hop + k + 2)
            reduce_copy(way, k).start()
    for u in ((None, 0), (None, 1)):
        if u not in done:
            unit(*u)
    swap = remote(part_of(dqa, 1), dqr, x_send.at[len(pairs)], x_recv.at[len(pairs)], sibling)
    swap.start()
    swap.wait_recv()

    @pl.loop(0, n_kv * n_sub)
    def _(i):
        h, s = i // n_sub, lax.rem(i, n_sub)
        dqo[h, s] = ((dqa[h, s, :rows, :] + dqr[h, s]) * scale).astype(BF16)

    put_dq = pltpu.make_async_copy(dqo, dq_out, out_sem.at[0])
    put_dq.start()
    for k in reversed(range(min(2, n_hop))):
        for way in range(2):
            reduce_copy(way, k).wait_recv()
            add(own + half_of(way, k), way * n_hop + k)

    @pl.loop(0, 2 * n_kv)
    def _(i):
        half, h = i // n_kv, lax.rem(i, n_kv)
        acc[own + half, h, :, :head_dim] = acc[own + half, h, :, :head_dim] * scale

    put_kv = pltpu.make_async_copy(acc.at[pl.ds(own, 2)], dkv_out, out_sem.at[1])
    put_kv.start()
    swap.wait_send()
    for way in range(2):
        for j in range(n_hop):
            gather(way, j).wait_send()
            reduce_copy(way, j).wait_send()
    put_dq.wait()
    put_kv.wait()


def solution(mesh):
    cp_size = mesh.shape['cp']
    q_spec = P(None, 'cp', 'tp', None)
    lse_spec = P(None, 'cp', 'tp')
    kv_spec = P('cp', 'tp', None)

    def local_backward(query, out_act, out_grad, row_lse, key_act, value_act, doc_ids):
        n_sub, local_len, n_heads, head_dim = query.shape
        keys_local, n_kv = key_act.shape[0], key_act.shape[1]
        group = n_heads // n_kv
        sub_len = local_len * cp_size
        sub_start = keys_local * cp_size - n_sub * sub_len
        scale = head_dim ** -0.5
        rows = local_len * group
        half = keys_local // 2
        n_hop = cp_size // CORES - 1
        n_slot = 2 * n_hop + 2
        me = lax.axis_index('cp')

        def by_head(x):
            x = x.reshape((n_sub, local_len, n_kv, group) + x.shape[3:])
            x = jnp.moveaxis(x, 2, 0)
            return x.reshape((n_kv, n_sub, rows) + x.shape[4:])

        delta = jnp.einsum('sqhd,sqhd->sqh', out_grad, out_act, preferred_element_type=F32)
        q_doc = lax.dynamic_slice_in_dim(doc_ids[sub_start:].reshape(n_sub, sub_len), me * local_len, local_len, axis=1)
        q_first = jnp.sum((doc_ids[None, None, :] < q_doc[:, :, None]).astype(F32), axis=-1)
        q_pos = (sub_start + me * local_len + jnp.arange(n_sub)[:, None] * sub_len + jnp.arange(local_len)[None, :]).astype(F32)
        wide = lambda x: jnp.broadcast_to(jnp.repeat(x, group, axis=1)[None], (n_kv, n_sub, rows))
        lines = [by_head(row_lse) * math.log2(math.e), by_head(delta), wide(q_first), wide(q_pos)]
        stats = jnp.stack(lines + [jnp.zeros_like(lines[0])] * 4, axis=2)
        qn, don = by_head(query), by_head(out_grad)
        cut = lambda x: jnp.transpose(x.reshape(2, half, n_kv, head_dim), (0, 2, 1, 3))
        kv = jnp.concatenate([cut(key_act), cut(value_act)], axis=-1)
        flops = 2 * 5 * n_kv * n_sub * 2 * rows * head_dim * keys_local * n_hop
        hbm = pl.BlockSpec(memory_space=pl.ANY)
        dma = pltpu.SemaphoreType.DMA
        dq, dkv = pl.pallas_call(
            functools.partial(ring_kernel, cp_size, sub_start, local_len, scale),
            name='ring_backward',
            out_shape=(jax.ShapeDtypeStruct((n_kv, n_sub, rows, head_dim), BF16),
                       jax.ShapeDtypeStruct((2, n_kv, half, 2 * head_dim), F32)),
            in_specs=[hbm] * 6,
            out_specs=(hbm, hbm),
            scratch_shapes=[
                pltpu.VMEM((n_slot, n_kv, half, 2 * head_dim), BF16),
                pltpu.VMEM((n_slot, n_kv, half, 2 * head_dim), F32),
                pltpu.VMEM((2 * n_hop, n_kv, half, 2 * head_dim), F32),
                pltpu.VMEM((n_kv, n_sub, CORES * rows, head_dim), BF16),
                pltpu.VMEM((n_kv, n_sub, head_dim, CORES * rows), BF16),
                pltpu.VMEM((n_kv, n_sub, CORES * rows, head_dim), BF16),
                pltpu.VMEM((n_kv, n_sub, head_dim, CORES * rows), BF16),
                pltpu.VMEM((n_kv, n_sub, 8, CORES * rows), F32),
                pltpu.VMEM((n_kv, n_sub, CORES * rows, head_dim), F32),
                pltpu.VMEM((n_kv, n_sub, rows, head_dim), F32),
                pltpu.VMEM((n_kv, n_sub, rows, head_dim), BF16),
                dma((2 * n_hop,)), dma((2 * n_hop,)), dma((2 * n_hop,)), dma((2 * n_hop,)),
                dma((6,)), dma((6,)), dma((6,)), dma((2,)),
            ],
            compiler_params=pltpu.CompilerParams(collective_id=0, has_side_effects=True, vmem_limit_bytes=62 * 1024 * 1024),
            cost_estimate=pl.CostEstimate(flops=flops, bytes_accessed=30 * 2 ** 20, transcendentals=0),
        )(kv, qn, jnp.swapaxes(qn, 2, 3), don, jnp.swapaxes(don, 2, 3), stats)
        dq = jnp.moveaxis(dq.reshape(n_kv, n_sub, local_len, group, head_dim), 0, 2).reshape(query.shape)
        dkv = jnp.transpose(dkv, (0, 2, 1, 3)).reshape(keys_local, n_kv, 2 * head_dim)
        return dq, dkv[..., :head_dim], dkv[..., head_dim:]

    return jax.shard_map(local_backward, mesh=mesh, in_specs=(q_spec, q_spec, q_spec, lse_spec, kv_spec, kv_spec, P()),
                         out_specs=(q_spec, kv_spec, kv_spec), check_vma=False)
```

```python
import functools
import math

import jax
import jax.numpy as jnp
from jax import lax
from jax.experimental import pallas as pl
from jax.experimental.pallas import tpu as pltpu
from jax.sharding import PartitionSpec as P

MESH = pl.DeviceIdType.MESH
CORES = 2
F32 = jnp.float32
BF16 = jnp.bfloat16
RUNS = 2
EARLY_ITEMS = 88


def ring_kernel(cp_size, sub_start, local_len, scale, early_items, kv_in, q_in, qt_in, do_in, dot_in, st_in, dq_out, dkv_out,
                kvb, acc, rsb, qn, qt, don, dot, st, dqa, dqr, dqo, pbuf, dsbuf,
                ag_send, ag_recv, rs_send, rs_recv, x_send, x_recv, loc_sem, out_sem):
    n_chip = cp_size // CORES
    n_hop = n_chip - 1
    n_kv, n_sub, rows = q_in.shape[0], q_in.shape[1], q_in.shape[2]
    key_tile = kv_in.shape[2]
    head_dim = kv_in.shape[3] // 2
    span = local_len * CORES
    sub_len = local_len * cp_size
    keys_local = 2 * key_tile
    own = 2 * n_hop
    width = CORES * rows

    me = lax.axis_index('cp')
    chip, core = me // CORES, lax.rem(me, CORES)
    right = lax.rem(me + CORES, cp_size)
    left = lax.rem(me + cp_size - CORES, cp_size)
    sibling = me + 1 - 2 * core
    nbr = (right, left)

    barrier = pltpu.get_barrier_semaphore()
    for peer in (right, left, sibling):
        pl.semaphore_signal(barrier, inc=1, device_id={'cp': peer}, device_id_type=MESH)
    pl.semaphore_wait(barrier, 3)

    def remote(src, dst, send, recv, peer):
        return pltpu.make_async_remote_copy(src_ref=src, dst_ref=dst, send_sem=send, recv_sem=recv,
                                            device_id={'cp': peer}, device_id_type=MESH)

    def half_of(way, k):
        return (k + way) % 2

    def gather(way, j):
        src = kv_in.at[half_of(way, j)] if j < 2 else kvb.at[way * n_hop + j - 2]
        i = way * n_hop + j
        return remote(src, kvb.at[i], ag_send.at[i], ag_recv.at[i], nbr[way])

    def reduce_copy(way, k):
        i = way * n_hop + k
        return remote(acc.at[i], rsb.at[i], rs_send.at[i], rs_recv.at[i], nbr[1 - way])

    pairs = ((q_in, qn), (qt_in, qt), (do_in, don), (dot_in, dot), (st_in, st))

    def part_of(ref, which):
        cut = pl.ds(which * rows, rows)
        return ref.at[:, :, cut, :] if ref is qn or ref is don else ref.at[:, :, :, cut]

    share = [remote(a, part_of(b, 1), x_send.at[i], x_recv.at[i], sibling) for i, (a, b) in enumerate(pairs)]
    local = [pltpu.make_async_copy(a, part_of(b, 0), loc_sem.at[i]) for i, (a, b) in enumerate(pairs)]
    local.append(pltpu.make_async_copy(kv_in, kvb.at[pl.ds(own, 2)], loc_sem.at[len(pairs)]))
    for j in range(2):
        for way in range(2):
            gather(way, j).start()
    for c in share + local:
        c.start()

    @pl.loop(0, n_kv * n_sub)
    def _(i):
        dqa[i // n_sub, lax.rem(i, n_sub)] = jnp.zeros(dqa.shape[2:], F32)

    @pl.loop(0, acc.shape[0] * n_kv)
    def _(i):
        acc[i // n_kv, lax.rem(i, n_kv)] = jnp.zeros(acc.shape[2:], F32)

    pbuf[...] = jnp.zeros(pbuf.shape, BF16)
    dsbuf[...] = jnp.zeros(dsbuf.shape, BF16)

    n_run = n_sub // RUNS
    n_early = 2 + min(8, 2 * n_hop)
    n_entry = n_early + 2 * n_hop

    def place(e):
        early = e < n_early
        f = jnp.where(early, e - 2, e - n_early)
        k = jnp.where(early, f // 2, n_hop - 1 - f // 2)
        way = f % 2
        mine = e < 2
        slot = jnp.where(mine, own + e, way * n_hop + k)
        half = jnp.where(mine, e, (k + way) % 2)
        hop = k // 2 + 1
        key_chip = jnp.where(mine, chip, lax.rem(chip + jnp.where(way == 1, hop, n_chip - hop), n_chip))
        pos0 = (key_chip * CORES + core) * keys_local + half * key_tile
        s_lo = jnp.minimum(jnp.maximum(pos0 - sub_start - span * chip - span + sub_len, 0) // sub_len, n_sub - 1)
        return slot, pos0, s_lo // RUNS

    counts, ends, taken = [], [], []
    total = jnp.int32(0)
    for e in range(n_entry):
        n = n_kv * (n_run - place(jnp.int32(e))[2])
        if e < n_early:
            fits = jnp.int32(1) if e < 2 else (total + n <= early_items).astype(jnp.int32)
            if len(taken) > 2:
                fits = fits * taken[-1]
            taken.append(fits)
            n = n * fits
        else:
            f = e - n_early
            i_early = 2 + 2 * (n_hop - 1 - f // 2) + f % 2
            if i_early < n_early:
                n = n * (1 - taken[i_early])
        total = total + n
        counts.append(n)
        ends.append(total)

    def item(i):
        i = jnp.minimum(i, total - 1)
        e, first = jnp.int32(0), jnp.int32(0)
        for n, end in zip(counts, ends):
            past = (i >= end).astype(jnp.int32)
            e, first = e + past, first + past * n
        slot, pos0, s_lo = place(e)
        j, head = i - first, jnp.int32(0)
        for m in range(1, n_kv):
            head = head + (i - first >= m * (n_run - s_lo)).astype(jnp.int32)
        return slot, head, (s_lo + j - head * (n_run - s_lo)) * RUNS, pos0

    for c in local:
        c.wait()
    for c in share:
        c.wait()

    exp_scale = scale * math.log2(math.e)

    def step(i, carry):
        (slot_p, head_p, s_p), (slot, head, s, pos0) = carry
        now = lax.rem(i, 2)
        k, v = kvb[slot, head, :, :head_dim], kvb[slot, head, :, head_dim:]
        s_t = [jnp.dot(k, qt[head, s + r], preferred_element_type=F32) for r in range(RUNS)]
        dp_t = [jnp.dot(v, dot[head, s + r], preferred_element_type=F32) for r in range(RUNS)]
        p_p, ds_p = pbuf[1 - now], dsbuf[1 - now]
        q_p = qn[head_p, pl.ds(s_p, RUNS)].reshape(RUNS * width, head_dim)
        do_p = don[head_p, pl.ds(s_p, RUNS)].reshape(RUNS * width, head_dim)
        acc[slot_p, head_p, :, head_dim:] += jnp.dot(p_p, do_p, preferred_element_type=F32)
        acc[slot_p, head_p, :, :head_dim] += jnp.dot(ds_p, q_p, preferred_element_type=F32)
        k_t = kvb[slot_p, head_p, :, :head_dim].T
        for r in range(RUNS):
            dqa[head_p, s_p + r] += jnp.dot(k_t, ds_p[:, r * width:(r + 1) * width], preferred_element_type=F32)
        pos_f = pos0.astype(F32)
        k_iota = lax.broadcasted_iota(jnp.int32, (key_tile, width), 0).astype(F32)
        for r in range(RUNS):
            lse, delta = st[head, s + r, 0:1, :], st[head, s + r, 1:2, :]
            lo, hi = st[head, s + r, 2:3, :] - pos_f, st[head, s + r, 3:4, :] - pos_f
            ok = (k_iota >= lo) & (k_iota <= hi)
            p = jnp.where(ok, jnp.exp2(s_t[r] * exp_scale - lse), 0.0)
            pbuf[now, :, r * width:(r + 1) * width] = p.astype(BF16)
            dsbuf[now, :, r * width:(r + 1) * width] = (p * (dp_t[r] - delta)).astype(BF16)
        return (slot, head, s), item(i + 1)

    def advance(state, target):
        i, carry = state
        return jnp.maximum(i, target), lax.fori_loop(i, target, step, carry)

    def add(dst, src):
        steps = n_kv * 4
        cut = key_tile // 4

        @pl.loop(0, steps)
        def _(i):
            h, r = i // 4, pl.ds(pl.multiple_of(lax.rem(i, 4) * cut, 8), cut)
            acc[dst, h, r, :] += rsb[src, h, r, :]

    def end_of(e):
        out = jnp.int32(0)
        for v, n in enumerate(counts):
            out = out + jnp.where(e >= v, n, 0)
        return out

    def gather_event(k, state):
        share_items = (early_items * (k + 1)) // (n_hop + 1)
        state = advance(state, jnp.minimum(share_items, end_of(jnp.minimum(2 * k + 1, n_early - 1))))
        for way in range(2):
            i = way * n_hop + k
            remote(kvb.at[i], kvb.at[i], ag_send.at[i], ag_recv.at[i], nbr[way]).wait_recv()

            @pl.when(k + 2 < n_hop)
            def _():
                remote(kvb.at[i], kvb.at[i + 2], ag_send.at[i + 2], ag_recv.at[i + 2], nbr[way]).start()
        return state

    def reduce_event(m, state):
        k, way = n_hop - 1 - m // 2, m % 2
        i = way * n_hop + k
        peer = jnp.where(way == 0, left, right)
        state = advance(state, end_of(n_early + m) + 1)

        @pl.when(k + 2 < n_hop)
        def _():
            remote(acc.at[i + 2], rsb.at[i + 2], rs_send.at[i + 2], rs_recv.at[i + 2], peer).wait_recv()
            add(i, i + 2)

        remote(acc.at[i], rsb.at[i], rs_send.at[i], rs_recv.at[i], peer).start()
        return state

    state = (jnp.int32(0), (item(jnp.int32(0))[:3], item(jnp.int32(0))))
    state = lax.fori_loop(0, n_hop, gather_event, state)
    state = lax.fori_loop(0, 2 * n_hop, reduce_event, state)
    swap = remote(part_of(dqa, 1), dqr, x_send.at[len(pairs)], x_recv.at[len(pairs)], sibling)
    swap.start()
    swap.wait_recv()

    @pl.loop(0, n_kv * n_sub)
    def _(i):
        h, s = i // n_sub, lax.rem(i, n_sub)
        dqo[h, s] = ((dqa[h, s, :, :rows] + dqr[h, s]) * scale).astype(BF16).T

    put_dq = pltpu.make_async_copy(dqo, dq_out, out_sem.at[0])
    put_dq.start()
    for k in reversed(range(min(2, n_hop))):
        for way in range(2):
            reduce_copy(way, k).wait_recv()
            add(own + half_of(way, k), way * n_hop + k)

    @pl.loop(0, 2 * n_kv)
    def _(i):
        half, h = i // n_kv, lax.rem(i, n_kv)
        acc[own + half, h, :, :head_dim] = acc[own + half, h, :, :head_dim] * scale

    put_kv = pltpu.make_async_copy(acc.at[pl.ds(own, 2)], dkv_out, out_sem.at[1])
    put_kv.start()
    swap.wait_send()
    for way in range(2):
        for j in range(n_hop):
            gather(way, j).wait_send()
            reduce_copy(way, j).wait_send()
    put_dq.wait()
    put_kv.wait()


def solution(mesh):
    cp_size = mesh.shape['cp']
    q_spec = P(None, 'cp', 'tp', None)
    lse_spec = P(None, 'cp', 'tp')
    kv_spec = P('cp', 'tp', None)

    def local_backward(query, out_act, out_grad, row_lse, key_act, value_act, doc_ids):
        n_sub, local_len, n_heads, head_dim = query.shape
        keys_local, n_kv = key_act.shape[0], key_act.shape[1]
        group = n_heads // n_kv
        sub_len = local_len * cp_size
        sub_start = keys_local * cp_size - n_sub * sub_len
        scale = head_dim ** -0.5
        rows = local_len * group
        half = keys_local // 2
        n_hop = cp_size // CORES - 1
        n_slot = 2 * n_hop + 2
        me = lax.axis_index('cp')

        def by_head(x):
            x = x.reshape((n_sub, local_len, n_kv, group) + x.shape[3:])
            x = jnp.moveaxis(x, 2, 0)
            return x.reshape((n_kv, n_sub, rows) + x.shape[4:])

        delta = jnp.einsum('sqhd,sqhd->sqh', out_grad, out_act, preferred_element_type=F32)
        q_doc = lax.dynamic_slice_in_dim(doc_ids[sub_start:].reshape(n_sub, sub_len), me * local_len, local_len, axis=1)
        q_first = jnp.sum((doc_ids[None, None, :] < q_doc[:, :, None]).astype(F32), axis=-1)
        q_pos = (sub_start + me * local_len + jnp.arange(n_sub)[:, None] * sub_len + jnp.arange(local_len)[None, :]).astype(F32)
        wide = lambda x: jnp.broadcast_to(jnp.repeat(x, group, axis=1)[None], (n_kv, n_sub, rows))
        lines = [by_head(row_lse) * math.log2(math.e), by_head(delta), wide(q_first), wide(q_pos)]
        stats = jnp.stack(lines + [jnp.zeros_like(lines[0])] * 4, axis=2)
        qn, don = by_head(query), by_head(out_grad)
        cut = lambda x: jnp.transpose(x.reshape(2, half, n_kv, head_dim), (0, 2, 1, 3))
        kv = jnp.concatenate([cut(key_act), cut(value_act)], axis=-1)
        flops = 2 * 5 * n_kv * n_sub * 2 * rows * head_dim * keys_local * n_hop
        hbm = pl.BlockSpec(memory_space=pl.ANY)
        dma = pltpu.SemaphoreType.DMA
        dq, dkv = pl.pallas_call(
            functools.partial(ring_kernel, cp_size, sub_start, local_len, scale, EARLY_ITEMS),
            name='ring_backward',
            out_shape=(jax.ShapeDtypeStruct((n_kv, n_sub, rows, head_dim), BF16),
                       jax.ShapeDtypeStruct((2, n_kv, half, 2 * head_dim), F32)),
            in_specs=[hbm] * 6,
            out_specs=(hbm, hbm),
            scratch_shapes=[
                pltpu.VMEM((n_slot, n_kv, half, 2 * head_dim), BF16),
                pltpu.VMEM((n_slot, n_kv, half, 2 * head_dim), F32),
                pltpu.VMEM((2 * n_hop, n_kv, half, 2 * head_dim), F32),
                pltpu.VMEM((n_kv, n_sub, CORES * rows, head_dim), BF16),
                pltpu.VMEM((n_kv, n_sub, head_dim, CORES * rows), BF16),
                pltpu.VMEM((n_kv, n_sub, CORES * rows, head_dim), BF16),
                pltpu.VMEM((n_kv, n_sub, head_dim, CORES * rows), BF16),
                pltpu.VMEM((n_kv, n_sub, 8, CORES * rows), F32),
                pltpu.VMEM((n_kv, n_sub, head_dim, CORES * rows), F32),
                pltpu.VMEM((n_kv, n_sub, head_dim, rows), F32),
                pltpu.VMEM((n_kv, n_sub, rows, head_dim), BF16),
                pltpu.VMEM((2, half, RUNS * CORES * rows), BF16),
                pltpu.VMEM((2, half, RUNS * CORES * rows), BF16),
                dma((2 * n_hop,)), dma((2 * n_hop,)), dma((2 * n_hop,)), dma((2 * n_hop,)),
                dma((6,)), dma((6,)), dma((6,)), dma((2,)),
            ],
            compiler_params=pltpu.CompilerParams(collective_id=0, has_side_effects=True, vmem_limit_bytes=62 * 1024 * 1024),
            cost_estimate=pl.CostEstimate(flops=flops, bytes_accessed=30 * 2 ** 20, transcendentals=0),
        )(kv, qn, jnp.swapaxes(qn, 2, 3), don, jnp.swapaxes(don, 2, 3), stats)
        dq = jnp.moveaxis(dq.reshape(n_kv, n_sub, local_len, group, head_dim), 0, 2).reshape(query.shape)
        dkv = jnp.transpose(dkv, (0, 2, 1, 3)).reshape(keys_local, n_kv, 2 * head_dim)
        return dq, dkv[..., :head_dim], dkv[..., head_dim:]

    return jax.shard_map(local_backward, mesh=mesh, in_specs=(q_spec, q_spec, q_spec, lse_spec, kv_spec, kv_spec, P()),
                         out_specs=(q_spec, kv_spec, kv_spec), check_vma=False)
```

```python
import functools
import math

import jax
import jax.numpy as jnp
from jax import lax
from jax.experimental import pallas as pl
from jax.experimental.pallas import tpu as pltpu
from jax.sharding import PartitionSpec as P

MESH = pl.DeviceIdType.MESH
CORES = 2
LANES = 128
RUNS = 2
UNROLL = 2
EARLY_ITEMS = 98
F32 = jnp.float32
BF16 = jnp.bfloat16


def ring_kernel(cp_size, sub_start, scale, kv_in, q_in, o_in, do_in, lse_in, doc_in, dq_out, dkv_out,
                kvb, acc, rsb, raw_q, raw_do, raw_o, lse, docs, qn, qt, don, dot, lines, key_doc, dqa, dqr, dqo, pbuf, dsbuf,
                ag_send, ag_recv, rs_send, rs_recv, x_send, x_recv, loc_sem, out_sem):
    n_chip = cp_size // CORES
    n_hop = n_chip - 1
    n_sub, local_len, n_kv, group, head_dim = q_in.shape
    rows = local_len * group
    width = CORES * rows
    key_tile = kv_in.shape[2]
    span = local_len * CORES
    sub_len = local_len * cp_size
    keys_local = 2 * key_tile
    own = 2 * n_hop

    me = lax.axis_index('cp')
    chip, core = me // CORES, lax.rem(me, CORES)
    right = lax.rem(me + CORES, cp_size)
    left = lax.rem(me + cp_size - CORES, cp_size)
    sibling = me + 1 - 2 * core
    nbr = (right, left)

    barrier = pltpu.get_barrier_semaphore()
    for peer in (right, left, sibling):
        pl.semaphore_signal(barrier, inc=1, device_id={'cp': peer}, device_id_type=MESH)
    pl.semaphore_wait(barrier, 3)

    def remote(src, dst, send, recv, peer):
        return pltpu.make_async_remote_copy(src_ref=src, dst_ref=dst, send_sem=send, recv_sem=recv,
                                            device_id={'cp': peer}, device_id_type=MESH)

    for j in range(2):
        for way in range(2):
            i = way * n_hop + j
            remote(kv_in.at[(j + way) % 2], kvb.at[i], ag_send.at[i], ag_recv.at[i], nbr[way]).start()
    share = [remote(q_in, raw_q.at[1], x_send.at[0], x_recv.at[0], sibling),
             remote(do_in, raw_do.at[1], x_send.at[1], x_recv.at[1], sibling)]
    local = [pltpu.make_async_copy(a, b, loc_sem.at[i]) for i, (a, b) in enumerate((
        (doc_in, docs), (lse_in, lse), (do_in, raw_do.at[0]), (o_in, raw_o), (q_in, raw_q.at[0]), (kv_in, kvb.at[pl.ds(own, 2)])))]
    for c in local + share:
        c.start()

    def mine(which):
        return lines.at[:, :, :, pl.ds(which * rows, rows)]

    share_lines = remote(mine(0), mine(1), x_send.at[2], x_recv.at[2], sibling)

    @pl.loop(0, n_sub)
    def _(s):
        for h in range(n_kv):
            dqa[h, s] = jnp.zeros(dqa.shape[2:], F32)

    @pl.loop(0, acc.shape[0])
    def _(i):
        for h in range(n_kv):
            acc[i, h] = jnp.zeros(acc.shape[2:], F32)

    pbuf[...] = jnp.zeros(pbuf.shape, BF16)
    dsbuf[...] = jnp.zeros(dsbuf.shape, BF16)
    local[0].wait()
    tiles = keys_local // LANES

    @pl.loop(0, n_chip * tiles)
    def _(i):
        b, r = i // tiles, lax.rem(i, tiles)
        row = (b * CORES + core) * tiles + r
        key_doc[b, pl.ds(pl.multiple_of(r * LANES, LANES), LANES), :] = jnp.broadcast_to(docs[pl.ds(row, 1), :], (LANES, LANES)).T

    lane = lax.broadcasted_iota(jnp.int32, (8, rows), 1)
    sub = lax.broadcasted_iota(jnp.int32, (8, rows), 0)
    for c in local[1:4]:
        c.wait()

    @pl.loop(0, n_sub)
    def _(s):
        rep = jnp.concatenate([lse[s]] * (LANES // local_len), axis=1)
        wide = jnp.take_along_axis(rep, lane // group, axis=1)
        for h in range(n_kv):
            line = jnp.sum(jnp.where(sub - group * h == lane % group, wide, 0.0), axis=0, keepdims=True) * math.log2(math.e)
            prod = raw_do[0, s, :, h].reshape(rows, head_dim).astype(F32) * raw_o[s, :, h].reshape(rows, head_dim).astype(F32)
            total = jnp.broadcast_to(jnp.sum(prod, axis=1, keepdims=True), (rows, LANES)).T
            first = sub_start + s * sub_len + me * local_len
            doc_row = jnp.broadcast_to(docs[pl.ds(first // LANES, 1), :], (8, LANES))
            doc = jnp.take_along_axis(doc_row, lax.rem(first, LANES) + lane // group, axis=1).astype(F32)
            lines[h, s, :, :rows] = jnp.where(sub == 0, line, jnp.where(sub == 1, total[:8, :], doc))

    share_lines.start()

    def spread(c):
        @pl.loop(0, n_sub)
        def _(s):
            for h in range(n_kv):
                for raw, nat, tr in ((raw_q, qn, qt), (raw_do, don, dot)):
                    x = raw[c, s, :, h].reshape(rows, head_dim)
                    nat[h, s, c * rows:(c + 1) * rows, :] = x
                    tr[h, s, :, c * rows:(c + 1) * rows] = x.T

    for c in local[4:]:
        c.wait()
    spread(0)
    for c in share:
        c.wait()
    spread(1)
    share_lines.wait()

    n_run = n_sub // RUNS
    n_early = 2 + min(8, 2 * n_hop)
    n_late = 2 * n_hop * n_kv

    def place(e):
        early = e < n_early
        f = jnp.where(early, e - 2, e - n_early)
        k = jnp.where(early, f // 2, n_hop - 1 - f // (2 * n_kv))
        way = f % 2
        mine = e < 2
        slot = jnp.where(mine, own + e, way * n_hop + k)
        half = jnp.where(mine, e, (k + way) % 2)
        hop = k // 2 + 1
        key_chip = jnp.where(mine, chip, lax.rem(chip + jnp.where(way == 1, hop, n_chip - hop), n_chip))
        pos0 = (key_chip * CORES + core) * keys_local + half * key_tile
        s_lo = jnp.minimum(jnp.maximum(pos0 - sub_start - span * chip - span + sub_len, 0) // sub_len, n_sub - 1)
        return slot, key_chip, half, s_lo // RUNS

    counts, ends, taken = [], [], []
    total = jnp.int32(0)
    for e in range(n_early + n_late):
        n = n_run - place(jnp.int32(e))[3]
        if e < n_early:
            n = n * n_kv
            fits = jnp.int32(1) if e < 2 else (total + n <= EARLY_ITEMS).astype(jnp.int32)
            if e > 2:
                fits = fits * taken[-1]
            taken.append(fits)
            n = n * fits
        else:
            f = e - n_early
            i_early = 2 + 2 * (n_hop - 1 - f // (2 * n_kv)) + f % 2
            if i_early < n_early:
                n = n * (1 - taken[i_early])
        total = total + n
        counts.append(n)
        ends.append(total)

    n_taken = taken[0]
    for t in taken[1:]:
        n_taken = n_taken + t

    def following(at):
        i, e, j, n = at
        over = j + 1 >= n
        e1 = e + 1
        e1 = jnp.where(e1 == n_taken, n_early, e1)
        f = e1 - n_early
        again = (f >= 0) & (2 + 2 * (n_hop - 1 - f // (2 * n_kv)) + f % 2 < n_taken)
        e1 = jnp.minimum(jnp.where(again, e1 + 1, e1), n_early + n_late - 1)
        e, j = jnp.where(over, e1, e), jnp.where(over, 0, j + 1)
        slot, key_chip, half, s_lo = place(e)
        nth = jnp.int32(0)
        for m in range(1, n_kv):
            nth = nth + (j >= m * (n_run - s_lo)).astype(jnp.int32)
        head = jnp.where(e < n_early, nth, (e - n_early) // 2 % n_kv)
        n = (n_run - s_lo) * jnp.where(e < n_early, n_kv, 1)
        i = i + 1
        s = (s_lo + j - jnp.where(e < n_early, nth, 0) * (n_run - s_lo)) * RUNS
        return (slot, head, s, key_chip, half, (i < total).astype(jnp.int32)), (i, e, j, n)

    exp_scale = scale * math.log2(math.e)
    k_iota = lax.broadcasted_iota(jnp.int32, (key_tile, width), 0)
    col = lax.broadcasted_iota(jnp.int32, (1, width), 1)
    q_off = sub_start + jnp.where(col < rows, me, sibling) * local_len + lax.rem(col, rows) // group

    def one(now, carry):
        (slot_p, head_p, s_p), (slot, head, s, key_chip, half, live), at = carry
        then, at = following(at)
        k, v = kvb[slot, head, :, :head_dim], kvb[slot, head, :, head_dim:]
        s_t = [jnp.dot(k, qt[head, s + r], preferred_element_type=F32) for r in range(RUNS)]
        dp_t = [jnp.dot(v, dot[head, s + r], preferred_element_type=F32) for r in range(RUNS)]
        p_p, ds_p = pbuf[1 - now], dsbuf[1 - now]
        q_p = qn[head_p, pl.ds(s_p, RUNS)].reshape(RUNS * width, head_dim)
        do_p = don[head_p, pl.ds(s_p, RUNS)].reshape(RUNS * width, head_dim)
        acc[slot_p, head_p, :, head_dim:] += jnp.dot(p_p, do_p, preferred_element_type=F32)
        acc[slot_p, head_p, :, :head_dim] += jnp.dot(ds_p, q_p, preferred_element_type=F32)
        k_t = kvb[slot_p, head_p, :, :head_dim].T
        for r in range(RUNS):
            dqa[head_p, s_p + r] += jnp.dot(k_t, ds_p[:, r * width:(r + 1) * width], preferred_element_type=F32)
        docs_k = key_doc[key_chip, pl.ds(pl.multiple_of(half * key_tile, 8), key_tile), :]
        docs_k = jnp.concatenate([docs_k] * (width // LANES), axis=1)
        pos0 = (key_chip * CORES + core) * keys_local + half * key_tile
        for r in range(RUNS):
            lse_r, delta_r, doc_r = [lines[head, s + r, m:m + 1, :] for m in range(3)]
            last = jnp.where(live == 1, q_off + (s + r) * sub_len - pos0, -1)
            ok = (docs_k == doc_r.astype(jnp.int32)) & (k_iota <= last)
            p = jnp.where(ok, jnp.exp2(s_t[r] * exp_scale - lse_r), 0.0)
            pbuf[now, :, r * width:(r + 1) * width] = p.astype(BF16)
            dsbuf[now, :, r * width:(r + 1) * width] = (p * (dp_t[r] - delta_r)).astype(BF16)
        return (slot, head, s), then, at

    def advance(state, target):
        i, carry = state
        m = jnp.maximum(target - i, 0) // UNROLL

        def step(_, carry):
            for u in range(UNROLL):
                carry = one(u % 2, carry)
            return carry

        return i + m * UNROLL, lax.fori_loop(0, m, step, carry)

    def end_of(e):
        out = jnp.int32(0)
        for v, n in enumerate(counts):
            out = out + jnp.where(e >= v, n, 0)
        return out

    def gather_event(k, state):
        goal = (EARLY_ITEMS * (k + 1)) // n_hop
        state = advance(state, jnp.minimum(goal, end_of(jnp.minimum(2 * k + 1, n_early - 1))))
        for way in range(2):
            i = way * n_hop + k
            remote(kvb.at[i], kvb.at[i], ag_send.at[i], ag_recv.at[i], nbr[way]).wait_recv()

            @pl.when(k + 2 < n_hop)
            def _():
                remote(kvb.at[i], kvb.at[i + 2], ag_send.at[i + 2], ag_recv.at[i + 2], nbr[way]).start()
        return state

    def add(dst, src, head):
        cut = key_tile // 4

        @pl.loop(0, 4)
        def _(i):
            r = pl.ds(pl.multiple_of(i * cut, 8), cut)
            acc[dst, head, r, :] += rsb[src, head, r, :]

    def partial(i, head, peer):
        return remote(acc.at[i, head], rsb.at[i, head], rs_send.at[i, head], rs_recv.at[i, head], peer)

    def reduce_event(m, state):
        k, head, way = n_hop - 1 - m // (2 * n_kv), m // 2 % n_kv, m % 2
        i = way * n_hop + k
        peer = jnp.where(way == 0, left, right)
        state = advance(state, end_of(n_early + m) + UNROLL)

        @pl.when(k + 2 < n_hop)
        def _():
            partial(i + 2, head, peer).wait_recv()
            add(i, i + 2, head)

        partial(i, head, peer).start()
        return state

    zero = jnp.int32(0)
    start, at = following((zero - 1, zero, zero - 1, zero + 1))
    state = (zero, (start[:3], start, at))
    state = lax.fori_loop(0, n_hop, gather_event, state)
    state = lax.fori_loop(0, n_late, reduce_event, state)
    half_rows = lambda which: dqa.at[:, :, :, pl.ds(which * rows, rows)]
    swap = remote(half_rows(1), dqr, x_send.at[3], x_recv.at[3], sibling)
    swap.start()
    swap.wait_recv()

    @pl.loop(0, n_sub)
    def _(s):
        for h in range(n_kv):
            x = ((dqa[h, s, :, :rows] + dqr[h, s]) * scale).astype(BF16).T
            dqo[s, :, h] = x.reshape(local_len, group, head_dim)

    put_dq = pltpu.make_async_copy(dqo, dq_out, out_sem.at[0])
    put_dq.start()
    for head in range(n_kv):
        for k in reversed(range(2)):
            for way in range(2):
                partial(way * n_hop + k, head, nbr[1 - way]).wait_recv()
                add(own + (k + way) % 2, way * n_hop + k, head)

    @pl.loop(0, 2)
    def _(half):
        for h in range(n_kv):
            acc[own + half, h, :, :head_dim] = acc[own + half, h, :, :head_dim] * scale

    put_kv = pltpu.make_async_copy(acc.at[pl.ds(own, 2)], dkv_out, out_sem.at[1])
    put_kv.start()
    swap.wait_send()
    for way in range(2):
        for j in range(n_hop):
            i = way * n_hop + j
            remote(kvb.at[i], kvb.at[i], ag_send.at[i], ag_recv.at[i], nbr[way]).wait_send()
            for head in range(n_kv):
                partial(i, head, nbr[1 - way]).wait_send()
    put_dq.wait()
    put_kv.wait()


def solution(mesh):
    cp_size = mesh.shape['cp']
    q_spec = P(None, 'cp', 'tp', None)
    lse_spec = P(None, 'cp', 'tp')
    kv_spec = P('cp', 'tp', None)

    def local_backward(query, out_act, out_grad, row_lse, key_act, value_act, doc_ids):
        n_sub, local_len, n_heads, head_dim = query.shape
        keys_local, n_kv = key_act.shape[0], key_act.shape[1]
        group = n_heads // n_kv
        sub_start = keys_local * cp_size - n_sub * local_len * cp_size
        rows = local_len * group
        half = keys_local // 2
        n_chip = cp_size // CORES
        n_hop = n_chip - 1
        n_slot = 2 * n_hop + 2
        q5 = (n_sub, local_len, n_kv, group, head_dim)
        cut = lambda x: jnp.transpose(x.reshape(2, half, n_kv, head_dim), (0, 2, 1, 3))
        kv = jnp.concatenate([cut(key_act), cut(value_act)], axis=-1)
        flops = 2 * 5 * n_kv * n_sub * 2 * rows * head_dim * keys_local * n_hop
        hbm = pl.BlockSpec(memory_space=pl.ANY)
        dma = pltpu.SemaphoreType.DMA
        vmem = pltpu.VMEM
        dq, dkv = pl.pallas_call(
            functools.partial(ring_kernel, cp_size, sub_start, head_dim ** -0.5),
            name='ring_backward',
            out_shape=(jax.ShapeDtypeStruct(q5, BF16), jax.ShapeDtypeStruct((2, n_kv, half, 2 * head_dim), F32)),
            in_specs=[hbm] * 6,
            out_specs=(hbm, hbm),
            scratch_shapes=[
                vmem((n_slot, n_kv, half, 2 * head_dim), BF16),
                vmem((n_slot, n_kv, half, 2 * head_dim), F32),
                vmem((2 * n_hop, n_kv, half, 2 * head_dim), F32),
                vmem((CORES,) + q5, BF16),
                vmem((CORES,) + q5, BF16),
                vmem(q5, BF16),
                vmem((n_sub, n_heads, local_len), F32),
                vmem((doc_ids.shape[0] // LANES, LANES), jnp.int32),
                vmem((n_kv, n_sub, CORES * rows, head_dim), BF16),
                vmem((n_kv, n_sub, head_dim, CORES * rows), BF16),
                vmem((n_kv, n_sub, CORES * rows, head_dim), BF16),
                vmem((n_kv, n_sub, head_dim, CORES * rows), BF16),
                vmem((n_kv, n_sub, 8, CORES * rows), F32),
                vmem((n_chip, keys_local, LANES), jnp.int32),
                vmem((n_kv, n_sub, head_dim, CORES * rows), F32),
                vmem((n_kv, n_sub, head_dim, rows), F32),
                vmem(q5, BF16),
                vmem((2, half, RUNS * CORES * rows), BF16),
                vmem((2, half, RUNS * CORES * rows), BF16),
                dma((2 * n_hop,)), dma((2 * n_hop,)), dma((2 * n_hop, n_kv)), dma((2 * n_hop, n_kv)),
                dma((4,)), dma((4,)), dma((6,)), dma((2,)),
            ],
            compiler_params=pltpu.CompilerParams(collective_id=0, has_side_effects=True, vmem_limit_bytes=62 * 1024 * 1024),
            cost_estimate=pl.CostEstimate(flops=flops, bytes_accessed=30 * 2 ** 20, transcendentals=0),
        )(kv, query.reshape(q5), out_act.reshape(q5), out_grad.reshape(q5), jnp.swapaxes(row_lse, 1, 2), doc_ids.reshape(-1, LANES))
        dkv = jnp.transpose(dkv, (0, 2, 1, 3)).reshape(keys_local, n_kv, 2 * head_dim)
        return dq.reshape(query.shape), dkv[..., :head_dim], dkv[..., head_dim:]

    return jax.shard_map(local_backward, mesh=mesh, in_specs=(q_spec, q_spec, q_spec, lse_spec, kv_spec, kv_spec, P()),
                         out_specs=(q_spec, kv_spec, kv_spec), check_vma=False)
```

```python
import functools
import math

import jax
import jax.numpy as jnp
from jax import lax
from jax.experimental import pallas as pl
from jax.experimental.pallas import tpu as pltpu
from jax.sharding import PartitionSpec as P

MESH = pl.DeviceIdType.MESH
CORES = 2
LANES = 128
RUNS = 2
UNROLL = 2
EARLY_ITEMS = (36, 40)
F32 = jnp.float32
BF16 = jnp.bfloat16


def ring_kernel(cp_size, sub_start, scale, kv_in, q_in, o_in, do_in, lse_in, doc_in, dq_out, dk_out, dv_out,
                kvb, acc, rsb, raw_q, raw_do, raw_o, lse, docs, qn, qt, don, dot, lines, key_doc, dqa, dqr, dqo, dko, dvo, pbuf, dsbuf,
                ag_send, ag_recv, rs_send, rs_recv, x_send, x_recv, loc_sem, out_sem):
    n_chip = cp_size // CORES
    n_hop = n_chip - 1
    n_sub, local_len, n_kv, group, head_dim = q_in.shape
    rows = local_len * group
    width = CORES * rows
    key_tile = kv_in.shape[2]
    span = local_len * CORES
    sub_len = local_len * cp_size
    keys_local = 2 * key_tile
    own = 2 * n_hop

    me = lax.axis_index('cp')
    chip, core = me // CORES, lax.rem(me, CORES)
    right = lax.rem(me + CORES, cp_size)
    left = lax.rem(me + cp_size - CORES, cp_size)
    sibling = me + 1 - 2 * core
    nbr = (right, left)

    barrier = pltpu.get_barrier_semaphore()
    for peer in (right, left, sibling):
        pl.semaphore_signal(barrier, inc=1, device_id={'cp': peer}, device_id_type=MESH)
    pl.semaphore_wait(barrier, 3)

    def remote(src, dst, send, recv, peer):
        return pltpu.make_async_remote_copy(src_ref=src, dst_ref=dst, send_sem=send, recv_sem=recv,
                                            device_id={'cp': peer}, device_id_type=MESH)

    def gather(way, k, head, src=None):
        i = way * n_hop + k
        return remote(kvb.at[i, head] if src is None else src, kvb.at[i, head], ag_send.at[i, head], ag_recv.at[i, head], nbr[way])

    def gather_own(head):
        for j in range(2):
            for way in range(2):
                gather(way, j, head, kv_in.at[(j + way) % 2, head]).start()

    def pass_on(k, head):
        for way in range(2):
            gather(way, k, head).wait_recv()
            i = way * n_hop + k

            @pl.when(k + 2 < n_hop)
            def _():
                gather(way, k + 2, head, kvb.at[i, head]).start()

    gather_own(0)
    share = [remote(q_in, raw_q.at[1], x_send.at[0], x_recv.at[0], sibling),
             remote(do_in, raw_do.at[1], x_send.at[1], x_recv.at[1], sibling)]
    local = [pltpu.make_async_copy(a, b, loc_sem.at[i]) for i, (a, b) in enumerate((
        (doc_in, docs), (lse_in, lse), (do_in, raw_do.at[0]), (o_in, raw_o), (q_in, raw_q.at[0]), (kv_in, kvb.at[pl.ds(own, 2)])))]
    for c in local + share:
        c.start()

    def mine(which):
        return lines.at[:, :, :, pl.ds(which * rows, rows)]

    share_lines = remote(mine(0), mine(1), x_send.at[2], x_recv.at[2], sibling)

    @pl.loop(0, n_sub)
    def _(s):
        for h in range(n_kv):
            dqa[h, s] = jnp.zeros(dqa.shape[2:], F32)

    @pl.loop(0, acc.shape[0])
    def _(i):
        for h in range(n_kv):
            acc[i, h] = jnp.zeros(acc.shape[2:], F32)

    pbuf[...] = jnp.zeros(pbuf.shape, BF16)
    dsbuf[...] = jnp.zeros(dsbuf.shape, BF16)
    local[0].wait()
    tiles = keys_local // LANES

    @pl.loop(0, n_chip * tiles)
    def _(i):
        b, r = i // tiles, lax.rem(i, tiles)
        row = (b * CORES + core) * tiles + r
        key_doc[b, pl.ds(pl.multiple_of(r * LANES, LANES), LANES), :] = jnp.broadcast_to(docs[pl.ds(row, 1), :], (LANES, LANES)).T

    lane = lax.broadcasted_iota(jnp.int32, (8, rows), 1)
    sub = lax.broadcasted_iota(jnp.int32, (8, rows), 0)
    for c in local[1:4]:
        c.wait()

    @pl.loop(0, n_sub)
    def _(s):
        rep = jnp.concatenate([lse[s]] * (LANES // local_len), axis=1)
        wide = jnp.take_along_axis(rep, lane // group, axis=1)
        for h in range(n_kv):
            line = jnp.sum(jnp.where(sub - group * h == lane % group, wide, 0.0), axis=0, keepdims=True) * math.log2(math.e)
            prod = raw_do[0, s, :, h].reshape(rows, head_dim).astype(F32) * raw_o[s, :, h].reshape(rows, head_dim).astype(F32)
            total = jnp.broadcast_to(jnp.sum(prod, axis=1, keepdims=True), (rows, LANES)).T
            first = sub_start + s * sub_len + me * local_len
            doc_row = jnp.broadcast_to(docs[pl.ds(first // LANES, 1), :], (8, LANES))
            doc = jnp.take_along_axis(doc_row, lax.rem(first, LANES) + lane // group, axis=1).astype(F32)
            lines[h, s, :, :rows] = jnp.where(sub == 0, line, jnp.where(sub == 1, total[:8, :], doc))

    share_lines.start()

    def spread(c):
        @pl.loop(0, n_sub)
        def _(s):
            for h in range(n_kv):
                for raw, nat, tr in ((raw_q, qn, qt), (raw_do, don, dot)):
                    x = raw[c, s, :, h].reshape(rows, head_dim)
                    nat[h, s, c * rows:(c + 1) * rows, :] = x
                    tr[h, s, :, c * rows:(c + 1) * rows] = x.T

    for c in local[4:]:
        c.wait()
    spread(0)
    pass_on(0, 0)
    for c in share:
        c.wait()
    spread(1)
    share_lines.wait()

    n_run = n_sub // RUNS
    n_early = 2 + min(8, 2 * n_hop)
    n_block = n_early + 2 * n_hop

    def place(e):
        head, e = e // n_block, lax.rem(e, n_block)
        early = e < n_early
        f = jnp.where(early, e - 2, e - n_early)
        k = jnp.where(early, f // 2, n_hop - 1 - f // 2)
        way = f % 2
        mine = e < 2
        slot = jnp.where(mine, own + e, way * n_hop + k)
        half = jnp.where(mine, e, (k + way) % 2)
        hop = k // 2 + 1
        key_chip = jnp.where(mine, chip, lax.rem(chip + jnp.where(way == 1, hop, n_chip - hop), n_chip))
        pos0 = (key_chip * CORES + core) * keys_local + half * key_tile
        s_lo = jnp.minimum(jnp.maximum(pos0 - sub_start - span * chip - span + sub_len, 0) // sub_len, n_sub - 1)
        return slot, head, key_chip, half, s_lo // RUNS

    counts, ends, n_taken = [], [], []
    total = jnp.int32(0)
    for head in range(n_kv):
        base, taken = total, []
        for e in range(n_block):
            n = n_run - place(jnp.int32(e))[4]
            if e < n_early:
                fits = jnp.int32(1) if e < 2 else (total + n <= base + EARLY_ITEMS[min(head, 1)]).astype(jnp.int32)
                taken.append(fits * taken[-1] if e > 2 else fits)
                n = n * taken[-1]
            else:
                f = e - n_early
                i_early = 2 + 2 * (n_hop - 1 - f // 2) + f % 2
                if i_early < n_early:
                    n = n * (1 - taken[i_early])
            total = total + n
            counts.append(n)
            ends.append(total)
        n_taken.append(sum(taken[1:], taken[0]))

    def following(at):
        i, e, j, n = at
        over = j + 1 >= n
        head, b = e // n_block, lax.rem(e, n_block) + 1
        limit = n_taken[0]
        for h in range(1, n_kv):
            limit = jnp.where(head == h, n_taken[h], limit)
        b = jnp.where(b == limit, n_early, b)
        f = b - n_early
        gone = lambda f: (f >= 0) & (2 + 2 * (n_hop - 1 - f // 2) + f % 2 < limit)
        b = jnp.where(gone(f), jnp.where((f % 2 == 1) | gone(f + 1), n_block, b + 1), b)
        e1 = jnp.minimum(head * n_block + b, n_kv * n_block - 1)
        e, j = jnp.where(over, e1, e), jnp.where(over, 0, j + 1)
        slot, head, key_chip, half, s_lo = place(e)
        i = i + 1
        return (slot, head, (s_lo + j) * RUNS, key_chip, half, (i < total).astype(jnp.int32)), (i, e, j, n_run - s_lo)

    exp_scale = scale * math.log2(math.e)
    k_iota = lax.broadcasted_iota(jnp.int32, (key_tile, width), 0)
    col = lax.broadcasted_iota(jnp.int32, (1, width), 1)
    q_off = sub_start + jnp.where(col < rows, me, sibling) * local_len + lax.rem(col, rows) // group

    def one(now, carry):
        (slot_p, head_p, s_p), (slot, head, s, key_chip, half, live), at = carry
        then, at = following(at)
        k, v = kvb[slot, head, :, :head_dim], kvb[slot, head, :, head_dim:]
        s_t = [jnp.dot(k, qt[head, s + r], preferred_element_type=F32) for r in range(RUNS)]
        dp_t = [jnp.dot(v, dot[head, s + r], preferred_element_type=F32) for r in range(RUNS)]
        p_p, ds_p = pbuf[1 - now], dsbuf[1 - now]
        q_p = qn[head_p, pl.ds(s_p, RUNS)].reshape(RUNS * width, head_dim)
        do_p = don[head_p, pl.ds(s_p, RUNS)].reshape(RUNS * width, head_dim)
        acc[slot_p, head_p, :, head_dim:] += jnp.dot(p_p, do_p, preferred_element_type=F32)
        acc[slot_p, head_p, :, :head_dim] += jnp.dot(ds_p, q_p, preferred_element_type=F32)
        k_t = kvb[slot_p, head_p, :, :head_dim].T
        for r in range(RUNS):
            dqa[head_p, s_p + r] += jnp.dot(k_t, ds_p[:, r * width:(r + 1) * width], preferred_element_type=F32)
        docs_k = key_doc[key_chip, pl.ds(pl.multiple_of(half * key_tile, 8), key_tile), :]
        docs_k = jnp.concatenate([docs_k] * (width // LANES), axis=1)
        pos0 = (key_chip * CORES + core) * keys_local + half * key_tile
        for r in range(RUNS):
            lse_r, delta_r, doc_r = [lines[head, s + r, m:m + 1, :] for m in range(3)]
            last = jnp.where(live == 1, q_off + (s + r) * sub_len - pos0, -1)
            ok = (docs_k == doc_r.astype(jnp.int32)) & (k_iota <= last)
            p = jnp.where(ok, jnp.exp2(s_t[r] * exp_scale - lse_r), 0.0)
            pbuf[now, :, r * width:(r + 1) * width] = p.astype(BF16)
            dsbuf[now, :, r * width:(r + 1) * width] = (p * (dp_t[r] - delta_r)).astype(BF16)
        return (slot, head, s), then, at

    def advance(state, target):
        i, carry = state
        m = jnp.maximum(target - i, 0) // UNROLL

        def step(_, carry):
            for u in range(UNROLL):
                carry = one(u % 2, carry)
            return carry

        return i + m * UNROLL, lax.fori_loop(0, m, step, carry)

    def end_of(e):
        out = jnp.int32(0)
        for v, n in enumerate(counts):
            out = out + jnp.where(e >= v, n, 0)
        return out

    def add(dst, src, head):
        cut = key_tile // 4

        @pl.loop(0, 4)
        def _(i):
            r = pl.ds(pl.multiple_of(i * cut, 8), cut)
            acc[dst, head, r, :] += rsb[src, head, r, :]

    def partial(i, head, peer):
        return remote(acc.at[i, head], rsb.at[i, head], rs_send.at[i, head], rs_recv.at[i, head], peer)

    def send_sums(k, way, head, state=None):
        i = way * n_hop + k
        peer = jnp.where(way == 0, left, right)
        if state is not None:
            state = advance(state, end_of(head * n_block + n_early + 2 * (n_hop - 1 - k) + way) + UNROLL)

        @pl.when(k + 2 < n_hop)
        def _():
            partial(i + 2, head, peer).wait_recv()
            add(i, i + 2, head)

        partial(i, head, peer).start()
        return state

    def arrive(k, state):
        goal = (EARLY_ITEMS[0] * k) // (n_hop - 1)
        state = advance(state, jnp.minimum(goal, end_of(jnp.minimum(2 * k + 1, n_early - 1))))
        pass_on(k, 0)

        @pl.when(k == max(n_hop - 3, 1))
        def _():
            gather_own(1)
        return state

    def both(head):
        def trip(m, state):
            state = lax.fori_loop(0, 2, lambda way, state: send_sums(n_hop - 1 - m, way, head, state), state)
            base = ends[(head + 1) * n_block - 1]
            goal = jnp.minimum(base + (EARLY_ITEMS[1] * (m + 1)) // n_hop, end_of((head + 1) * n_block + jnp.minimum(2 * m + 1, n_early - 1)))
            state = advance(state, jnp.where(state[0] >= base, goal, state[0]))
            pass_on(m, head + 1)
            if head + 2 < n_kv:
                @pl.when(m == max(n_hop - 3, 1))
                def _():
                    gather_own(head + 2)
            return state
        return trip

    def settle(head):
        for k in (1, 0):
            for way in range(2):
                partial(way * n_hop + k, head, nbr[1 - way]).wait_recv()
                add(own + (k + way) % 2, way * n_hop + k, head)

        @pl.loop(0, 2)
        def _(half):
            r = pl.ds(pl.multiple_of(half * key_tile, 8), key_tile)
            dko[r, head, :] = acc[own + half, head, :, :head_dim] * scale
            dvo[r, head, :] = acc[own + half, head, :, head_dim:]

    zero = jnp.int32(0)
    start, at = following((zero - 1, zero, zero - 1, zero + 1))
    state = (zero, (start[:3], start, at))
    state = lax.fori_loop(1, n_hop, arrive, state)
    for head in range(n_kv - 1):
        state = lax.fori_loop(0, n_hop, both(head), state)
    state = lax.fori_loop(0, 2 * n_hop - 4, lambda m, state: send_sums(n_hop - 1 - m // 2, m % 2, n_kv - 1, state), state)
    state = advance(state, total + UNROLL)
    half_rows = lambda which: dqa.at[:, :, :, pl.ds(which * rows, rows)]
    swap = remote(half_rows(1), dqr, x_send.at[3], x_recv.at[3], sibling)
    swap.start()
    for way in range(2):
        send_sums(1, way, n_kv - 1)
    swap.wait_recv()

    @pl.loop(0, n_sub)
    def _(s):
        for h in range(n_kv):
            x = ((dqa[h, s, :, :rows] + dqr[h, s]) * scale).astype(BF16).T
            dqo[s, :, h] = x.reshape(local_len, group, head_dim)

    puts = [pltpu.make_async_copy(a, b, out_sem.at[i]) for i, (a, b) in enumerate(((dqo, dq_out), (dko, dk_out), (dvo, dv_out)))]
    puts[0].start()
    for head in range(n_kv - 1):
        settle(head)
    for way in range(2):
        send_sums(0, way, n_kv - 1)
    settle(n_kv - 1)
    puts[1].start()
    puts[2].start()
    swap.wait_send()
    for way in range(2):
        for k in range(n_hop):
            for head in range(n_kv):
                gather(way, k, head).wait_send()
                partial(way * n_hop + k, head, nbr[1 - way]).wait_send()
    for c in puts:
        c.wait()


def solution(mesh):
    cp_size = mesh.shape['cp']
    q_spec = P(None, 'cp', 'tp', None)
    lse_spec = P(None, 'cp', 'tp')
    kv_spec = P('cp', 'tp', None)

    def local_backward(query, out_act, out_grad, row_lse, key_act, value_act, doc_ids):
        n_sub, local_len, n_heads, head_dim = query.shape
        keys_local, n_kv = key_act.shape[0], key_act.shape[1]
        group = n_heads // n_kv
        sub_start = keys_local * cp_size - n_sub * local_len * cp_size
        rows = local_len * group
        half = keys_local // 2
        n_chip = cp_size // CORES
        n_hop = n_chip - 1
        n_slot = 2 * n_hop + 2
        q5 = (n_sub, local_len, n_kv, group, head_dim)
        cut = lambda x: jnp.transpose(x.reshape(2, half, n_kv, head_dim), (0, 2, 1, 3))
        kv = jnp.concatenate([cut(key_act), cut(value_act)], axis=-1)
        flops = 2 * 5 * n_kv * n_sub * 2 * rows * head_dim * keys_local * n_hop
        hbm = pl.BlockSpec(memory_space=pl.ANY)
        dma = pltpu.SemaphoreType.DMA
        vmem = pltpu.VMEM
        dq, dk, dv = pl.pallas_call(
            functools.partial(ring_kernel, cp_size, sub_start, head_dim ** -0.5),
            name='ring_backward',
            out_shape=(jax.ShapeDtypeStruct(q5, BF16),) + (jax.ShapeDtypeStruct(key_act.shape, F32),) * 2,
            in_specs=[hbm] * 6,
            out_specs=(hbm,) * 3,
            scratch_shapes=[
                vmem((n_slot, n_kv, half, 2 * head_dim), BF16),
                vmem((n_slot, n_kv, half, 2 * head_dim), F32),
                vmem((2 * n_hop, n_kv, half, 2 * head_dim), F32),
                vmem((CORES,) + q5, BF16),
                vmem((CORES,) + q5, BF16),
                vmem(q5, BF16),
                vmem((n_sub, n_heads, local_len), F32),
                vmem((doc_ids.shape[0] // LANES, LANES), jnp.int32),
                vmem((n_kv, n_sub, CORES * rows, head_dim), BF16),
                vmem((n_kv, n_sub, head_dim, CORES * rows), BF16),
                vmem((n_kv, n_sub, CORES * rows, head_dim), BF16),
                vmem((n_kv, n_sub, head_dim, CORES * rows), BF16),
                vmem((n_kv, n_sub, 8, CORES * rows), F32),
                vmem((n_chip, keys_local, LANES), jnp.int32),
                vmem((n_kv, n_sub, head_dim, CORES * rows), F32),
                vmem((n_kv, n_sub, head_dim, rows), F32),
                vmem(q5, BF16),
                vmem(key_act.shape, F32),
                vmem(key_act.shape, F32),
                vmem((2, half, RUNS * CORES * rows), BF16),
                vmem((2, half, RUNS * CORES * rows), BF16),
                dma((2 * n_hop, n_kv)), dma((2 * n_hop, n_kv)), dma((2 * n_hop, n_kv)), dma((2 * n_hop, n_kv)),
                dma((4,)), dma((4,)), dma((6,)), dma((3,)),
            ],
            compiler_params=pltpu.CompilerParams(collective_id=0, has_side_effects=True, vmem_limit_bytes=62 * 1024 * 1024),
            cost_estimate=pl.CostEstimate(flops=flops, bytes_accessed=30 * 2 ** 20, transcendentals=0),
        )(kv, query.reshape(q5), out_act.reshape(q5), out_grad.reshape(q5), jnp.swapaxes(row_lse, 1, 2), doc_ids.reshape(-1, LANES))
        return dq.reshape(query.shape), dk, dv

    return jax.shard_map(local_backward, mesh=mesh, in_specs=(q_spec, q_spec, q_spec, lse_spec, kv_spec, kv_spec, P()),
                         out_specs=(q_spec, kv_spec, kv_spec), check_vma=False)
```

```python
import functools
import math

import jax
import jax.numpy as jnp
from jax import lax
from jax.experimental import pallas as pl
from jax.experimental.pallas import tpu as pltpu
from jax.sharding import PartitionSpec as P

MESH = pl.DeviceIdType.MESH
CORES = 2
LANES = 128
RUNS = 2
UNROLL = 2
EARLY_ITEMS = (36, 40)
F32 = jnp.float32
BF16 = jnp.bfloat16


def ring_kernel(cp_size, sub_start, scale, k_in, v_in, q_in, o_in, do_in, lse_in, doc_in, dq_out, dk_out, dv_out,
                kvb, acc, rsb, raw_q, raw_do, raw_o, lse, docs, qn, qt, don, dot, lines, key_doc, dqa, dqr, dqo, dko, dvo, pbuf, dsbuf,
                ag_send, ag_recv, rs_send, rs_recv, x_send, x_recv, loc_sem, out_sem):
    n_chip = cp_size // CORES
    n_hop = n_chip - 1
    n_sub, local_len, n_kv, group, head_dim = q_in.shape
    rows = local_len * group
    width = CORES * rows
    key_tile = k_in.shape[2]
    span = local_len * CORES
    sub_len = local_len * cp_size
    keys_local = 2 * key_tile
    own = 2 * n_hop

    me = lax.axis_index('cp')
    chip, core = me // CORES, lax.rem(me, CORES)
    right = lax.rem(me + CORES, cp_size)
    left = lax.rem(me + cp_size - CORES, cp_size)
    sibling = me + 1 - 2 * core
    nbr = (right, left)

    barrier = pltpu.get_barrier_semaphore()
    for peer in (right, left, sibling):
        pl.semaphore_signal(barrier, inc=1, device_id={'cp': peer}, device_id_type=MESH)
    pl.semaphore_wait(barrier, 3)

    def remote(src, dst, send, recv, peer):
        return pltpu.make_async_remote_copy(src_ref=src, dst_ref=dst, send_sem=send, recv_sem=recv,
                                            device_id={'cp': peer}, device_id_type=MESH)

    def gather(way, k, head, src=None):
        i = way * n_hop + k
        return remote(kvb.at[i, head] if src is None else src, kvb.at[i, head], ag_send.at[i, head], ag_recv.at[i, head], nbr[way])

    def sides(ref):
        return (ref.at[:, pl.ds(0, head_dim)], ref.at[:, pl.ds(head_dim, head_dim)])

    def gather_own(head):
        for j in range(2):
            for way in range(2):
                i = way * n_hop + j
                for src, dst in zip((k_in, v_in), sides(kvb.at[i, head])):
                    remote(src.at[(j + way) % 2, head], dst, ag_send.at[i, head], ag_recv.at[i, head], nbr[way]).start()

    def pass_on(k, head):
        for way in range(2):
            gather(way, k, head).wait_recv()
            i = way * n_hop + k

            @pl.when(k + 2 < n_hop)
            def _():
                gather(way, k + 2, head, kvb.at[i, head]).start()

    gather_own(0)
    share = [remote(q_in, raw_q.at[1], x_send.at[0], x_recv.at[0], sibling),
             remote(do_in, raw_do.at[1], x_send.at[1], x_recv.at[1], sibling)]
    local = [pltpu.make_async_copy(a, b, loc_sem.at[i]) for i, (a, b) in enumerate((
        (doc_in, docs), (lse_in, lse), (do_in, raw_do.at[0]), (o_in, raw_o), (q_in, raw_q.at[0]),
        (k_in, kvb.at[pl.ds(own, 2), :, :, pl.ds(0, head_dim)]), (v_in, kvb.at[pl.ds(own, 2), :, :, pl.ds(head_dim, head_dim)])))]
    for c in local + share:
        c.start()

    def mine(which):
        return lines.at[:, :, :, pl.ds(which * rows, rows)]

    share_lines = remote(mine(0), mine(1), x_send.at[2], x_recv.at[2], sibling)

    @pl.loop(0, n_sub)
    def _(s):
        for h in range(n_kv):
            dqa[h, s] = jnp.zeros(dqa.shape[2:], F32)

    @pl.loop(0, acc.shape[0])
    def _(i):
        for h in range(n_kv):
            acc[i, h] = jnp.zeros(acc.shape[2:], F32)

    pbuf[...] = jnp.zeros(pbuf.shape, BF16)
    dsbuf[...] = jnp.zeros(dsbuf.shape, BF16)
    local[0].wait()
    tiles = keys_local // LANES

    @pl.loop(0, n_chip * tiles)
    def _(i):
        b, r = i // tiles, lax.rem(i, tiles)
        row = (b * CORES + core) * tiles + r
        key_doc[b, pl.ds(pl.multiple_of(r * LANES, LANES), LANES), :] = jnp.broadcast_to(docs[pl.ds(row, 1), :], (LANES, LANES)).T

    lane = lax.broadcasted_iota(jnp.int32, (8, rows), 1)
    sub = lax.broadcasted_iota(jnp.int32, (8, rows), 0)
    for c in local[1:4]:
        c.wait()

    @pl.loop(0, n_sub)
    def _(s):
        rep = jnp.concatenate([lse[s]] * (LANES // local_len), axis=1)
        wide = jnp.take_along_axis(rep, lane // group, axis=1)
        for h in range(n_kv):
            line = jnp.sum(jnp.where(sub - group * h == lane % group, wide, 0.0), axis=0, keepdims=True) * math.log2(math.e)
            prod = raw_do[0, s, :, h].reshape(rows, head_dim).astype(F32) * raw_o[s, :, h].reshape(rows, head_dim).astype(F32)
            total = jnp.broadcast_to(jnp.sum(prod, axis=1, keepdims=True), (rows, LANES)).T
            first = sub_start + s * sub_len + me * local_len
            doc_row = jnp.broadcast_to(docs[pl.ds(first // LANES, 1), :], (8, LANES))
            doc = jnp.take_along_axis(doc_row, lax.rem(first, LANES) + lane // group, axis=1).astype(F32)
            lines[h, s, :, :rows] = jnp.where(sub == 0, line, jnp.where(sub == 1, total[:8, :], doc))

    share_lines.start()

    def spread(c):
        @pl.loop(0, n_sub)
        def _(s):
            for h in range(n_kv):
                for raw, nat, tr in ((raw_q, qn, qt), (raw_do, don, dot)):
                    x = raw[c, s, :, h].reshape(rows, head_dim)
                    nat[h, s, c * rows:(c + 1) * rows, :] = x
                    tr[h, s, :, c * rows:(c + 1) * rows] = x.T

    for c in local[4:]:
        c.wait()
    spread(0)
    pass_on(0, 0)
    for c in share:
        c.wait()
    spread(1)
    share_lines.wait()

    n_run = n_sub // RUNS
    n_early = 2 + min(8, 2 * n_hop)
    n_block = n_early + 2 * n_hop

    def place(e):
        head, e = e // n_block, lax.rem(e, n_block)
        early = e < n_early
        f = jnp.where(early, e - 2, e - n_early)
        k = jnp.where(early, f // 2, n_hop - 1 - f // 2)
        way = f % 2
        mine = e < 2
        slot = jnp.where(mine, own + e, way * n_hop + k)
        half = jnp.where(mine, e, (k + way) % 2)
        hop = k // 2 + 1
        key_chip = jnp.where(mine, chip, lax.rem(chip + jnp.where(way == 1, hop, n_chip - hop), n_chip))
        pos0 = (key_chip * CORES + core) * keys_local + half * key_tile
        s_lo = jnp.minimum(jnp.maximum(pos0 - sub_start - span * chip - span + sub_len, 0) // sub_len, n_sub - 1)
        return slot, head, key_chip, half, s_lo // RUNS

    counts, ends, n_taken = [], [], []
    total = jnp.int32(0)
    for head in range(n_kv):
        base, taken = total, []
        for e in range(n_block):
            n = n_run - place(jnp.int32(e))[4]
            if e < n_early:
                fits = jnp.int32(1) if e < 2 else (total + n <= base + EARLY_ITEMS[min(head, 1)]).astype(jnp.int32)
                taken.append(fits * taken[-1] if e > 2 else fits)
                n = n * taken[-1]
            else:
                f = e - n_early
                i_early = 2 + 2 * (n_hop - 1 - f // 2) + f % 2
                if i_early < n_early:
                    n = n * (1 - taken[i_early])
            total = total + n
            counts.append(n)
            ends.append(total)
        n_taken.append(sum(taken[1:], taken[0]))

    def following(at):
        i, e, j, n = at
        over = j + 1 >= n
        head, b = e // n_block, lax.rem(e, n_block) + 1
        limit = n_taken[0]
        for h in range(1, n_kv):
            limit = jnp.where(head == h, n_taken[h], limit)
        b = jnp.where(b == limit, n_early, b)
        f = b - n_early
        gone = lambda f: (f >= 0) & (2 + 2 * (n_hop - 1 - f // 2) + f % 2 < limit)
        b = jnp.where(gone(f), jnp.where((f % 2 == 1) | gone(f + 1), n_block, b + 1), b)
        e1 = jnp.minimum(head * n_block + b, n_kv * n_block - 1)
        e, j = jnp.where(over, e1, e), jnp.where(over, 0, j + 1)
        slot, head, key_chip, half, s_lo = place(e)
        i = i + 1
        return (slot, head, (s_lo + j) * RUNS, key_chip, half, (i < total).astype(jnp.int32)), (i, e, j, n_run - s_lo)

    exp_scale = scale * math.log2(math.e)
    k_iota = lax.broadcasted_iota(jnp.int32, (key_tile, width), 0)
    col = lax.broadcasted_iota(jnp.int32, (1, width), 1)
    q_off = sub_start + jnp.where(col < rows, me, sibling) * local_len + lax.rem(col, rows) // group

    def one(now, carry):
        (slot_p, head_p, s_p), (slot, head, s, key_chip, half, live), at = carry
        then, at = following(at)
        k, v = kvb[slot, head, :, :head_dim], kvb[slot, head, :, head_dim:]
        s_t = [jnp.dot(k, qt[head, s + r], preferred_element_type=F32) for r in range(RUNS)]
        dp_t = [jnp.dot(v, dot[head, s + r], preferred_element_type=F32) for r in range(RUNS)]
        p_p, ds_p = pbuf[1 - now], dsbuf[1 - now]
        q_p = qn[head_p, pl.ds(s_p, RUNS)].reshape(RUNS * width, head_dim)
        do_p = don[head_p, pl.ds(s_p, RUNS)].reshape(RUNS * width, head_dim)
        acc[slot_p, head_p, :, head_dim:] += jnp.dot(p_p, do_p, preferred_element_type=F32)
        acc[slot_p, head_p, :, :head_dim] += jnp.dot(ds_p, q_p, preferred_element_type=F32)
        k_t = kvb[slot_p, head_p, :, :head_dim].T
        for r in range(RUNS):
            dqa[head_p, s_p + r] += jnp.dot(k_t, ds_p[:, r * width:(r + 1) * width], preferred_element_type=F32)
        docs_k = key_doc[key_chip, pl.ds(pl.multiple_of(half * key_tile, 8), key_tile), :]
        docs_k = jnp.concatenate([docs_k] * (width // LANES), axis=1)
        pos0 = (key_chip * CORES + core) * keys_local + half * key_tile
        for r in range(RUNS):
            lse_r, delta_r, doc_r = [lines[head, s + r, m:m + 1, :] for m in range(3)]
            last = jnp.where(live == 1, q_off + (s + r) * sub_len - pos0, -1)
            ok = (docs_k == doc_r.astype(jnp.int32)) & (k_iota <= last)
            p = jnp.where(ok, jnp.exp2(s_t[r] * exp_scale - lse_r), 0.0)
            pbuf[now, :, r * width:(r + 1) * width] = p.astype(BF16)
            dsbuf[now, :, r * width:(r + 1) * width] = (p * (dp_t[r] - delta_r)).astype(BF16)
        return (slot, head, s), then, at

    def advance(state, target):
        i, carry = state
        m = jnp.maximum(target - i, 0) // UNROLL

        def step(_, carry):
            for u in range(UNROLL):
                carry = one(u % 2, carry)
            return carry

        return i + m * UNROLL, lax.fori_loop(0, m, step, carry)

    def end_of(e):
        out = jnp.int32(0)
        for v, n in enumerate(counts):
            out = out + jnp.where(e >= v, n, 0)
        return out

    def add(dst, src, head):
        cut = key_tile // 4

        @pl.loop(0, 4)
        def _(i):
            r = pl.ds(pl.multiple_of(i * cut, 8), cut)
            acc[dst, head, r, :] += rsb[src, head, r, :]

    def partial(i, head, peer):
        return remote(acc.at[i, head], rsb.at[i, head], rs_send.at[i, head], rs_recv.at[i, head], peer)

    def send_sums(k, way, head, state=None):
        i = way * n_hop + k
        peer = jnp.where(way == 0, left, right)
        if state is not None:
            state = advance(state, end_of(head * n_block + n_early + 2 * (n_hop - 1 - k) + way) + UNROLL)

        @pl.when(k + 2 < n_hop)
        def _():
            partial(i + 2, head, peer).wait_recv()
            add(i, i + 2, head)

        partial(i, head, peer).start()
        return state

    def arrive(k, state):
        goal = (EARLY_ITEMS[0] * k) // (n_hop - 1)
        state = advance(state, jnp.minimum(goal, end_of(jnp.minimum(2 * k + 1, n_early - 1))))
        pass_on(k, 0)

        @pl.when(k == max(n_hop - 3, 1))
        def _():
            gather_own(1)
        return state

    def both(head):
        def trip(m, state):
            state = lax.fori_loop(0, 2, lambda way, state: send_sums(n_hop - 1 - m, way, head, state), state)
            base = ends[(head + 1) * n_block - 1]
            goal = jnp.minimum(base + (EARLY_ITEMS[1] * (m + 1)) // n_hop, end_of((head + 1) * n_block + jnp.minimum(2 * m + 1, n_early - 1)))
            state = advance(state, jnp.where(state[0] >= base, goal, state[0]))
            pass_on(m, head + 1)
            if head + 2 < n_kv:
                @pl.when(m == max(n_hop - 3, 1))
                def _():
                    gather_own(head + 2)
            return state
        return trip

    def settle(head):
        for k in (1, 0):
            for way in range(2):
                partial(way * n_hop + k, head, nbr[1 - way]).wait_recv()
                add(own + (k + way) % 2, way * n_hop + k, head)

        @pl.loop(0, 2)
        def _(half):
            r = pl.ds(pl.multiple_of(half * key_tile, 8), key_tile)
            dko[r, head, :] = acc[own + half, head, :, :head_dim]
            dvo[r, head, :] = acc[own + half, head, :, head_dim:]

    zero = jnp.int32(0)
    start, at = following((zero - 1, zero, zero - 1, zero + 1))
    state = (zero, (start[:3], start, at))
    state = lax.fori_loop(1, n_hop, arrive, state)
    for head in range(n_kv - 1):
        state = lax.fori_loop(0, n_hop, both(head), state)
    state = lax.fori_loop(0, 2 * n_hop - 4, lambda m, state: send_sums(n_hop - 1 - m // 2, m % 2, n_kv - 1, state), state)
    state = advance(state, total + UNROLL)
    half_rows = lambda which: dqa.at[:, :, :, pl.ds(which * rows, rows)]
    swap = remote(half_rows(1), dqr, x_send.at[3], x_recv.at[3], sibling)
    swap.start()
    for way in range(2):
        send_sums(1, way, n_kv - 1)
    swap.wait_recv()

    @pl.loop(0, n_sub)
    def _(s):
        for h in range(n_kv):
            x = (dqa[h, s, :, :rows] + dqr[h, s]).T
            dqo[s, :, h] = x.reshape(local_len, group, head_dim)

    puts = [pltpu.make_async_copy(a, b, out_sem.at[i]) for i, (a, b) in enumerate(((dqo, dq_out), (dko, dk_out), (dvo, dv_out)))]
    puts[0].start()
    for head in range(n_kv - 1):
        settle(head)
    for way in range(2):
        send_sums(0, way, n_kv - 1)
    settle(n_kv - 1)
    puts[1].start()
    puts[2].start()
    swap.wait_send()
    for way in range(2):
        for k in range(n_hop):
            for head in range(n_kv):
                gather(way, k, head).wait_send()
                partial(way * n_hop + k, head, nbr[1 - way]).wait_send()
    for c in puts:
        c.wait()


def solution(mesh):
    cp_size = mesh.shape['cp']
    q_spec = P(None, 'cp', 'tp', None)
    lse_spec = P(None, 'cp', 'tp')
    kv_spec = P('cp', 'tp', None)

    def local_backward(query, out_act, out_grad, row_lse, key_act, value_act, doc_ids):
        n_sub, local_len, n_heads, head_dim = query.shape
        keys_local, n_kv = key_act.shape[0], key_act.shape[1]
        group = n_heads // n_kv
        sub_start = keys_local * cp_size - n_sub * local_len * cp_size
        rows = local_len * group
        half = keys_local // 2
        n_chip = cp_size // CORES
        n_hop = n_chip - 1
        n_slot = 2 * n_hop + 2
        q5 = (n_sub, local_len, n_kv, group, head_dim)
        cut = lambda x: jnp.transpose(x.reshape(2, half, n_kv, head_dim), (0, 2, 1, 3))
        scale = head_dim ** -0.5
        flops = 2 * 5 * n_kv * n_sub * 2 * rows * head_dim * keys_local * n_hop
        hbm = pl.BlockSpec(memory_space=pl.ANY)
        dma = pltpu.SemaphoreType.DMA
        vmem = pltpu.VMEM
        dq, dk, dv = pl.pallas_call(
            functools.partial(ring_kernel, cp_size, sub_start, scale),
            name='ring_backward',
            out_shape=(jax.ShapeDtypeStruct(q5, F32),) + (jax.ShapeDtypeStruct(key_act.shape, F32),) * 2,
            in_specs=[hbm] * 7,
            out_specs=(hbm,) * 3,
            scratch_shapes=[
                vmem((n_slot, n_kv, half, 2 * head_dim), BF16),
                vmem((n_slot, n_kv, half, 2 * head_dim), F32),
                vmem((2 * n_hop, n_kv, half, 2 * head_dim), F32),
                vmem((CORES,) + q5, BF16),
                vmem((CORES,) + q5, BF16),
                vmem(q5, BF16),
                vmem((n_sub, n_heads, local_len), F32),
                vmem((doc_ids.shape[0] // LANES, LANES), jnp.int32),
                vmem((n_kv, n_sub, CORES * rows, head_dim), BF16),
                vmem((n_kv, n_sub, head_dim, CORES * rows), BF16),
                vmem((n_kv, n_sub, CORES * rows, head_dim), BF16),
                vmem((n_kv, n_sub, head_dim, CORES * rows), BF16),
                vmem((n_kv, n_sub, 8, CORES * rows), F32),
                vmem((n_chip, keys_local, LANES), jnp.int32),
                vmem((n_kv, n_sub, head_dim, CORES * rows), F32),
                vmem((n_kv, n_sub, head_dim, rows), F32),
                vmem(q5, F32),
                vmem(key_act.shape, F32),
                vmem(key_act.shape, F32),
                vmem((2, half, RUNS * CORES * rows), BF16),
                vmem((2, half, RUNS * CORES * rows), BF16),
                dma((2 * n_hop, n_kv)), dma((2 * n_hop, n_kv)), dma((2 * n_hop, n_kv)), dma((2 * n_hop, n_kv)),
                dma((4,)), dma((4,)), dma((7,)), dma((3,)),
            ],
            compiler_params=pltpu.CompilerParams(collective_id=0, has_side_effects=True, vmem_limit_bytes=52 * 1024 * 1024),
            cost_estimate=pl.CostEstimate(flops=flops, bytes_accessed=30 * 2 ** 20, transcendentals=0),
        )(cut(key_act), cut(value_act), query.reshape(q5), out_act.reshape(q5), out_grad.reshape(q5), jnp.swapaxes(row_lse, 1, 2), doc_ids.reshape(-1, LANES))
        return (dq.reshape(query.shape) * scale).astype(BF16), dk * scale, dv

    return jax.shard_map(local_backward, mesh=mesh, in_specs=(q_spec, q_spec, q_spec, lse_spec, kv_spec, kv_spec, P()),
                         out_specs=(q_spec, kv_spec, kv_spec), check_vma=False)
```

```python
import functools
import math

import jax
import jax.numpy as jnp
from jax import lax
from jax.experimental import pallas as pl
from jax.experimental.pallas import tpu as pltpu
from jax.sharding import PartitionSpec as P

MESH = pl.DeviceIdType.MESH
CORES = 2
LANES = 128
RUNS = 2
UNROLL = 2
EARLY_ITEMS = (36, 40)
F32 = jnp.float32
BF16 = jnp.bfloat16


def ring_kernel(cp_size, sub_start, scale, k_in, v_in, q_in, o_in, do_in, lse_in, doc_in, dq_out, dk_out, dv_out,
                kvb, acc, rsb, raw_q, raw_do, raw_o, lse, docs, qn, qt, don, dot, lines, key_doc, dqa, dqr, dko, dvo, pbuf, dsbuf,
                ag_send, ag_recv, rs_send, rs_recv, x_send, x_recv, loc_sem, out_sem):
    n_chip = cp_size // CORES
    n_hop = n_chip - 1
    n_sub, local_len, n_kv, group, head_dim = q_in.shape
    rows = local_len * group
    width = CORES * rows
    key_tile = k_in.shape[2]
    span = local_len * CORES
    sub_len = local_len * cp_size
    keys_local = 2 * key_tile
    own = 2 * n_hop

    me = lax.axis_index('cp')
    chip, core = me // CORES, lax.rem(me, CORES)
    right = lax.rem(me + CORES, cp_size)
    left = lax.rem(me + cp_size - CORES, cp_size)
    sibling = me + 1 - 2 * core
    nbr = (right, left)

    barrier = pltpu.get_barrier_semaphore()
    for peer in (right, left, sibling):
        pl.semaphore_signal(barrier, inc=1, device_id={'cp': peer}, device_id_type=MESH)
    pl.semaphore_wait(barrier, 3)

    def remote(src, dst, send, recv, peer):
        return pltpu.make_async_remote_copy(src_ref=src, dst_ref=dst, send_sem=send, recv_sem=recv,
                                            device_id={'cp': peer}, device_id_type=MESH)

    def gather(way, k, head, src=None):
        i = way * n_hop + k
        return remote(kvb.at[i, head] if src is None else src, kvb.at[i, head], ag_send.at[i, head], ag_recv.at[i, head], nbr[way])

    def sides(ref):
        return (ref.at[:, pl.ds(0, head_dim)], ref.at[:, pl.ds(head_dim, head_dim)])

    def gather_own(head):
        for j in range(2):
            for way in range(2):
                i = way * n_hop + j
                for src, dst in zip((k_in, v_in), sides(kvb.at[i, head])):
                    remote(src.at[(j + way) % 2, head], dst, ag_send.at[i, head], ag_recv.at[i, head], nbr[way]).start()

    def pass_on(k, head):
        for way in range(2):
            gather(way, k, head).wait_recv()
            i = way * n_hop + k

            @pl.when(k + 2 < n_hop)
            def _():
                gather(way, k + 2, head, kvb.at[i, head]).start()

    gather_own(0)
    share = [remote(q_in, raw_q.at[1], x_send.at[0], x_recv.at[0], sibling),
             remote(do_in, raw_do.at[1], x_send.at[1], x_recv.at[1], sibling)]
    local = [pltpu.make_async_copy(a, b, loc_sem.at[i]) for i, (a, b) in enumerate((
        (doc_in, docs), (lse_in, lse), (do_in, raw_do.at[0]), (o_in, raw_o), (q_in, raw_q.at[0]),
        (k_in, kvb.at[pl.ds(own, 2), :, :, pl.ds(0, head_dim)]), (v_in, kvb.at[pl.ds(own, 2), :, :, pl.ds(head_dim, head_dim)])))]
    for c in local + share:
        c.start()

    def mine(which):
        return lines.at[:, :, :, pl.ds(which * rows, rows)]

    share_lines = remote(mine(0), mine(1), x_send.at[2], x_recv.at[2], sibling)

    @pl.loop(0, n_sub)
    def _(s):
        for h in range(n_kv):
            dqa[h, s] = jnp.zeros(dqa.shape[2:], F32)

    @pl.loop(0, acc.shape[0])
    def _(i):
        for h in range(n_kv):
            acc[i, h] = jnp.zeros(acc.shape[2:], F32)

    pbuf[...] = jnp.zeros(pbuf.shape, BF16)
    dsbuf[...] = jnp.zeros(dsbuf.shape, BF16)
    local[0].wait()
    tiles = keys_local // LANES

    @pl.loop(0, n_chip * tiles)
    def _(i):
        b, r = i // tiles, lax.rem(i, tiles)
        row = (b * CORES + core) * tiles + r
        key_doc[b, pl.ds(pl.multiple_of(r * LANES, LANES), LANES), :] = jnp.broadcast_to(docs[pl.ds(row, 1), :], (LANES, LANES)).T

    lane = lax.broadcasted_iota(jnp.int32, (8, rows), 1)
    sub = lax.broadcasted_iota(jnp.int32, (8, rows), 0)
    for c in local[1:4]:
        c.wait()

    @pl.loop(0, n_sub)
    def _(s):
        rep = jnp.concatenate([lse[s]] * (LANES // local_len), axis=1)
        wide = jnp.take_along_axis(rep, lane // group, axis=1)
        for h in range(n_kv):
            line = jnp.sum(jnp.where(sub - group * h == lane % group, wide, 0.0), axis=0, keepdims=True) * math.log2(math.e)
            prod = raw_do[0, s, :, h].reshape(rows, head_dim).astype(F32) * raw_o[s, :, h].reshape(rows, head_dim).astype(F32)
            total = jnp.broadcast_to(jnp.sum(prod, axis=1, keepdims=True), (rows, LANES)).T
            first = sub_start + s * sub_len + me * local_len
            doc_row = jnp.broadcast_to(docs[pl.ds(first // LANES, 1), :], (8, LANES))
            doc = jnp.take_along_axis(doc_row, lax.rem(first, LANES) + lane // group, axis=1).astype(F32)
            lines[h, s, :, :rows] = jnp.where(sub == 0, line, jnp.where(sub == 1, total[:8, :], doc))

    share_lines.start()

    def spread(c):
        @pl.loop(0, n_sub)
        def _(s):
            for h in range(n_kv):
                for raw, nat, tr in ((raw_q, qn, qt), (raw_do, don, dot)):
                    x = raw[c, s, :, h].reshape(rows, head_dim)
                    nat[h, s, c * rows:(c + 1) * rows, :] = x
                    tr[h, s, :, c * rows:(c + 1) * rows] = x.T

    for c in local[4:]:
        c.wait()
    spread(0)
    pass_on(0, 0)
    for c in share:
        c.wait()
    spread(1)
    share_lines.wait()

    n_run = n_sub // RUNS
    n_early = 2 + min(8, 2 * n_hop)
    n_block = n_early + 2 * n_hop

    def place(e):
        head, e = e // n_block, lax.rem(e, n_block)
        early = e < n_early
        f = jnp.where(early, e - 2, e - n_early)
        k = jnp.where(early, f // 2, n_hop - 1 - f // 2)
        way = f % 2
        mine = e < 2
        slot = jnp.where(mine, own + e, way * n_hop + k)
        half = jnp.where(mine, e, (k + way) % 2)
        hop = k // 2 + 1
        key_chip = jnp.where(mine, chip, lax.rem(chip + jnp.where(way == 1, hop, n_chip - hop), n_chip))
        pos0 = (key_chip * CORES + core) * keys_local + half * key_tile
        s_lo = jnp.minimum(jnp.maximum(pos0 - sub_start - span * chip - span + sub_len, 0) // sub_len, n_sub - 1)
        return slot, head, key_chip, half, s_lo // RUNS

    counts, ends, n_taken = [], [], []
    total = jnp.int32(0)
    for head in range(n_kv):
        base, taken = total, []
        for e in range(n_block):
            n = n_run - place(jnp.int32(e))[4]
            if e < n_early:
                fits = jnp.int32(1) if e < 2 else (total + n <= base + EARLY_ITEMS[min(head, 1)]).astype(jnp.int32)
                taken.append(fits * taken[-1] if e > 2 else fits)
                n = n * taken[-1]
            else:
                f = e - n_early
                i_early = 2 + 2 * (n_hop - 1 - f // 2) + f % 2
                if i_early < n_early:
                    n = n * (1 - taken[i_early])
            total = total + n
            counts.append(n)
            ends.append(total)
        n_taken.append(sum(taken[1:], taken[0]))

    def following(at):
        i, e, j, n = at
        over = j + 1 >= n
        head, b = e // n_block, lax.rem(e, n_block) + 1
        limit = n_taken[0]
        for h in range(1, n_kv):
            limit = jnp.where(head == h, n_taken[h], limit)
        b = jnp.where(b == limit, n_early, b)
        f = b - n_early
        gone = lambda f: (f >= 0) & (2 + 2 * (n_hop - 1 - f // 2) + f % 2 < limit)
        b = jnp.where(gone(f), jnp.where((f % 2 == 1) | gone(f + 1), n_block, b + 1), b)
        e1 = jnp.minimum(head * n_block + b, n_kv * n_block - 1)
        e, j = jnp.where(over, e1, e), jnp.where(over, 0, j + 1)
        slot, head, key_chip, half, s_lo = place(e)
        i = i + 1
        return (slot, head, (s_lo + j) * RUNS, key_chip, half, (i < total).astype(jnp.int32)), (i, e, j, n_run - s_lo)

    exp_scale = scale * math.log2(math.e)
    k_iota = lax.broadcasted_iota(jnp.int32, (key_tile, width), 0)
    col = lax.broadcasted_iota(jnp.int32, (1, width), 1)
    q_off = sub_start + jnp.where(col < rows, me, sibling) * local_len + lax.rem(col, rows) // group

    def one(now, carry):
        (slot_p, head_p, s_p), (slot, head, s, key_chip, half, live), at = carry
        then, at = following(at)
        k, v = kvb[slot, head, :, :head_dim], kvb[slot, head, :, head_dim:]
        s_t = [jnp.dot(k, qt[head, s + r], preferred_element_type=F32) for r in range(RUNS)]
        dp_t = [jnp.dot(v, dot[head, s + r], preferred_element_type=F32) for r in range(RUNS)]
        p_p, ds_p = pbuf[1 - now], dsbuf[1 - now]
        q_p = qn[head_p, pl.ds(s_p, RUNS)].reshape(RUNS * width, head_dim)
        do_p = don[head_p, pl.ds(s_p, RUNS)].reshape(RUNS * width, head_dim)
        acc[slot_p, head_p, :, head_dim:] += jnp.dot(p_p, do_p, preferred_element_type=F32)
        acc[slot_p, head_p, :, :head_dim] += jnp.dot(ds_p, q_p, preferred_element_type=F32)
        k_t = kvb[slot_p, head_p, :, :head_dim].T
        for r in range(RUNS):
            dqa[head_p, s_p + r] += jnp.dot(k_t, ds_p[:, r * width:(r + 1) * width], preferred_element_type=F32)
        docs_k = key_doc[key_chip, pl.ds(pl.multiple_of(half * key_tile, 8), key_tile), :]
        docs_k = jnp.concatenate([docs_k] * (width // LANES), axis=1)
        pos0 = (key_chip * CORES + core) * keys_local + half * key_tile
        for r in range(RUNS):
            lse_r, delta_r, doc_r = [lines[head, s + r, m:m + 1, :] for m in range(3)]
            last = jnp.where(live == 1, q_off + (s + r) * sub_len - pos0, -1)
            ok = (docs_k == doc_r.astype(jnp.int32)) & (k_iota <= last)
            p = jnp.where(ok, jnp.exp2(s_t[r] * exp_scale - lse_r), 0.0)
            pbuf[now, :, r * width:(r + 1) * width] = p.astype(BF16)
            dsbuf[now, :, r * width:(r + 1) * width] = (p * (dp_t[r] - delta_r)).astype(BF16)
        return (slot, head, s), then, at

    def advance(state, target):
        i, carry = state
        m = jnp.maximum(target - i, 0) // UNROLL

        def step(_, carry):
            for u in range(UNROLL):
                carry = one(u % 2, carry)
            return carry

        return i + m * UNROLL, lax.fori_loop(0, m, step, carry)

    def end_of(e):
        out = jnp.int32(0)
        for v, n in enumerate(counts):
            out = out + jnp.where(e >= v, n, 0)
        return out

    def add(dst, src, head):
        cut = key_tile // 4

        @pl.loop(0, 4)
        def _(i):
            r = pl.ds(pl.multiple_of(i * cut, 8), cut)
            acc[dst, head, r, :] += rsb[src, head, r, :]

    def partial(i, head, peer):
        return remote(acc.at[i, head], rsb.at[i, head], rs_send.at[i, head], rs_recv.at[i, head], peer)

    def send_sums(k, way, head, state=None):
        i = way * n_hop + k
        peer = jnp.where(way == 0, left, right)
        if state is not None:
            state = advance(state, end_of(head * n_block + n_early + 2 * (n_hop - 1 - k) + way) + UNROLL)

        @pl.when(k + 2 < n_hop)
        def _():
            partial(i + 2, head, peer).wait_recv()
            add(i, i + 2, head)

        partial(i, head, peer).start()
        return state

    def arrive(k, state):
        goal = (EARLY_ITEMS[0] * k) // (n_hop - 1)
        state = advance(state, jnp.minimum(goal, end_of(jnp.minimum(2 * k + 1, n_early - 1))))
        pass_on(k, 0)

        @pl.when(k == max(n_hop - 3, 1))
        def _():
            gather_own(1)
        return state

    def both(head):
        def trip(m, state):
            state = lax.fori_loop(0, 2, lambda way, state: send_sums(n_hop - 1 - m, way, head, state), state)
            base = ends[(head + 1) * n_block - 1]
            goal = jnp.minimum(base + (EARLY_ITEMS[1] * (m + 1)) // n_hop, end_of((head + 1) * n_block + jnp.minimum(2 * m + 1, n_early - 1)))
            state = advance(state, jnp.where(state[0] >= base, goal, state[0]))
            pass_on(m, head + 1)
            if head + 2 < n_kv:
                @pl.when(m == max(n_hop - 3, 1))
                def _():
                    gather_own(head + 2)
            return state
        return trip

    def settle(head):
        for k in (1, 0):
            for way in range(2):
                partial(way * n_hop + k, head, nbr[1 - way]).wait_recv()
                add(own + (k + way) % 2, way * n_hop + k, head)

        @pl.loop(0, 2)
        def _(half):
            r = pl.ds(pl.multiple_of(half * key_tile, 8), key_tile)
            dko[r, head, :] = acc[own + half, head, :, :head_dim] * scale
            dvo[r, head, :] = acc[own + half, head, :, head_dim:]

    zero = jnp.int32(0)
    start, at = following((zero - 1, zero, zero - 1, zero + 1))
    state = (zero, (start[:3], start, at))
    state = lax.fori_loop(1, n_hop, arrive, state)
    for head in range(n_kv - 1):
        state = lax.fori_loop(0, n_hop, both(head), state)
    state = lax.fori_loop(0, 2 * n_hop - 4, lambda m, state: send_sums(n_hop - 1 - m // 2, m % 2, n_kv - 1, state), state)
    state = advance(state, total + UNROLL)
    half_rows = lambda which: dqa.at[:, :, :, pl.ds(which * rows, rows)]
    swap = remote(half_rows(1), dqr, x_send.at[3], x_recv.at[3], sibling)
    swap.start()
    for way in range(2):
        send_sums(1, way, n_kv - 1)
    swap.wait_recv()

    @pl.loop(0, n_sub)
    def _(s):
        for h in range(n_kv):
            x = ((dqa[h, s, :, :rows] + dqr[h, s]) * scale).astype(BF16).T
            raw_q[0, s, :, h] = x.reshape(local_len, group, head_dim)

    puts = [pltpu.make_async_copy(a, b, out_sem.at[i]) for i, (a, b) in enumerate(((raw_q.at[0], dq_out), (dko, dk_out), (dvo, dv_out)))]
    puts[0].start()
    for head in range(n_kv - 1):
        settle(head)
    for way in range(2):
        send_sums(0, way, n_kv - 1)
    settle(n_kv - 1)
    puts[1].start()
    puts[2].start()
    swap.wait_send()
    for way in range(2):
        for k in range(n_hop):
            for head in range(n_kv):
                gather(way, k, head).wait_send()
                partial(way * n_hop + k, head, nbr[1 - way]).wait_send()
    for c in puts:
        c.wait()


def copy_kernel(a, b, c, a_out, b_out, c_out, a_buf, b_buf, c_buf, in_sem, out_sem):
    ins = [pltpu.make_async_copy(x, y, in_sem.at[i]) for i, (x, y) in enumerate(((a, a_buf), (b, b_buf), (c, c_buf)))]
    outs = [pltpu.make_async_copy(x, y, out_sem.at[i]) for i, (x, y) in enumerate(((a_buf, a_out), (b_buf, b_out), (c_buf, c_out)))]
    for x in ins:
        x.start()
    for x, y in zip(ins, outs):
        x.wait()
        y.start()
    for y in outs:
        y.wait()


def solution(mesh):
    cp_size = mesh.shape['cp']
    q_spec = P(None, 'cp', 'tp', None)
    lse_spec = P(None, 'cp', 'tp')
    kv_spec = P('cp', 'tp', None)

    def local_backward(query, out_act, out_grad, row_lse, key_act, value_act, doc_ids):
        n_sub, local_len, n_heads, head_dim = query.shape
        keys_local, n_kv = key_act.shape[0], key_act.shape[1]
        group = n_heads // n_kv
        sub_start = keys_local * cp_size - n_sub * local_len * cp_size
        rows = local_len * group
        half = keys_local // 2
        n_chip = cp_size // CORES
        n_hop = n_chip - 1
        n_slot = 2 * n_hop + 2
        q5 = (n_sub, local_len, n_kv, group, head_dim)
        cut = lambda x: jnp.transpose(x.reshape(2, half, n_kv, head_dim), (0, 2, 1, 3))
        scale = head_dim ** -0.5
        flops = 2 * 5 * n_kv * n_sub * 2 * rows * head_dim * keys_local * n_hop
        hbm = pl.BlockSpec(memory_space=pl.ANY)
        dma = pltpu.SemaphoreType.DMA
        vmem = pltpu.VMEM
        dq, dk, dv = pl.pallas_call(
            functools.partial(ring_kernel, cp_size, sub_start, scale),
            name='ring_backward',
            out_shape=(jax.ShapeDtypeStruct(q5, BF16),) + (jax.ShapeDtypeStruct(key_act.shape, F32),) * 2,
            in_specs=[hbm] * 7,
            out_specs=(hbm,) * 3,
            scratch_shapes=[
                vmem((n_slot, n_kv, half, 2 * head_dim), BF16),
                vmem((n_slot, n_kv, half, 2 * head_dim), F32),
                vmem((2 * n_hop, n_kv, half, 2 * head_dim), F32),
                vmem((CORES,) + q5, BF16),
                vmem((CORES,) + q5, BF16),
                vmem(q5, BF16),
                vmem((n_sub, n_heads, local_len), F32),
                vmem((doc_ids.shape[0] // LANES, LANES), jnp.int32),
                vmem((n_kv, n_sub, CORES * rows, head_dim), BF16),
                vmem((n_kv, n_sub, head_dim, CORES * rows), BF16),
                vmem((n_kv, n_sub, CORES * rows, head_dim), BF16),
                vmem((n_kv, n_sub, head_dim, CORES * rows), BF16),
                vmem((n_kv, n_sub, 8, CORES * rows), F32),
                vmem((n_chip, keys_local, LANES), jnp.int32),
                vmem((n_kv, n_sub, head_dim, CORES * rows), F32),
                vmem((n_kv, n_sub, head_dim, rows), F32),
                vmem(key_act.shape, F32),
                vmem(key_act.shape, F32),
                vmem((2, half, RUNS * CORES * rows), BF16),
                vmem((2, half, RUNS * CORES * rows), BF16),
                dma((2 * n_hop, n_kv)), dma((2 * n_hop, n_kv)), dma((2 * n_hop, n_kv)), dma((2 * n_hop, n_kv)),
                dma((4,)), dma((4,)), dma((7,)), dma((3,)),
            ],
            compiler_params=pltpu.CompilerParams(collective_id=0, has_side_effects=True, vmem_limit_bytes=62 * 1024 * 1024),
            cost_estimate=pl.CostEstimate(flops=flops, bytes_accessed=30 * 2 ** 20, transcendentals=0),
        )(cut(key_act), cut(value_act), query.reshape(q5), out_act.reshape(q5), out_grad.reshape(q5), jnp.swapaxes(row_lse, 1, 2), doc_ids.reshape(-1, LANES))
        dq, dk, dv = pl.pallas_call(
            copy_kernel,
            name='results',
            out_shape=tuple(jax.ShapeDtypeStruct(x.shape, x.dtype) for x in (dq, dk, dv)),
            in_specs=[hbm] * 3,
            out_specs=(hbm,) * 3,
            scratch_shapes=[vmem(x.shape, x.dtype) for x in (dq, dk, dv)] + [dma((3,)), dma((3,))],
            cost_estimate=pl.CostEstimate(flops=0, bytes_accessed=2 ** 22, transcendentals=0),
        )(dq, dk, dv)
        return dq.reshape(query.shape), dk, dv

    return jax.shard_map(local_backward, mesh=mesh, in_specs=(q_spec, q_spec, q_spec, lse_spec, kv_spec, kv_spec, P()),
                         out_specs=(q_spec, kv_spec, kv_spec), check_vma=False)
```

```python
import functools
import math

import jax
import jax.numpy as jnp
from jax import lax
from jax.experimental import pallas as pl
from jax.experimental.pallas import tpu as pltpu
from jax.sharding import PartitionSpec as P

MESH = pl.DeviceIdType.MESH
CORES = 2
LANES = 128
SPLIT = 64
RUNS = 2
UNROLL = 2
EARLY_ITEMS = (26, 20)
F32 = jnp.float32
BF16 = jnp.bfloat16


def ring_kernel(cp_size, sub_start, scale, k_in, v_in, q_in, o_in, do_in, lse_in, doc_in, dq_out, dk_out, dv_out,
                kvb, acc, rsb, raw_q, raw_do, raw_o, lse, docs, qn, qt, don, dot, lines, key_doc, dqa, dqr, dko, dvo, pbuf, dsbuf, raw_kv,
                ag_send, ag_recv, rs_send, rs_recv, x_send, x_recv, loc_sem, out_sem):
    n_chip = cp_size // CORES
    n_hop = n_chip - 1
    n_sub, local_len, n_kv, group, head_dim = q_in.shape
    rows = local_len * group
    width = CORES * rows
    key_tile = k_in.shape[0] // 2
    span = local_len * CORES
    sub_len = local_len * cp_size
    keys_local = 2 * key_tile
    own = 2 * n_hop

    me = lax.axis_index('cp')
    chip, core = me // CORES, lax.rem(me, CORES)
    right = lax.rem(me + CORES, cp_size)
    left = lax.rem(me + cp_size - CORES, cp_size)
    sibling = me + 1 - 2 * core
    nbr = (right, left)

    barrier = pltpu.get_barrier_semaphore()
    for peer in (right, left, sibling):
        pl.semaphore_signal(barrier, inc=1, device_id={'cp': peer}, device_id_type=MESH)

    own_kv = [pltpu.make_async_copy(x, raw_kv.at[i], loc_sem.at[5 + i]) for i, x in enumerate((k_in, v_in))]
    local = [pltpu.make_async_copy(a, b, loc_sem.at[i]) for i, (a, b) in enumerate((
        (doc_in, docs), (lse_in, lse), (do_in, raw_do.at[0]), (o_in, raw_o), (q_in, raw_q.at[0])))]
    for c in own_kv + local:
        c.start()

    @pl.loop(0, n_sub)
    def _(s):
        for h in range(n_kv):
            dqa[h, s] = jnp.zeros(dqa.shape[2:], F32)

    for c in own_kv:
        c.wait()
    for half in range(2):
        @pl.loop(0, key_tile // SPLIT)
        def _(i):
            r = pl.multiple_of(i * SPLIT, SPLIT)
            for part in range(2):
                x = raw_kv[part, pl.ds(half * key_tile + r, SPLIT)].astype(F32)
                for h in range(n_kv):
                    kvb[own + half, h, pl.ds(r, SPLIT), part * head_dim:(part + 1) * head_dim] = x[:, h].astype(BF16)

    pl.semaphore_wait(barrier, 3)

    def remote(src, dst, send, recv, peer):
        return pltpu.make_async_remote_copy(src_ref=src, dst_ref=dst, send_sem=send, recv_sem=recv,
                                            device_id={'cp': peer}, device_id_type=MESH)

    def gather(way, k, head, src=None):
        i = way * n_hop + k
        return remote(kvb.at[i, head] if src is None else src, kvb.at[i, head], ag_send.at[i, head], ag_recv.at[i, head], nbr[way])

    def gather_own(head):
        for j in range(2):
            for way in range(2):
                gather(way, j, head, kvb.at[own + (j + way) % 2, head]).start()

    def pass_on(k, head):
        for way in range(2):
            gather(way, k, head).wait_recv()
            i = way * n_hop + k

            @pl.when(k + 2 < n_hop)
            def _():
                gather(way, k + 2, head, kvb.at[i, head]).start()

    gather_own(0)
    share = [remote(q_in, raw_q.at[1], x_send.at[0], x_recv.at[0], sibling),
             remote(do_in, raw_do.at[1], x_send.at[1], x_recv.at[1], sibling)]
    for c in share:
        c.start()

    def mine(which):
        return lines.at[:, :, :, pl.ds(which * rows, rows)]

    share_lines = remote(mine(0), mine(1), x_send.at[2], x_recv.at[2], sibling)

    @pl.loop(0, acc.shape[0])
    def _(i):
        for h in range(n_kv):
            acc[i, h] = jnp.zeros(acc.shape[2:], F32)

    pbuf[...] = jnp.zeros(pbuf.shape, BF16)
    dsbuf[...] = jnp.zeros(dsbuf.shape, BF16)
    local[0].wait()
    tiles = keys_local // LANES

    @pl.loop(0, n_chip * tiles)
    def _(i):
        b, r = i // tiles, lax.rem(i, tiles)
        row = (b * CORES + core) * tiles + r
        key_doc[b, pl.ds(pl.multiple_of(r * LANES, LANES), LANES), :] = jnp.broadcast_to(docs[pl.ds(row, 1), :], (LANES, LANES)).T

    lane = lax.broadcasted_iota(jnp.int32, (8, rows), 1)
    sub = lax.broadcasted_iota(jnp.int32, (8, rows), 0)
    for c in local[1:4]:
        c.wait()

    @pl.loop(0, n_sub)
    def _(s):
        rep = jnp.concatenate([lse[s]] * (LANES // local_len), axis=1)
        wide = jnp.take_along_axis(rep, lane // group, axis=1)
        for h in range(n_kv):
            line = jnp.sum(jnp.where(sub - group * h == lane % group, wide, 0.0), axis=0, keepdims=True) * math.log2(math.e)
            prod = raw_do[0, s, :, h].reshape(rows, head_dim).astype(F32) * raw_o[s, :, h].reshape(rows, head_dim).astype(F32)
            total = jnp.broadcast_to(jnp.sum(prod, axis=1, keepdims=True), (rows, LANES)).T
            first = sub_start + s * sub_len + me * local_len
            doc_row = jnp.broadcast_to(docs[pl.ds(first // LANES, 1), :], (8, LANES))
            doc = jnp.take_along_axis(doc_row, lax.rem(first, LANES) + lane // group, axis=1).astype(F32)
            lines[h, s, :, :rows] = jnp.where(sub == 0, line, jnp.where(sub == 1, total[:8, :], doc))

    share_lines.start()

    def spread(c):
        @pl.loop(0, n_sub)
        def _(s):
            for h in range(n_kv):
                for raw, nat, tr in ((raw_q, qn, qt), (raw_do, don, dot)):
                    x = raw[c, s, :, h].reshape(rows, head_dim)
                    nat[h, s, c * rows:(c + 1) * rows, :] = x
                    tr[h, s, :, c * rows:(c + 1) * rows] = x.T

    for c in local[4:]:
        c.wait()
    spread(0)
    pass_on(0, 0)
    for c in share:
        c.wait()
    spread(1)
    share_lines.wait()

    n_run = n_sub // RUNS
    n_early = 2 + min(8, 2 * n_hop)
    n_block = n_early + 2 * n_hop

    def place(e):
        head, e = e // n_block, lax.rem(e, n_block)
        early = e < n_early
        f = jnp.where(early, e - 2, e - n_early)
        k = jnp.where(early, f // 2, n_hop - 1 - f // 2)
        way = f % 2
        mine = e < 2
        slot = jnp.where(mine, own + e, way * n_hop + k)
        half = jnp.where(mine, e, (k + way) % 2)
        hop = k // 2 + 1
        key_chip = jnp.where(mine, chip, lax.rem(chip + jnp.where(way == 1, hop, n_chip - hop), n_chip))
        pos0 = (key_chip * CORES + core) * keys_local + half * key_tile
        s_lo = jnp.minimum(jnp.maximum(pos0 - sub_start - span * chip - span + sub_len, 0) // sub_len, n_sub - 1)
        return slot, head, key_chip, half, s_lo // RUNS

    counts, ends, n_taken = [], [], []
    total = jnp.int32(0)
    for head in range(n_kv):
        base, taken = total, []
        for e in range(n_block):
            n = n_run - place(jnp.int32(e))[4]
            if e < n_early:
                fits = jnp.int32(1) if e < 2 else (total + n <= base + EARLY_ITEMS[min(head, 1)]).astype(jnp.int32)
                taken.append(fits * taken[-1] if e > 2 else fits)
                n = n * taken[-1]
            else:
                f = e - n_early
                i_early = 2 + 2 * (n_hop - 1 - f // 2) + f % 2
                if i_early < n_early:
                    n = n * (1 - taken[i_early])
            total = total + n
            counts.append(n)
            ends.append(total)
        n_taken.append(sum(taken[1:], taken[0]))

    def following(at):
        i, e, j, n = at
        over = j + 1 >= n
        head, b = e // n_block, lax.rem(e, n_block) + 1
        limit = n_taken[0]
        for h in range(1, n_kv):
            limit = jnp.where(head == h, n_taken[h], limit)
        b = jnp.where(b == limit, n_early, b)
        f = b - n_early
        gone = lambda f: (f >= 0) & (2 + 2 * (n_hop - 1 - f // 2) + f % 2 < limit)
        b = jnp.where(gone(f), jnp.where((f % 2 == 1) | gone(f + 1), n_block, b + 1), b)
        e1 = jnp.minimum(head * n_block + b, n_kv * n_block - 1)
        e, j = jnp.where(over, e1, e), jnp.where(over, 0, j + 1)
        slot, head, key_chip, half, s_lo = place(e)
        i = i + 1
        return (slot, head, (s_lo + j) * RUNS, key_chip, half, (i < total).astype(jnp.int32)), (i, e, j, n_run - s_lo)

    exp_scale = scale * math.log2(math.e)
    k_iota = lax.broadcasted_iota(jnp.int32, (key_tile, width), 0)
    col = lax.broadcasted_iota(jnp.int32, (1, width), 1)
    q_off = sub_start + jnp.where(col < rows, me, sibling) * local_len + lax.rem(col, rows) // group

    def one(now, carry):
        (slot_p, head_p, s_p), (slot, head, s, key_chip, half, live), at = carry
        then, at = following(at)
        k, v = kvb[slot, head, :, :head_dim], kvb[slot, head, :, head_dim:]
        s_t = [jnp.dot(k, qt[head, s + r], preferred_element_type=F32) for r in range(RUNS)]
        dp_t = [jnp.dot(v, dot[head, s + r], preferred_element_type=F32) for r in range(RUNS)]
        p_p, ds_p = pbuf[1 - now], dsbuf[1 - now]
        q_p = qn[head_p, pl.ds(s_p, RUNS)].reshape(RUNS * width, head_dim)
        do_p = don[head_p, pl.ds(s_p, RUNS)].reshape(RUNS * width, head_dim)
        acc[slot_p, head_p, :, head_dim:] += jnp.dot(p_p, do_p, preferred_element_type=F32)
        acc[slot_p, head_p, :, :head_dim] += jnp.dot(ds_p, q_p, preferred_element_type=F32)
        k_t = kvb[slot_p, head_p, :, :head_dim].T
        for r in range(RUNS):
            dqa[head_p, s_p + r] += jnp.dot(k_t, ds_p[:, r * width:(r + 1) * width], preferred_element_type=F32)
        docs_k = key_doc[key_chip, pl.ds(pl.multiple_of(half * key_tile, 8), key_tile), :]
        docs_k = jnp.concatenate([docs_k] * (width // LANES), axis=1)
        pos0 = (key_chip * CORES + core) * keys_local + half * key_tile
        for r in range(RUNS):
            lse_r, delta_r, doc_r = [lines[head, s + r, m:m + 1, :] for m in range(3)]
            last = jnp.where(live == 1, q_off + (s + r) * sub_len - pos0, -1)
            ok = (docs_k == doc_r.astype(jnp.int32)) & (k_iota <= last)
            p = jnp.where(ok, jnp.exp2(s_t[r] * exp_scale - lse_r), 0.0)
            pbuf[now, :, r * width:(r + 1) * width] = p.astype(BF16)
            dsbuf[now, :, r * width:(r + 1) * width] = (p * (dp_t[r] - delta_r)).astype(BF16)
        return (slot, head, s), then, at

    def advance(state, target):
        i, carry = state
        m = jnp.maximum(target - i, 0) // UNROLL

        def step(_, carry):
            for u in range(UNROLL):
                carry = one(u % 2, carry)
            return carry

        return i + m * UNROLL, lax.fori_loop(0, m, step, carry)

    def end_of(e):
        out = jnp.int32(0)
        for v, n in enumerate(counts):
            out = out + jnp.where(e >= v, n, 0)
        return out

    def add(dst, src, head):
        cut = key_tile // 4

        @pl.loop(0, 4)
        def _(i):
            r = pl.ds(pl.multiple_of(i * cut, 8), cut)
            acc[dst, head, r, :] += rsb[src, head, r, :]

    def partial(i, head, peer):
        return remote(acc.at[i, head], rsb.at[i, head], rs_send.at[i, head], rs_recv.at[i, head], peer)

    def send_sums(k, way, head, state=None):
        i = way * n_hop + k
        peer = jnp.where(way == 0, left, right)
        if state is not None:
            state = advance(state, end_of(head * n_block + n_early + 2 * (n_hop - 1 - k) + way) + UNROLL)

        @pl.when(k + 2 < n_hop)
        def _():
            partial(i + 2, head, peer).wait_recv()
            add(i, i + 2, head)

        partial(i, head, peer).start()
        return state

    def arrive(k, state):
        goal = (EARLY_ITEMS[0] * k) // (n_hop - 1)
        state = advance(state, jnp.minimum(goal, end_of(jnp.minimum(2 * k + 1, n_early - 1))))
        pass_on(k, 0)

        @pl.when(k == max(n_hop - 3, 1))
        def _():
            gather_own(1)
        return state

    def both(head):
        def trip(m, state):
            state = lax.fori_loop(0, 2, lambda way, state: send_sums(n_hop - 1 - m, way, head, state), state)
            base = ends[(head + 1) * n_block - 1]
            goal = jnp.minimum(base + (EARLY_ITEMS[1] * (m + 1)) // n_hop, end_of((head + 1) * n_block + jnp.minimum(2 * m + 1, n_early - 1)))
            state = advance(state, jnp.where(state[0] >= base, goal, state[0]))
            pass_on(m, head + 1)
            if head + 2 < n_kv:
                @pl.when(m == max(n_hop - 3, 1))
                def _():
                    gather_own(head + 2)
            return state
        return trip

    def settle(head):
        for k in (1, 0):
            for way in range(2):
                partial(way * n_hop + k, head, nbr[1 - way]).wait_recv()
                add(own + (k + way) % 2, way * n_hop + k, head)

        @pl.loop(0, 2)
        def _(half):
            r = pl.ds(pl.multiple_of(half * key_tile, 8), key_tile)
            dko[r, head, :] = acc[own + half, head, :, :head_dim] * scale
            dvo[r, head, :] = acc[own + half, head, :, head_dim:]

    zero = jnp.int32(0)
    start, at = following((zero - 1, zero, zero - 1, zero + 1))
    state = (zero, (start[:3], start, at))
    state = lax.fori_loop(1, n_hop, arrive, state)
    for head in range(n_kv - 1):
        state = lax.fori_loop(0, n_hop, both(head), state)
    state = lax.fori_loop(0, 2 * n_hop - 4, lambda m, state: send_sums(n_hop - 1 - m // 2, m % 2, n_kv - 1, state), state)
    state = advance(state, total + UNROLL)
    half_rows = lambda which: dqa.at[:, :, :, pl.ds(which * rows, rows)]
    swap = remote(half_rows(1), dqr, x_send.at[3], x_recv.at[3], sibling)
    swap.start()
    for way in range(2):
        send_sums(1, way, n_kv - 1)
    swap.wait_recv()

    @pl.loop(0, n_sub)
    def _(s):
        for h in range(n_kv):
            x = ((dqa[h, s, :, :rows] + dqr[h, s]) * scale).astype(BF16).T
            raw_q[0, s, :, h] = x.reshape(local_len, group, head_dim)

    puts = [pltpu.make_async_copy(a, b, out_sem.at[i]) for i, (a, b) in enumerate(((raw_q.at[0], dq_out), (dko, dk_out), (dvo, dv_out)))]
    puts[0].start()
    for head in range(n_kv - 1):
        settle(head)
    for way in range(2):
        send_sums(0, way, n_kv - 1)
    settle(n_kv - 1)
    puts[1].start()
    puts[2].start()
    swap.wait_send()
    for way in range(2):
        for k in range(n_hop):
            for head in range(n_kv):
                gather(way, k, head).wait_send()
                partial(way * n_hop + k, head, nbr[1 - way]).wait_send()
    for c in puts:
        c.wait()


def copy_kernel(a, b, c, a_out, b_out, c_out, a_buf, b_buf, c_buf, in_sem, out_sem):
    ins = [pltpu.make_async_copy(x, y, in_sem.at[i]) for i, (x, y) in enumerate(((a, a_buf), (b, b_buf), (c, c_buf)))]
    outs = [pltpu.make_async_copy(x, y, out_sem.at[i]) for i, (x, y) in enumerate(((a_buf, a_out), (b_buf, b_out), (c_buf, c_out)))]
    for x in ins:
        x.start()
    for x, y in zip(ins, outs):
        x.wait()
        y.start()
    for y in outs:
        y.wait()


def solution(mesh):
    cp_size = mesh.shape['cp']
    q_spec = P(None, 'cp', 'tp', None)
    lse_spec = P(None, 'cp', 'tp')
    kv_spec = P('cp', 'tp', None)

    def local_backward(query, out_act, out_grad, row_lse, key_act, value_act, doc_ids):
        n_sub, local_len, n_heads, head_dim = query.shape
        keys_local, n_kv = key_act.shape[0], key_act.shape[1]
        group = n_heads // n_kv
        sub_start = keys_local * cp_size - n_sub * local_len * cp_size
        rows = local_len * group
        half = keys_local // 2
        n_chip = cp_size // CORES
        n_hop = n_chip - 1
        n_slot = 2 * n_hop + 2
        q5 = (n_sub, local_len, n_kv, group, head_dim)
        scale = head_dim ** -0.5
        flops = 2 * 5 * n_kv * n_sub * 2 * rows * head_dim * keys_local * n_hop
        hbm = pl.BlockSpec(memory_space=pl.ANY)
        dma = pltpu.SemaphoreType.DMA
        vmem = pltpu.VMEM
        dq, dk, dv = pl.pallas_call(
            functools.partial(ring_kernel, cp_size, sub_start, scale),
            name='ring_backward',
            out_shape=(jax.ShapeDtypeStruct(q5, BF16),) + (jax.ShapeDtypeStruct(key_act.shape, F32),) * 2,
            in_specs=[hbm] * 7,
            out_specs=(hbm,) * 3,
            scratch_shapes=[
                vmem((n_slot, n_kv, half, 2 * head_dim), BF16),
                vmem((n_slot, n_kv, half, 2 * head_dim), F32),
                vmem((2 * n_hop, n_kv, half, 2 * head_dim), F32),
                vmem((CORES,) + q5, BF16),
                vmem((CORES,) + q5, BF16),
                vmem(q5, BF16),
                vmem((n_sub, n_heads, local_len), F32),
                vmem((doc_ids.shape[0] // LANES, LANES), jnp.int32),
                vmem((n_kv, n_sub, CORES * rows, head_dim), BF16),
                vmem((n_kv, n_sub, head_dim, CORES * rows), BF16),
                vmem((n_kv, n_sub, CORES * rows, head_dim), BF16),
                vmem((n_kv, n_sub, head_dim, CORES * rows), BF16),
                vmem((n_kv, n_sub, 8, CORES * rows), F32),
                vmem((n_chip, keys_local, LANES), jnp.int32),
                vmem((n_kv, n_sub, head_dim, CORES * rows), F32),
                vmem((n_kv, n_sub, head_dim, rows), F32),
                vmem(key_act.shape, F32),
                vmem(key_act.shape, F32),
                vmem((2, half, RUNS * CORES * rows), BF16),
                vmem((2, half, RUNS * CORES * rows), BF16),
                vmem((2,) + key_act.shape, BF16),
                dma((2 * n_hop, n_kv)), dma((2 * n_hop, n_kv)), dma((2 * n_hop, n_kv)), dma((2 * n_hop, n_kv)),
                dma((4,)), dma((4,)), dma((7,)), dma((3,)),
            ],
            compiler_params=pltpu.CompilerParams(collective_id=0, has_side_effects=True, vmem_limit_bytes=62 * 1024 * 1024),
            cost_estimate=pl.CostEstimate(flops=flops, bytes_accessed=30 * 2 ** 20, transcendentals=0),
        )(key_act, value_act, query.reshape(q5), out_act.reshape(q5), out_grad.reshape(q5), jnp.swapaxes(row_lse, 1, 2), doc_ids.reshape(-1, LANES))
        dq, dk, dv = pl.pallas_call(
            copy_kernel,
            name='results',
            out_shape=tuple(jax.ShapeDtypeStruct(x.shape, x.dtype) for x in (dq, dk, dv)),
            in_specs=[hbm] * 3,
            out_specs=(hbm,) * 3,
            scratch_shapes=[vmem(x.shape, x.dtype) for x in (dq, dk, dv)] + [dma((3,)), dma((3,))],
            cost_estimate=pl.CostEstimate(flops=0, bytes_accessed=2 ** 22, transcendentals=0),
        )(dq, dk, dv)
        return dq.reshape(query.shape), dk, dv

    return jax.shard_map(local_backward, mesh=mesh, in_specs=(q_spec, q_spec, q_spec, lse_spec, kv_spec, kv_spec, P()),
                         out_specs=(q_spec, kv_spec, kv_spec), check_vma=False)
```

```python
import functools
import math

import jax
import jax.numpy as jnp
from jax import lax
from jax.experimental import pallas as pl
from jax.experimental.pallas import tpu as pltpu
from jax.sharding import PartitionSpec as P

MESH = pl.DeviceIdType.MESH
CORES = 2
LANES = 128
SPLIT = 64
RUNS = 2
UNROLL = 2
EARLY_ITEMS = (26, 16)
F32 = jnp.float32
BF16 = jnp.bfloat16


def ring_kernel(cp_size, sub_start, scale, k_in, v_in, q_in, o_in, do_in, lse_in, doc_in, dq_out, dk_out, dv_out,
                kvb, acc, rsb, raw_q, raw_do, raw_o, lse, docs, qn, qt, don, dot, lines, key_doc, dqa, dqr, dko, dvo, pbuf, dsbuf, raw_kv,
                ag_send, ag_recv, rs_send, rs_recv, x_send, x_recv, loc_sem, out_sem):
    n_chip = cp_size // CORES
    n_hop = n_chip - 1
    n_sub, local_len, n_kv, group, head_dim = q_in.shape
    rows = local_len * group
    width = CORES * rows
    key_tile = k_in.shape[0] // 2
    span = local_len * CORES
    sub_len = local_len * cp_size
    keys_local = 2 * key_tile
    own = 2 * n_hop

    me = lax.axis_index('cp')
    chip, core = me // CORES, lax.rem(me, CORES)
    right = lax.rem(me + CORES, cp_size)
    left = lax.rem(me + cp_size - CORES, cp_size)
    sibling = me + 1 - 2 * core
    nbr = (right, left)

    barrier = pltpu.get_barrier_semaphore()
    for peer in (right, left, sibling):
        pl.semaphore_signal(barrier, inc=1, device_id={'cp': peer}, device_id_type=MESH)

    own_kv = [pltpu.make_async_copy(x, raw_kv.at[i], loc_sem.at[5 + i]) for i, x in enumerate((k_in, v_in))]
    local = [pltpu.make_async_copy(a, b, loc_sem.at[i]) for i, (a, b) in enumerate((
        (doc_in, docs), (lse_in, lse), (do_in, raw_do.at[0]), (o_in, raw_o), (q_in, raw_q.at[0])))]
    for c in own_kv + local:
        c.start()

    @pl.loop(0, n_sub)
    def _(s):
        for h in range(n_kv):
            dqa[h, s] = jnp.zeros(dqa.shape[2:], F32)

    for c in own_kv:
        c.wait()
    for half in range(2):
        @pl.loop(0, key_tile // SPLIT)
        def _(i):
            r = pl.multiple_of(i * SPLIT, SPLIT)
            for part in range(2):
                x = raw_kv[part, pl.ds(half * key_tile + r, SPLIT)].astype(F32)
                for h in range(n_kv):
                    kvb[own + half, h, pl.ds(r, SPLIT), part * head_dim:(part + 1) * head_dim] = x[:, h].astype(BF16)

    pl.semaphore_wait(barrier, 3)

    def remote(src, dst, send, recv, peer):
        return pltpu.make_async_remote_copy(src_ref=src, dst_ref=dst, send_sem=send, recv_sem=recv,
                                            device_id={'cp': peer}, device_id_type=MESH)

    def gather(way, k, head, src=None):
        i = way * n_hop + k
        return remote(kvb.at[i, head] if src is None else src, kvb.at[i, head], ag_send.at[i, head], ag_recv.at[i, head], nbr[way])

    def gather_own(head):
        for j in range(2):
            for way in range(2):
                gather(way, j, head, kvb.at[own + (j + way) % 2, head]).start()

    def pass_on(k, head):
        for way in range(2):
            gather(way, k, head).wait_recv()
            i = way * n_hop + k

            @pl.when(k + 2 < n_hop)
            def _():
                gather(way, k + 2, head, kvb.at[i, head]).start()

    gather_own(0)
    share = [remote(q_in, raw_q.at[1], x_send.at[0], x_recv.at[0], sibling),
             remote(do_in, raw_do.at[1], x_send.at[1], x_recv.at[1], sibling)]
    for c in share:
        c.start()

    def mine(which):
        return lines.at[:, :, :, pl.ds(which * rows, rows)]

    share_lines = remote(mine(0), mine(1), x_send.at[2], x_recv.at[2], sibling)

    @pl.loop(0, acc.shape[0])
    def _(i):
        for h in range(n_kv):
            acc[i, h] = jnp.zeros(acc.shape[2:], F32)

    pbuf[...] = jnp.zeros(pbuf.shape, BF16)
    dsbuf[...] = jnp.zeros(dsbuf.shape, BF16)
    local[0].wait()
    tiles = keys_local // LANES

    @pl.loop(0, n_chip * tiles)
    def _(i):
        b, r = i // tiles, lax.rem(i, tiles)
        row = (b * CORES + core) * tiles + r
        key_doc[b, pl.ds(pl.multiple_of(r * LANES, LANES), LANES), :] = jnp.broadcast_to(docs[pl.ds(row, 1), :], (LANES, LANES)).T

    lane = lax.broadcasted_iota(jnp.int32, (8, rows), 1)
    sub = lax.broadcasted_iota(jnp.int32, (8, rows), 0)
    for c in local[1:4]:
        c.wait()

    @pl.loop(0, n_sub)
    def _(s):
        rep = jnp.concatenate([lse[s]] * (LANES // local_len), axis=1)
        wide = jnp.take_along_axis(rep, lane // group, axis=1)
        for h in range(n_kv):
            line = jnp.sum(jnp.where(sub - group * h == lane % group, wide, 0.0), axis=0, keepdims=True) * math.log2(math.e)
            prod = raw_do[0, s, :, h].reshape(rows, head_dim).astype(F32) * raw_o[s, :, h].reshape(rows, head_dim).astype(F32)
            total = jnp.broadcast_to(jnp.sum(prod, axis=1, keepdims=True), (rows, LANES)).T
            first = sub_start + s * sub_len + me * local_len
            doc_row = jnp.broadcast_to(docs[pl.ds(first // LANES, 1), :], (8, LANES))
            doc = jnp.take_along_axis(doc_row, lax.rem(first, LANES) + lane // group, axis=1).astype(F32)
            lines[h, s, :, :rows] = jnp.where(sub == 0, line, jnp.where(sub == 1, total[:8, :], doc))

    share_lines.start()

    def spread(c):
        @pl.loop(0, n_sub)
        def _(s):
            for h in range(n_kv):
                for raw, nat, tr in ((raw_q, qn, qt), (raw_do, don, dot)):
                    x = raw[c, s, :, h].reshape(rows, head_dim)
                    nat[h, s, c * rows:(c + 1) * rows, :] = x
                    tr[h, s, :, c * rows:(c + 1) * rows] = x.T

    for c in local[4:]:
        c.wait()
    spread(0)
    pass_on(0, 0)
    for c in share:
        c.wait()
    spread(1)
    share_lines.wait()

    n_run = n_sub // RUNS
    n_early = 2 + min(8, 2 * n_hop)
    n_block = n_early + 2 * n_hop

    def place(e):
        head, e = e // n_block, lax.rem(e, n_block)
        early = e < n_early
        f = jnp.where(early, e - 2, e - n_early)
        k = jnp.where(early, f // 2, n_hop - 1 - f // 2)
        way = f % 2
        mine = e < 2
        slot = jnp.where(mine, own + e, way * n_hop + k)
        half = jnp.where(mine, e, (k + way) % 2)
        hop = k // 2 + 1
        key_chip = jnp.where(mine, chip, lax.rem(chip + jnp.where(way == 1, hop, n_chip - hop), n_chip))
        pos0 = (key_chip * CORES + core) * keys_local + half * key_tile
        s_lo = jnp.minimum(jnp.maximum(pos0 - sub_start - span * chip - span + sub_len, 0) // sub_len, n_sub - 1)
        return slot, head, key_chip, half, s_lo // RUNS

    counts, ends, n_taken = [], [], []
    total = jnp.int32(0)
    for head in range(n_kv):
        base, taken = total, []
        for e in range(n_block):
            n = n_run - place(jnp.int32(e))[4]
            if e < n_early:
                fits = jnp.int32(1) if e < 2 else (total + n <= base + EARLY_ITEMS[min(head, 1)]).astype(jnp.int32)
                taken.append(fits * taken[-1] if e > 2 else fits)
                n = n * taken[-1]
            else:
                f = e - n_early
                i_early = 2 + 2 * (n_hop - 1 - f // 2) + f % 2
                if i_early < n_early:
                    n = n * (1 - taken[i_early])
            total = total + n
            counts.append(n)
            ends.append(total)
        n_taken.append(sum(taken[1:], taken[0]))

    def following(at):
        i, e, j, n = at
        over = j + 1 >= n
        head, b = e // n_block, lax.rem(e, n_block) + 1
        limit = n_taken[0]
        for h in range(1, n_kv):
            limit = jnp.where(head == h, n_taken[h], limit)
        b = jnp.where(b == limit, n_early, b)
        f = b - n_early
        gone = lambda f: (f >= 0) & (2 + 2 * (n_hop - 1 - f // 2) + f % 2 < limit)
        b = jnp.where(gone(f), jnp.where((f % 2 == 1) | gone(f + 1), n_block, b + 1), b)
        e1 = jnp.minimum(head * n_block + b, n_kv * n_block - 1)
        e, j = jnp.where(over, e1, e), jnp.where(over, 0, j + 1)
        slot, head, key_chip, half, s_lo = place(e)
        i = i + 1
        return (slot, head, (s_lo + j) * RUNS, key_chip, half, (i < total).astype(jnp.int32)), (i, e, j, n_run - s_lo)

    exp_scale = scale * math.log2(math.e)
    k_iota = lax.broadcasted_iota(jnp.int32, (key_tile, width), 0)
    col = lax.broadcasted_iota(jnp.int32, (1, width), 1)
    q_off = sub_start + jnp.where(col < rows, me, sibling) * local_len + lax.rem(col, rows) // group

    def one(now, carry):
        (slot_p, head_p, s_p), (slot, head, s, key_chip, half, live), at = carry
        then, at = following(at)
        k, v = kvb[slot, head, :, :head_dim], kvb[slot, head, :, head_dim:]
        s_t = [jnp.dot(k, qt[head, s + r], preferred_element_type=F32) for r in range(RUNS)]
        dp_t = [jnp.dot(v, dot[head, s + r], preferred_element_type=F32) for r in range(RUNS)]
        p_p, ds_p = pbuf[1 - now], dsbuf[1 - now]
        q_p = qn[head_p, pl.ds(s_p, RUNS)].reshape(RUNS * width, head_dim)
        do_p = don[head_p, pl.ds(s_p, RUNS)].reshape(RUNS * width, head_dim)
        acc[slot_p, head_p, :, head_dim:] += jnp.dot(p_p, do_p, preferred_element_type=F32)
        acc[slot_p, head_p, :, :head_dim] += jnp.dot(ds_p, q_p, preferred_element_type=F32)
        k_t = kvb[slot_p, head_p, :, :head_dim].T
        for r in range(RUNS):
            dqa[head_p, s_p + r] += jnp.dot(k_t, ds_p[:, r * width:(r + 1) * width], preferred_element_type=F32)
        docs_k = key_doc[key_chip, pl.ds(pl.multiple_of(half * key_tile, 8), key_tile), :]
        docs_k = jnp.concatenate([docs_k] * (width // LANES), axis=1)
        pos0 = (key_chip * CORES + core) * keys_local + half * key_tile
        for r in range(RUNS):
            lse_r, delta_r, doc_r = [lines[head, s + r, m:m + 1, :] for m in range(3)]
            last = jnp.where(live == 1, q_off + (s + r) * sub_len - pos0, -1)
            ok = (docs_k == doc_r.astype(jnp.int32)) & (k_iota <= last)
            p = jnp.where(ok, jnp.exp2(s_t[r] * exp_scale - lse_r), 0.0)
            pbuf[now, :, r * width:(r + 1) * width] = p.astype(BF16)
            dsbuf[now, :, r * width:(r + 1) * width] = (p * (dp_t[r] - delta_r)).astype(BF16)
        return (slot, head, s), then, at

    def advance(state, target):
        i, carry = state
        m = jnp.maximum(target - i, 0) // UNROLL

        def step(_, carry):
            for u in range(UNROLL):
                carry = one(u % 2, carry)
            return carry

        return i + m * UNROLL, lax.fori_loop(0, m, step, carry)

    def end_of(e):
        out = jnp.int32(0)
        for v, n in enumerate(counts):
            out = out + jnp.where(e >= v, n, 0)
        return out

    def add(dst, src, head):
        cut = key_tile // 4

        @pl.loop(0, 4)
        def _(i):
            r = pl.ds(pl.multiple_of(i * cut, 8), cut)
            acc[dst, head, r, :] += rsb[src, head, r, :]

    def partial(i, head, peer):
        return remote(acc.at[i, head], rsb.at[i, head], rs_send.at[i, head], rs_recv.at[i, head], peer)

    def send_sums(k, way, head, state=None):
        i = way * n_hop + k
        peer = jnp.where(way == 0, left, right)
        if state is not None:
            state = advance(state, end_of(head * n_block + n_early + 2 * (n_hop - 1 - k) + way) + UNROLL)

        @pl.when(k + 2 < n_hop)
        def _():
            partial(i + 2, head, peer).wait_recv()
            add(i, i + 2, head)

        partial(i, head, peer).start()
        return state

    def arrive(k, state):
        goal = (EARLY_ITEMS[0] * k) // (n_hop - 1)
        state = advance(state, jnp.minimum(goal, end_of(jnp.minimum(2 * k + 1, n_early - 1))))
        pass_on(k, 0)

        @pl.when(k == max(n_hop - 3, 1))
        def _():
            gather_own(1)
        return state

    def both(head):
        def trip(m, state):
            state = lax.fori_loop(0, 2, lambda way, state: send_sums(n_hop - 1 - m, way, head, state), state)
            base = ends[(head + 1) * n_block - 1]
            goal = jnp.minimum(base + (EARLY_ITEMS[1] * (m + 1)) // n_hop, end_of((head + 1) * n_block + jnp.minimum(2 * m + 1, n_early - 1)))
            state = advance(state, jnp.where(state[0] >= base, goal, state[0]))
            pass_on(m, head + 1)
            if head + 2 < n_kv:
                @pl.when(m == max(n_hop - 3, 1))
                def _():
                    gather_own(head + 2)
            return state
        return trip

    def settle(head):
        for k in (1, 0):
            for way in range(2):
                partial(way * n_hop + k, head, nbr[1 - way]).wait_recv()
                add(own + (k + way) % 2, way * n_hop + k, head)

        @pl.loop(0, 2)
        def _(half):
            r = pl.ds(pl.multiple_of(half * key_tile, 8), key_tile)
            dko[r, head, :] = acc[own + half, head, :, :head_dim] * scale
            dvo[r, head, :] = acc[own + half, head, :, head_dim:]

    zero = jnp.int32(0)
    start, at = following((zero - 1, zero, zero - 1, zero + 1))
    state = (zero, (start[:3], start, at))
    state = lax.fori_loop(1, n_hop, arrive, state)
    for head in range(n_kv - 1):
        state = lax.fori_loop(0, n_hop, both(head), state)
    state = lax.fori_loop(0, 2 * n_hop - 2, lambda m, state: send_sums(n_hop - 1 - m // 2, m % 2, n_kv - 1, state), state)
    state = advance(state, total + UNROLL)
    half_rows = lambda which: dqa.at[:, :, :, pl.ds(which * rows, rows)]
    swap = remote(half_rows(1), dqr, x_send.at[3], x_recv.at[3], sibling)
    swap.start()
    for way in range(2):
        send_sums(0, way, n_kv - 1)
    swap.wait_recv()

    @pl.loop(0, n_sub)
    def _(s):
        for h in range(n_kv):
            x = ((dqa[h, s, :, :rows] + dqr[h, s]) * scale).astype(BF16).T
            raw_q[0, s, :, h] = x.reshape(local_len, group, head_dim)

    puts = [pltpu.make_async_copy(a, b, out_sem.at[i]) for i, (a, b) in enumerate(((raw_q.at[0], dq_out), (dko, dk_out), (dvo, dv_out)))]
    puts[0].start()
    for head in range(n_kv):
        settle(head)
    puts[1].start()
    puts[2].start()
    swap.wait_send()
    for way in range(2):
        for k in range(n_hop):
            for head in range(n_kv):
                gather(way, k, head).wait_send()
                partial(way * n_hop + k, head, nbr[1 - way]).wait_send()
    for c in puts:
        c.wait()


def copy_kernel(a, b, c, a_out, b_out, c_out, a_buf, b_buf, c_buf, in_sem, out_sem):
    ins = [pltpu.make_async_copy(x, y, in_sem.at[i]) for i, (x, y) in enumerate(((a, a_buf), (b, b_buf), (c, c_buf)))]
    outs = [pltpu.make_async_copy(x, y, out_sem.at[i]) for i, (x, y) in enumerate(((a_buf, a_out), (b_buf, b_out), (c_buf, c_out)))]
    for x in ins:
        x.start()
    for x, y in zip(ins, outs):
        x.wait()
        y.start()
    for y in outs:
        y.wait()


def solution(mesh):
    cp_size = mesh.shape['cp']
    q_spec = P(None, 'cp', 'tp', None)
    lse_spec = P(None, 'cp', 'tp')
    kv_spec = P('cp', 'tp', None)

    def local_backward(query, out_act, out_grad, row_lse, key_act, value_act, doc_ids):
        n_sub, local_len, n_heads, head_dim = query.shape
        keys_local, n_kv = key_act.shape[0], key_act.shape[1]
        group = n_heads // n_kv
        sub_start = keys_local * cp_size - n_sub * local_len * cp_size
        rows = local_len * group
        half = keys_local // 2
        n_chip = cp_size // CORES
        n_hop = n_chip - 1
        n_slot = 2 * n_hop + 2
        q5 = (n_sub, local_len, n_kv, group, head_dim)
        scale = head_dim ** -0.5
        flops = 2 * 5 * n_kv * n_sub * 2 * rows * head_dim * keys_local * n_hop
        hbm = pl.BlockSpec(memory_space=pl.ANY)
        dma = pltpu.SemaphoreType.DMA
        vmem = pltpu.VMEM
        dq, dk, dv = pl.pallas_call(
            functools.partial(ring_kernel, cp_size, sub_start, scale),
            name='ring_backward',
            out_shape=(jax.ShapeDtypeStruct(q5, BF16),) + (jax.ShapeDtypeStruct(key_act.shape, F32),) * 2,
            in_specs=[hbm] * 7,
            out_specs=(hbm,) * 3,
            scratch_shapes=[
                vmem((n_slot, n_kv, half, 2 * head_dim), BF16),
                vmem((n_slot, n_kv, half, 2 * head_dim), F32),
                vmem((2 * n_hop, n_kv, half, 2 * head_dim), F32),
                vmem((CORES,) + q5, BF16),
                vmem((CORES,) + q5, BF16),
                vmem(q5, BF16),
                vmem((n_sub, n_heads, local_len), F32),
                vmem((doc_ids.shape[0] // LANES, LANES), jnp.int32),
                vmem((n_kv, n_sub, CORES * rows, head_dim), BF16),
                vmem((n_kv, n_sub, head_dim, CORES * rows), BF16),
                vmem((n_kv, n_sub, CORES * rows, head_dim), BF16),
                vmem((n_kv, n_sub, head_dim, CORES * rows), BF16),
                vmem((n_kv, n_sub, 8, CORES * rows), F32),
                vmem((n_chip, keys_local, LANES), jnp.int32),
                vmem((n_kv, n_sub, head_dim, CORES * rows), F32),
                vmem((n_kv, n_sub, head_dim, rows), F32),
                vmem(key_act.shape, F32),
                vmem(key_act.shape, F32),
                vmem((2, half, RUNS * CORES * rows), BF16),
                vmem((2, half, RUNS * CORES * rows), BF16),
                vmem((2,) + key_act.shape, BF16),
                dma((2 * n_hop, n_kv)), dma((2 * n_hop, n_kv)), dma((2 * n_hop, n_kv)), dma((2 * n_hop, n_kv)),
                dma((4,)), dma((4,)), dma((7,)), dma((3,)),
            ],
            compiler_params=pltpu.CompilerParams(collective_id=0, has_side_effects=True, vmem_limit_bytes=62 * 1024 * 1024),
            cost_estimate=pl.CostEstimate(flops=flops, bytes_accessed=30 * 2 ** 20, transcendentals=0),
        )(key_act, value_act, query.reshape(q5), out_act.reshape(q5), out_grad.reshape(q5), jnp.swapaxes(row_lse, 1, 2), doc_ids.reshape(-1, LANES))
        dq, dk, dv = pl.pallas_call(
            copy_kernel,
            name='results',
            out_shape=tuple(jax.ShapeDtypeStruct(x.shape, x.dtype) for x in (dq, dk, dv)),
            in_specs=[hbm] * 3,
            out_specs=(hbm,) * 3,
            scratch_shapes=[vmem(x.shape, x.dtype) for x in (dq, dk, dv)] + [dma((3,)), dma((3,))],
            cost_estimate=pl.CostEstimate(flops=0, bytes_accessed=2 ** 22, transcendentals=0),
        )(dq, dk, dv)
        return dq.reshape(query.shape), dk, dv

    return jax.shard_map(local_backward, mesh=mesh, in_specs=(q_spec, q_spec, q_spec, lse_spec, kv_spec, kv_spec, P()),
                         out_specs=(q_spec, kv_spec, kv_spec), check_vma=False)
```

```python
import functools
import math

import jax
import jax.numpy as jnp
from jax import lax
from jax.experimental import pallas as pl
from jax.experimental.pallas import tpu as pltpu
from jax.sharding import PartitionSpec as P

MESH = pl.DeviceIdType.MESH
CORES = 2
LANES = 128
SPLIT = 64
RUNS = 2
UNROLL = 2
EARLY_ITEMS = 26
ORDER = ('e1 W4 e2 W4 e3 W4 e4 O W4 e5 W4 e6 R60 R61 E0 R50 R51 E1 R40 R41 E2 R30 R31 E3 R20 R21 E4 R10 R11 E5 R00 R01 E6 '
         'T60 T61 T50 T51 T40 T41 T30 T31 T20 T21 T10 T11 F T00 T01')
F32 = jnp.float32
BF16 = jnp.bfloat16


def ring_kernel(cp_size, sub_start, scale, k_in, v_in, q_in, o_in, do_in, lse_in, doc_in, dq_out, dk_out, dv_out,
                kvb, acc, rsb, raw_q, raw_do, raw_o, lse, docs, qn, qt, don, dot, lines, key_doc, dqa, dqr, dko, dvo, pbuf, dsbuf, raw_kv,
                ag_send, ag_recv, rs_send, rs_recv, x_send, x_recv, loc_sem, out_sem):
    n_chip = cp_size // CORES
    n_hop = n_chip - 1
    n_sub, local_len, n_kv, group, head_dim = q_in.shape
    rows = local_len * group
    width = CORES * rows
    key_tile = k_in.shape[0] // 2
    span = local_len * CORES
    sub_len = local_len * cp_size
    keys_local = 2 * key_tile
    own = 2 * n_hop

    me = lax.axis_index('cp')
    chip, core = me // CORES, lax.rem(me, CORES)
    right = lax.rem(me + CORES, cp_size)
    left = lax.rem(me + cp_size - CORES, cp_size)
    sibling = me + 1 - 2 * core
    nbr = (right, left)

    barrier = pltpu.get_barrier_semaphore()
    for peer in (right, left, sibling):
        pl.semaphore_signal(barrier, inc=1, device_id={'cp': peer}, device_id_type=MESH)

    own_kv = [pltpu.make_async_copy(x, raw_kv.at[i], loc_sem.at[5 + i]) for i, x in enumerate((k_in, v_in))]
    local = [pltpu.make_async_copy(a, b, loc_sem.at[i]) for i, (a, b) in enumerate((
        (doc_in, docs), (lse_in, lse), (do_in, raw_do.at[0]), (o_in, raw_o), (q_in, raw_q.at[0])))]
    for c in own_kv + local:
        c.start()

    @pl.loop(0, n_sub)
    def _(s):
        for h in range(n_kv):
            dqa[h, s] = jnp.zeros(dqa.shape[2:], F32)

    for c in own_kv:
        c.wait()
    for half in range(2):
        @pl.loop(0, key_tile // SPLIT)
        def _(i):
            r = pl.multiple_of(i * SPLIT, SPLIT)
            for part in range(2):
                x = raw_kv[part, pl.ds(half * key_tile + r, SPLIT)].astype(F32)
                for h in range(n_kv):
                    kvb[own + half, h, pl.ds(r, SPLIT), part * head_dim:(part + 1) * head_dim] = x[:, h].astype(BF16)

    pl.semaphore_wait(barrier, 3)

    def remote(src, dst, send, recv, peer):
        return pltpu.make_async_remote_copy(src_ref=src, dst_ref=dst, send_sem=send, recv_sem=recv,
                                            device_id={'cp': peer}, device_id_type=MESH)

    def gather(way, k, head, src=None):
        i = way * n_hop + k
        return remote(kvb.at[i, head] if src is None else src, kvb.at[i, head], ag_send.at[i, head], ag_recv.at[i, head], nbr[way])

    def gather_own(head):
        for j in range(2):
            for way in range(2):
                gather(way, j, head, kvb.at[own + (j + way) % 2, head]).start()

    def pass_on(k, head):
        for way in range(2):
            gather(way, k, head).wait_recv()
            i = way * n_hop + k

            @pl.when(k + 2 < n_hop)
            def _():
                gather(way, k + 2, head, kvb.at[i, head]).start()

    gather_own(0)
    share = [remote(q_in, raw_q.at[1], x_send.at[0], x_recv.at[0], sibling),
             remote(do_in, raw_do.at[1], x_send.at[1], x_recv.at[1], sibling)]
    for c in share:
        c.start()

    def mine(which):
        return lines.at[:, :, :, pl.ds(which * rows, rows)]

    share_lines = remote(mine(0), mine(1), x_send.at[2], x_recv.at[2], sibling)

    @pl.loop(0, acc.shape[0])
    def _(i):
        for h in range(n_kv):
            acc[i, h] = jnp.zeros(acc.shape[2:], F32)

    pbuf[...] = jnp.zeros(pbuf.shape, BF16)
    dsbuf[...] = jnp.zeros(dsbuf.shape, BF16)
    local[0].wait()
    tiles = keys_local // LANES

    @pl.loop(0, n_chip)
    def _(b):
        for r in range(tiles):
            row = docs[pl.ds((b * CORES + core) * tiles + r, 1), :]
            key_doc[b, r * LANES:(r + 1) * LANES, :] = jnp.broadcast_to(row, (LANES, LANES)).T

    lane = lax.broadcasted_iota(jnp.int32, (8, rows), 1)
    sub = lax.broadcasted_iota(jnp.int32, (8, rows), 0)
    for c in local[1:4]:
        c.wait()

    side = math.gcd(n_sub, 4)

    @pl.loop(0, n_sub // side)
    def _(t):
        for u in range(side):
            s = t * side + u
            rep = jnp.concatenate([lse[s]] * (LANES // local_len), axis=1)
            wide = jnp.take_along_axis(rep, lane // group, axis=1)
            for h in range(n_kv):
                line = jnp.sum(jnp.where(sub - group * h == lane % group, wide, 0.0), axis=0, keepdims=True) * math.log2(math.e)
                prod = raw_do[0, s, :, h].reshape(rows, head_dim).astype(F32) * raw_o[s, :, h].reshape(rows, head_dim).astype(F32)
                total = jnp.broadcast_to(jnp.sum(prod, axis=1, keepdims=True), (rows, LANES)).T
                first = sub_start + s * sub_len + me * local_len
                doc_row = jnp.broadcast_to(docs[pl.ds(first // LANES, 1), :], (8, LANES))
                doc = jnp.take_along_axis(doc_row, lax.rem(first, LANES) + lane // group, axis=1).astype(F32)
                lines[h, s, :, :rows] = jnp.where(sub == 0, line, jnp.where(sub == 1, total[:8, :], doc))

    share_lines.start()

    def spread(c):
        @pl.loop(0, n_sub // RUNS)
        def _(t):
            for u in range(RUNS):
                s = t * RUNS + u
                for h in range(n_kv):
                    for raw, nat, tr in ((raw_q, qn, qt), (raw_do, don, dot)):
                        x = raw[c, s, :, h].reshape(rows, head_dim)
                        nat[h, s, c * rows:(c + 1) * rows, :] = x
                        tr[h, s, :, c * rows:(c + 1) * rows] = x.T

    for c in local[4:]:
        c.wait()
    spread(0)
    pass_on(0, 0)
    for c in share:
        c.wait()
    spread(1)
    share_lines.wait()

    n_run = n_sub // RUNS
    n_early = 2 + min(8, 2 * n_hop)
    n_first = n_early + 2 * n_hop
    n_block = 2 * n_hop + 2
    n_entry = n_first + (n_kv - 1) * n_block

    def place(e):
        first, early = e < n_first, e < n_early
        past = jnp.maximum(e - n_first, 0)
        head = jnp.where(first, 0, 1 + lax.div(past, n_block))
        b = lax.rem(past, n_block)
        mine = jnp.where(first, e, b) < 2
        f = jnp.maximum(jnp.where(early, e - 2, jnp.where(first, e - n_early, b - 2)), 0)
        step = lax.div(f, 2)
        way = f - 2 * step
        k = jnp.where(early, step, n_hop - 1 - step)
        half = jnp.where(mine, jnp.where(first, e, b), lax.rem(k + way, 2))
        slot = jnp.where(mine, own + half, way * n_hop + k)
        hop = lax.div(k, 2) + 1
        key_chip = jnp.where(mine, chip, lax.rem(chip + jnp.where(way == 1, hop, n_chip - hop), n_chip))
        pos0 = (key_chip * CORES + core) * keys_local + half * key_tile
        s_lo = jnp.minimum(lax.div(jnp.maximum(pos0 - sub_start - span * chip - span + sub_len, 0), sub_len * RUNS), n_run - 1)
        return slot, head, key_chip, half, s_lo

    taken, until, n_taken = [], [], jnp.int32(0)
    total = jnp.int32(0)
    for e in range(n_entry):
        n = n_run - place(jnp.int32(e))[4]
        if e < n_early:
            fits = jnp.int32(1) if e < 2 else (total + n <= EARLY_ITEMS).astype(jnp.int32) * taken[-1]
            taken.append(fits)
            n_taken = n_taken + fits
            n = n * fits
        elif e < n_first:
            f = e - n_early
            i_early = 2 + 2 * (n_hop - 1 - f // 2) + f % 2
            if i_early < n_early:
                n = n * (1 - taken[i_early])
        total = total + n
        until.append(total)

    def following(at):
        i, e, j, n = at
        over = j + 1 >= n
        e1 = e + 1
        e1 = jnp.where(e1 == n_taken, n_early, e1)
        f = e1 - n_early
        back = n_hop - 1 - lax.div(jnp.maximum(f, 0), 2)
        odd = lax.rem(jnp.maximum(f, 0), 2)
        inside = (f >= 0) & (f < 2 * n_hop)
        gone = inside & (2 + 2 * back + odd < n_taken)
        both = (odd == 1) | (3 + 2 * back < n_taken)
        e1 = jnp.where(gone, jnp.where(both, n_first, e1 + 1), e1)
        e1 = jnp.minimum(e1, n_entry - 1)
        e, j = jnp.where(over, e1, e), jnp.where(over, 0, j + 1)
        slot, head, key_chip, half, s_lo = place(e)
        i = i + 1
        return (slot, head, (s_lo + j) * RUNS, key_chip, half, (i < total).astype(jnp.int32)), (i, e, j, n_run - s_lo)

    exp_scale = scale * math.log2(math.e)
    k_iota = lax.broadcasted_iota(jnp.int32, (key_tile, width), 0)
    col = lax.broadcasted_iota(jnp.int32, (1, width), 1)
    q_off = sub_start + jnp.where(col < rows, me, sibling) * local_len + lax.rem(col, rows) // group

    def one(now, carry):
        (slot_p, head_p, s_p), (slot, head, s, key_chip, half, live), at = carry
        then, at = following(at)
        k, v = kvb[slot, head, :, :head_dim], kvb[slot, head, :, head_dim:]
        s_t = [jnp.dot(k, qt[head, s + r], preferred_element_type=F32) for r in range(RUNS)]
        dp_t = [jnp.dot(v, dot[head, s + r], preferred_element_type=F32) for r in range(RUNS)]
        p_p, ds_p = pbuf[1 - now], dsbuf[1 - now]
        q_p = qn[head_p, pl.ds(s_p, RUNS)].reshape(RUNS * width, head_dim)
        do_p = don[head_p, pl.ds(s_p, RUNS)].reshape(RUNS * width, head_dim)
        acc[slot_p, head_p, :, head_dim:] += jnp.dot(p_p, do_p, preferred_element_type=F32)
        acc[slot_p, head_p, :, :head_dim] += jnp.dot(ds_p, q_p, preferred_element_type=F32)
        k_t = kvb[slot_p, head_p, :, :head_dim].T
        for r in range(RUNS):
            dqa[head_p, s_p + r] += jnp.dot(k_t, ds_p[:, r * width:(r + 1) * width], preferred_element_type=F32)
        docs_k = key_doc[key_chip, pl.ds(pl.multiple_of(half * key_tile, 8), key_tile), :]
        docs_k = jnp.concatenate([docs_k] * (width // LANES), axis=1)
        pos0 = (key_chip * CORES + core) * keys_local + half * key_tile
        for r in range(RUNS):
            lse_r, delta_r, doc_r = [lines[head, s + r, m:m + 1, :] for m in range(3)]
            last = jnp.where(live == 1, q_off + (s + r) * sub_len - pos0, -1)
            ok = (docs_k == doc_r.astype(jnp.int32)) & (k_iota <= last)
            p = jnp.where(ok, jnp.exp2(s_t[r] * exp_scale - lse_r), 0.0)
            pbuf[now, :, r * width:(r + 1) * width] = p.astype(BF16)
            dsbuf[now, :, r * width:(r + 1) * width] = (p * (dp_t[r] - delta_r)).astype(BF16)
        return (slot, head, s), then, at

    def advance(state, target):
        i, carry = state
        m = jnp.maximum(target - i, 0) // UNROLL

        def step(_, carry):
            for u in range(UNROLL):
                carry = one(u % 2, carry)
            return carry

        return i + m * UNROLL, lax.fori_loop(0, m, step, carry)

    def add(dst, src, head):
        cut = key_tile // 4

        @pl.loop(0, 4)
        def _(i):
            r = pl.ds(pl.multiple_of(i * cut, 8), cut)
            acc[dst, head, r, :] += rsb[src, head, r, :]

    def partial(i, head, peer):
        return remote(acc.at[i, head], rsb.at[i, head], rs_send.at[i, head], rs_recv.at[i, head], peer)

    half_rows = lambda which: dqa.at[:, :, :, pl.ds(which * rows, rows)]
    swap = remote(half_rows(1), dqr, x_send.at[3], x_recv.at[3], sibling)

    GATHER, SUMS, WORK, OWN, ALL = 0, 1, 2, 3, 63
    steps, arrived = [], [1, 0]
    for word in ORDER.split():
        kind, digits = word[0], word[1:]
        head = 1 if kind in 'ET' else 0
        if arrived[0] < n_hop:
            bound = min(2 * arrived[0] + 1, n_early - 1)
        else:
            bound = n_entry - 1 if arrived[1] == n_hop else n_first + 1
        k = way = items = 0
        if kind in 'eE':
            what, k = GATHER, int(digits)
            arrived[head] = k + 1
        elif kind in 'RT':
            what, k, way = SUMS, int(digits[0]), int(digits[1])
            bound = (n_first + 2 if head else n_early) + 2 * (n_hop - 1 - k) + way
        elif kind == 'O':
            what = OWN
        else:
            what, items = WORK, ALL if kind == 'F' else int(digits)
        steps.append(what + 4 * (k + 16 * (way + 2 * (head + 2 * (items + 64 * bound)))))
    def pick(table, t):
        out = jnp.int32(0)
        for j, x in enumerate(table):
            out = out + jnp.where(t == j, x, 0)
        return out

    def carry_out(t, state):
        number = pick(steps, t)
        what, number = lax.rem(number, 4), lax.div(number, 4)
        k, number = lax.rem(number, 16), lax.div(number, 16)
        way, number = lax.rem(number, 2), lax.div(number, 2)
        head, number = lax.rem(number, 2), lax.div(number, 2)
        items, bound = lax.rem(number, 64), lax.div(number, 64)
        last = pick(until, bound)
        some = jnp.where(items == ALL, last + UNROLL, jnp.minimum(state[0] + items, last))
        state = advance(state, jnp.where(what == SUMS, last + UNROLL, jnp.where(what == WORK, some, state[0])))

        @pl.when(what == GATHER)
        def _():
            pass_on(k, head)

        @pl.when(what == OWN)
        def _():
            gather_own(1)

        @pl.when(items == ALL)
        def _():
            swap.start()

        @pl.when(what == SUMS)
        def _():
            i = way * n_hop + k
            peer = jnp.where(way == 0, left, right)

            @pl.when(k + 2 < n_hop)
            def _():
                partial(i + 2, head, peer).wait_recv()
                add(i, i + 2, head)

            partial(i, head, peer).start()
        return state

    def settle(head):
        for k in (1, 0):
            for way in range(2):
                partial(way * n_hop + k, head, nbr[1 - way]).wait_recv()
                add(own + (k + way) % 2, way * n_hop + k, head)

        @pl.loop(0, 2)
        def _(half):
            r = pl.ds(pl.multiple_of(half * key_tile, 8), key_tile)
            dko[r, head, :] = acc[own + half, head, :, :head_dim] * scale
            dvo[r, head, :] = acc[own + half, head, :, head_dim:]

    zero = jnp.int32(0)
    start, at = following((zero - 1, zero, zero - 1, zero + 1))
    lax.fori_loop(0, len(steps), carry_out, (zero, (start[:3], start, at)))
    swap.wait_recv()

    @pl.loop(0, n_sub)
    def _(s):
        for h in range(n_kv):
            x = ((dqa[h, s, :, :rows] + dqr[h, s]) * scale).astype(BF16).T
            raw_q[0, s, :, h] = x.reshape(local_len, group, head_dim)

    puts = [pltpu.make_async_copy(a, b, out_sem.at[i]) for i, (a, b) in enumerate(((raw_q.at[0], dq_out), (dko, dk_out), (dvo, dv_out)))]
    puts[0].start()
    for head in range(n_kv):
        settle(head)
    puts[1].start()
    puts[2].start()
    swap.wait_send()
    for way in range(2):
        for k in range(n_hop):
            for head in range(n_kv):
                gather(way, k, head).wait_send()
                partial(way * n_hop + k, head, nbr[1 - way]).wait_send()
    for c in puts:
        c.wait()


def copy_kernel(a, b, c, a_out, b_out, c_out, a_buf, b_buf, c_buf, in_sem, out_sem):
    ins = [pltpu.make_async_copy(x, y, in_sem.at[i]) for i, (x, y) in enumerate(((a, a_buf), (b, b_buf), (c, c_buf)))]
    outs = [pltpu.make_async_copy(x, y, out_sem.at[i]) for i, (x, y) in enumerate(((a_buf, a_out), (b_buf, b_out), (c_buf, c_out)))]
    for x in ins:
        x.start()
    for x, y in zip(ins, outs):
        x.wait()
        y.start()
    for y in outs:
        y.wait()


def solution(mesh):
    cp_size = mesh.shape['cp']
    q_spec = P(None, 'cp', 'tp', None)
    lse_spec = P(None, 'cp', 'tp')
    kv_spec = P('cp', 'tp', None)

    def local_backward(query, out_act, out_grad, row_lse, key_act, value_act, doc_ids):
        n_sub, local_len, n_heads, head_dim = query.shape
        keys_local, n_kv = key_act.shape[0], key_act.shape[1]
        group = n_heads // n_kv
        sub_start = keys_local * cp_size - n_sub * local_len * cp_size
        rows = local_len * group
        half = keys_local // 2
        n_chip = cp_size // CORES
        n_hop = n_chip - 1
        n_slot = 2 * n_hop + 2
        q5 = (n_sub, local_len, n_kv, group, head_dim)
        scale = head_dim ** -0.5
        flops = 2 * 5 * n_kv * n_sub * 2 * rows * head_dim * keys_local * n_hop
        hbm = pl.BlockSpec(memory_space=pl.ANY)
        dma = pltpu.SemaphoreType.DMA
        vmem = pltpu.VMEM
        dq, dk, dv = pl.pallas_call(
            functools.partial(ring_kernel, cp_size, sub_start, scale),
            name='ring_backward',
            out_shape=(jax.ShapeDtypeStruct(q5, BF16),) + (jax.ShapeDtypeStruct(key_act.shape, F32),) * 2,
            in_specs=[hbm] * 7,
            out_specs=(hbm,) * 3,
            scratch_shapes=[
                vmem((n_slot, n_kv, half, 2 * head_dim), BF16),
                vmem((n_slot, n_kv, half, 2 * head_dim), F32),
                vmem((2 * n_hop, n_kv, half, 2 * head_dim), F32),
                vmem((CORES,) + q5, BF16),
                vmem((CORES,) + q5, BF16),
                vmem(q5, BF16),
                vmem((n_sub, n_heads, local_len), F32),
                vmem((doc_ids.shape[0] // LANES, LANES), jnp.int32),
                vmem((n_kv, n_sub, CORES * rows, head_dim), BF16),
                vmem((n_kv, n_sub, head_dim, CORES * rows), BF16),
                vmem((n_kv, n_sub, CORES * rows, head_dim), BF16),
                vmem((n_kv, n_sub, head_dim, CORES * rows), BF16),
                vmem((n_kv, n_sub, 8, CORES * rows), F32),
                vmem((n_chip, keys_local, LANES), jnp.int32),
                vmem((n_kv, n_sub, head_dim, CORES * rows), F32),
                vmem((n_kv, n_sub, head_dim, rows), F32),
                vmem(key_act.shape, F32),
                vmem(key_act.shape, F32),
                vmem((2, half, RUNS * CORES * rows), BF16),
                vmem((2, half, RUNS * CORES * rows), BF16),
                vmem((2,) + key_act.shape, BF16),
                dma((2 * n_hop, n_kv)), dma((2 * n_hop, n_kv)), dma((2 * n_hop, n_kv)), dma((2 * n_hop, n_kv)),
                dma((4,)), dma((4,)), dma((7,)), dma((3,)),
            ],
            compiler_params=pltpu.CompilerParams(collective_id=0, has_side_effects=True, vmem_limit_bytes=62 * 1024 * 1024),
            cost_estimate=pl.CostEstimate(flops=flops, bytes_accessed=30 * 2 ** 20, transcendentals=0),
        )(key_act, value_act, query.reshape(q5), out_act.reshape(q5), out_grad.reshape(q5), jnp.swapaxes(row_lse, 1, 2), doc_ids.reshape(-1, LANES))
        dq, dk, dv = pl.pallas_call(
            copy_kernel,
            name='results',
            out_shape=tuple(jax.ShapeDtypeStruct(x.shape, x.dtype) for x in (dq, dk, dv)),
            in_specs=[hbm] * 3,
            out_specs=(hbm,) * 3,
            scratch_shapes=[vmem(x.shape, x.dtype) for x in (dq, dk, dv)] + [dma((3,)), dma((3,))],
            cost_estimate=pl.CostEstimate(flops=0, bytes_accessed=2 ** 22, transcendentals=0),
        )(dq, dk, dv)
        return dq.reshape(query.shape), dk, dv

    return jax.shard_map(local_backward, mesh=mesh, in_specs=(q_spec, q_spec, q_spec, lse_spec, kv_spec, kv_spec, P()),
                         out_specs=(q_spec, kv_spec, kv_spec), check_vma=False)
```

```python
import functools
import math

import jax
import jax.numpy as jnp
from jax import lax
from jax.experimental import pallas as pl
from jax.experimental.pallas import tpu as pltpu
from jax.sharding import PartitionSpec as P

MESH = pl.DeviceIdType.MESH
CORES = 2
LANES = 128
SPLIT = 64
RUNS = 2
UNROLL = 2
EARLY_ITEMS = 26
ORDER = ('e1 W6 e2 e3 W6 e4 W4 O W8 e5 e6 W4 E0 R60 E1 R61 R50 E2 R51 R40 R41 W10 E3 W8 R30 R31 R20 R21 E4 E5 R10 R11 W4 R00 R01 W2 E6 '
         'T60 T61 T50 T51 T40 T41 T30 T31 T20 T21 T10 T11 F T00 T01')
F32 = jnp.float32
BF16 = jnp.bfloat16


def ring_kernel(cp_size, sub_start, scale, k_in, v_in, q_in, o_in, do_in, lse_in, doc_in, dq_out, dk_out, dv_out,
                kvb, acc, rsb, raw_q, raw_do, raw_o, lse, docs, qn, qt, don, dot, lines, key_doc, dqa, dqr, dko, dvo, pbuf, dsbuf, raw_kv,
                ag_send, ag_recv, rs_send, rs_recv, x_send, x_recv, loc_sem, out_sem):
    n_chip = cp_size // CORES
    n_hop = n_chip - 1
    n_sub, local_len, n_kv, group, head_dim = q_in.shape
    rows = local_len * group
    width = CORES * rows
    key_tile = k_in.shape[0] // 2
    span = local_len * CORES
    sub_len = local_len * cp_size
    keys_local = 2 * key_tile
    own = 2 * n_hop

    me = lax.axis_index('cp')
    chip, core = me // CORES, lax.rem(me, CORES)
    right = lax.rem(me + CORES, cp_size)
    left = lax.rem(me + cp_size - CORES, cp_size)
    sibling = me + 1 - 2 * core
    nbr = (right, left)

    barrier = pltpu.get_barrier_semaphore()
    for peer in (right, left, sibling):
        pl.semaphore_signal(barrier, inc=1, device_id={'cp': peer}, device_id_type=MESH)

    own_kv = [pltpu.make_async_copy(x, raw_kv.at[i], loc_sem.at[5 + i]) for i, x in enumerate((k_in, v_in))]
    local = [pltpu.make_async_copy(a, b, loc_sem.at[i]) for i, (a, b) in enumerate((
        (doc_in, docs), (lse_in, lse), (do_in, raw_do.at[0]), (o_in, raw_o), (q_in, raw_q.at[0])))]
    for c in own_kv + local:
        c.start()

    @pl.loop(0, n_sub)
    def _(s):
        for h in range(n_kv):
            dqa[h, s] = jnp.zeros(dqa.shape[2:], F32)

    for c in own_kv:
        c.wait()
    for half in range(2):
        @pl.loop(0, key_tile // SPLIT)
        def _(i):
            r = pl.multiple_of(i * SPLIT, SPLIT)
            for part in range(2):
                x = raw_kv[part, pl.ds(half * key_tile + r, SPLIT)].astype(F32)
                for h in range(n_kv):
                    kvb[own + half, h, pl.ds(r, SPLIT), part * head_dim:(part + 1) * head_dim] = x[:, h].astype(BF16)

    pl.semaphore_wait(barrier, 3)

    def remote(src, dst, send, recv, peer):
        return pltpu.make_async_remote_copy(src_ref=src, dst_ref=dst, send_sem=send, recv_sem=recv,
                                            device_id={'cp': peer}, device_id_type=MESH)

    def gather(way, k, head, src=None):
        i = way * n_hop + k
        return remote(kvb.at[i, head] if src is None else src, kvb.at[i, head], ag_send.at[i, head], ag_recv.at[i, head], nbr[way])

    def gather_own(head):
        for j in range(2):
            for way in range(2):
                gather(way, j, head, kvb.at[own + (j + way) % 2, head]).start()

    def pass_on(k, head):
        for way in range(2):
            gather(way, k, head).wait_recv()
            i = way * n_hop + k

            @pl.when(k + 2 < n_hop)
            def _():
                gather(way, k + 2, head, kvb.at[i, head]).start()

    gather_own(0)
    share = [remote(q_in, raw_q.at[1], x_send.at[0], x_recv.at[0], sibling),
             remote(do_in, raw_do.at[1], x_send.at[1], x_recv.at[1], sibling)]
    for c in share:
        c.start()

    def mine(which):
        return lines.at[:, :, :, pl.ds(which * rows, rows)]

    share_lines = remote(mine(0), mine(1), x_send.at[2], x_recv.at[2], sibling)

    @pl.loop(0, acc.shape[0])
    def _(i):
        for h in range(n_kv):
            acc[i, h] = jnp.zeros(acc.shape[2:], F32)

    pbuf[...] = jnp.zeros(pbuf.shape, BF16)
    dsbuf[...] = jnp.zeros(dsbuf.shape, BF16)
    local[0].wait()
    tiles = keys_local // LANES

    @pl.loop(0, n_chip)
    def _(b):
        for r in range(tiles):
            row = docs[pl.ds((b * CORES + core) * tiles + r, 1), :]
            key_doc[b, r * LANES:(r + 1) * LANES, :] = jnp.broadcast_to(row, (LANES, LANES)).T

    lane = lax.broadcasted_iota(jnp.int32, (8, rows), 1)
    sub = lax.broadcasted_iota(jnp.int32, (8, rows), 0)
    for c in local[1:4]:
        c.wait()

    side = math.gcd(n_sub, 4)

    @pl.loop(0, n_sub // side)
    def _(t):
        for u in range(side):
            s = t * side + u
            rep = jnp.concatenate([lse[s]] * (LANES // local_len), axis=1)
            wide = jnp.take_along_axis(rep, lane // group, axis=1)
            for h in range(n_kv):
                line = jnp.sum(jnp.where(sub - group * h == lane % group, wide, 0.0), axis=0, keepdims=True) * math.log2(math.e)
                prod = raw_do[0, s, :, h].reshape(rows, head_dim).astype(F32) * raw_o[s, :, h].reshape(rows, head_dim).astype(F32)
                total = jnp.broadcast_to(jnp.sum(prod, axis=1, keepdims=True), (rows, LANES)).T
                first = sub_start + s * sub_len + me * local_len
                doc_row = jnp.broadcast_to(docs[pl.ds(first // LANES, 1), :], (8, LANES))
                doc = jnp.take_along_axis(doc_row, lax.rem(first, LANES) + lane // group, axis=1).astype(F32)
                lines[h, s, :, :rows] = jnp.where(sub == 0, line, jnp.where(sub == 1, total[:8, :], doc))

    share_lines.start()

    def spread(c):
        @pl.loop(0, n_sub // RUNS)
        def _(t):
            for u in range(RUNS):
                s = t * RUNS + u
                for h in range(n_kv):
                    for raw, nat, tr in ((raw_q, qn, qt), (raw_do, don, dot)):
                        x = raw[c, s, :, h].reshape(rows, head_dim)
                        nat[h, s, c * rows:(c + 1) * rows, :] = x
                        tr[h, s, :, c * rows:(c + 1) * rows] = x.T

    for c in local[4:]:
        c.wait()
    spread(0)
    pass_on(0, 0)
    for c in share:
        c.wait()
    spread(1)
    share_lines.wait()

    n_run = n_sub // RUNS
    n_early = 2 + min(8, 2 * n_hop)
    n_first = n_early + 2 * n_hop
    n_block = 2 * n_hop + 2
    n_entry = n_first + (n_kv - 1) * n_block

    def place(e):
        first, early = e < n_first, e < n_early
        past = jnp.maximum(e - n_first, 0)
        head = jnp.where(first, 0, 1 + lax.div(past, n_block))
        b = lax.rem(past, n_block)
        mine = jnp.where(first, e, b) < 2
        f = jnp.maximum(jnp.where(early, e - 2, jnp.where(first, e - n_early, b - 2)), 0)
        step = lax.div(f, 2)
        way = f - 2 * step
        k = jnp.where(early, step, n_hop - 1 - step)
        half = jnp.where(mine, jnp.where(first, e, b), lax.rem(k + way, 2))
        slot = jnp.where(mine, own + half, way * n_hop + k)
        hop = lax.div(k, 2) + 1
        key_chip = jnp.where(mine, chip, lax.rem(chip + jnp.where(way == 1, hop, n_chip - hop), n_chip))
        pos0 = (key_chip * CORES + core) * keys_local + half * key_tile
        s_lo = jnp.minimum(lax.div(jnp.maximum(pos0 - sub_start - span * chip - span + sub_len, 0), sub_len * RUNS), n_run - 1)
        return slot, head, key_chip, half, s_lo

    taken, until, n_taken = [], [], jnp.int32(0)
    total = jnp.int32(0)
    for e in range(n_entry):
        n = n_run - place(jnp.int32(e))[4]
        if e < n_early:
            fits = jnp.int32(1) if e < 2 else (total + n <= EARLY_ITEMS).astype(jnp.int32) * taken[-1]
            taken.append(fits)
            n_taken = n_taken + fits
            n = n * fits
        elif e < n_first:
            f = e - n_early
            i_early = 2 + 2 * (n_hop - 1 - f // 2) + f % 2
            if i_early < n_early:
                n = n * (1 - taken[i_early])
        total = total + n
        until.append(total)

    def following(at):
        i, e, j, n = at
        over = j + 1 >= n
        e1 = e + 1
        e1 = jnp.where(e1 == n_taken, n_early, e1)
        f = e1 - n_early
        back = n_hop - 1 - lax.div(jnp.maximum(f, 0), 2)
        odd = lax.rem(jnp.maximum(f, 0), 2)
        inside = (f >= 0) & (f < 2 * n_hop)
        gone = inside & (2 + 2 * back + odd < n_taken)
        both = (odd == 1) | (3 + 2 * back < n_taken)
        e1 = jnp.where(gone, jnp.where(both, n_first, e1 + 1), e1)
        e1 = jnp.minimum(e1, n_entry - 1)
        e, j = jnp.where(over, e1, e), jnp.where(over, 0, j + 1)
        slot, head, key_chip, half, s_lo = place(e)
        i = i + 1
        return (slot, head, (s_lo + j) * RUNS, key_chip, half, (i < total).astype(jnp.int32)), (i, e, j, n_run - s_lo)

    exp_scale = scale * math.log2(math.e)
    k_iota = lax.broadcasted_iota(jnp.int32, (key_tile, width), 0)
    col = lax.broadcasted_iota(jnp.int32, (1, width), 1)
    q_off = sub_start + jnp.where(col < rows, me, sibling) * local_len + lax.rem(col, rows) // group

    def one(now, carry):
        (slot_p, head_p, s_p), (slot, head, s, key_chip, half, live), at = carry
        then, at = following(at)
        k, v = kvb[slot, head, :, :head_dim], kvb[slot, head, :, head_dim:]
        s_t = [jnp.dot(k, qt[head, s + r], preferred_element_type=F32) for r in range(RUNS)]
        dp_t = [jnp.dot(v, dot[head, s + r], preferred_element_type=F32) for r in range(RUNS)]
        p_p, ds_p = pbuf[1 - now], dsbuf[1 - now]
        q_p = qn[head_p, pl.ds(s_p, RUNS)].reshape(RUNS * width, head_dim)
        do_p = don[head_p, pl.ds(s_p, RUNS)].reshape(RUNS * width, head_dim)
        acc[slot_p, head_p, :, head_dim:] += jnp.dot(p_p, do_p, preferred_element_type=F32)
        acc[slot_p, head_p, :, :head_dim] += jnp.dot(ds_p, q_p, preferred_element_type=F32)
        k_t = kvb[slot_p, head_p, :, :head_dim].T
        for r in range(RUNS):
            dqa[head_p, s_p + r] += jnp.dot(k_t, ds_p[:, r * width:(r + 1) * width], preferred_element_type=F32)
        docs_k = key_doc[key_chip, pl.ds(pl.multiple_of(half * key_tile, 8), key_tile), :]
        docs_k = jnp.concatenate([docs_k] * (width // LANES), axis=1)
        pos0 = (key_chip * CORES + core) * keys_local + half * key_tile
        for r in range(RUNS):
            lse_r, delta_r, doc_r = [lines[head, s + r, m:m + 1, :] for m in range(3)]
            last = jnp.where(live == 1, q_off + (s + r) * sub_len - pos0, -1)
            ok = (docs_k == doc_r.astype(jnp.int32)) & (k_iota <= last)
            p = jnp.where(ok, jnp.exp2(s_t[r] * exp_scale - lse_r), 0.0)
            pbuf[now, :, r * width:(r + 1) * width] = p.astype(BF16)
            dsbuf[now, :, r * width:(r + 1) * width] = (p * (dp_t[r] - delta_r)).astype(BF16)
        return (slot, head, s), then, at

    def advance(state, target):
        i, carry = state
        m = jnp.maximum(target - i, 0) // UNROLL

        def step(_, carry):
            for u in range(UNROLL):
                carry = one(u % 2, carry)
            return carry

        return i + m * UNROLL, lax.fori_loop(0, m, step, carry)

    def add(dst, src, head):
        cut = key_tile // 4

        @pl.loop(0, 4)
        def _(i):
            r = pl.ds(pl.multiple_of(i * cut, 8), cut)
            acc[dst, head, r, :] += rsb[src, head, r, :]

    def partial(i, head, peer):
        return remote(acc.at[i, head], rsb.at[i, head], rs_send.at[i, head], rs_recv.at[i, head], peer)

    half_rows = lambda which: dqa.at[:, :, :, pl.ds(which * rows, rows)]
    swap = remote(half_rows(1), dqr, x_send.at[3], x_recv.at[3], sibling)

    GATHER, SUMS, WORK, OWN, ALL = 0, 1, 2, 3, 63
    steps, arrived = [], [1, 0]
    for word in ORDER.split():
        kind, digits = word[0], word[1:]
        head = 1 if kind in 'ET' else 0
        if arrived[0] < n_hop:
            bound = min(2 * arrived[0] + 1, n_early - 1)
        else:
            bound = n_entry - 1 if arrived[1] == n_hop else n_first + 1
        k = way = items = 0
        if kind in 'eE':
            what, k = GATHER, int(digits)
            arrived[head] = k + 1
        elif kind in 'RT':
            what, k, way = SUMS, int(digits[0]), int(digits[1])
            bound = (n_first + 2 if head else n_early) + 2 * (n_hop - 1 - k) + way
        elif kind == 'O':
            what = OWN
        else:
            what, items = WORK, ALL if kind == 'F' else int(digits)
        steps.append(what + 4 * (k + 16 * (way + 2 * (head + 2 * (items + 64 * bound)))))
    def pick(table, t):
        out = jnp.int32(0)
        for j, x in enumerate(table):
            out = out + jnp.where(t == j, x, 0)
        return out

    def carry_out(t, state):
        number = pick(steps, t)
        what, number = lax.rem(number, 4), lax.div(number, 4)
        k, number = lax.rem(number, 16), lax.div(number, 16)
        way, number = lax.rem(number, 2), lax.div(number, 2)
        head, number = lax.rem(number, 2), lax.div(number, 2)
        items, bound = lax.rem(number, 64), lax.div(number, 64)
        last = pick(until, bound)
        some = jnp.where(items == ALL, last + UNROLL, jnp.minimum(state[0] + items, last))
        state = advance(state, jnp.where(what == SUMS, last + UNROLL, jnp.where(what == WORK, some, state[0])))

        @pl.when(what == GATHER)
        def _():
            pass_on(k, head)

        @pl.when(what == OWN)
        def _():
            gather_own(1)

        @pl.when(items == ALL)
        def _():
            swap.start()

        @pl.when(what == SUMS)
        def _():
            i = way * n_hop + k
            peer = jnp.where(way == 0, left, right)

            @pl.when(k + 2 < n_hop)
            def _():
                partial(i + 2, head, peer).wait_recv()
                add(i, i + 2, head)

            partial(i, head, peer).start()
        return state

    def settle(head):
        for k in (1, 0):
            for way in range(2):
                partial(way * n_hop + k, head, nbr[1 - way]).wait_recv()
                add(own + (k + way) % 2, way * n_hop + k, head)

        @pl.loop(0, 2)
        def _(half):
            r = pl.ds(pl.multiple_of(half * key_tile, 8), key_tile)
            dko[r, head, :] = acc[own + half, head, :, :head_dim] * scale
            dvo[r, head, :] = acc[own + half, head, :, head_dim:]

    zero = jnp.int32(0)
    start, at = following((zero - 1, zero, zero - 1, zero + 1))
    lax.fori_loop(0, len(steps), carry_out, (zero, (start[:3], start, at)))
    swap.wait_recv()

    @pl.loop(0, n_sub)
    def _(s):
        for h in range(n_kv):
            x = ((dqa[h, s, :, :rows] + dqr[h, s]) * scale).astype(BF16).T
            raw_q[0, s, :, h] = x.reshape(local_len, group, head_dim)

    puts = [pltpu.make_async_copy(a, b, out_sem.at[i]) for i, (a, b) in enumerate(((raw_q.at[0], dq_out), (dko, dk_out), (dvo, dv_out)))]
    puts[0].start()
    for head in range(n_kv):
        settle(head)
    puts[1].start()
    puts[2].start()
    swap.wait_send()
    for way in range(2):
        for k in range(n_hop):
            for head in range(n_kv):
                gather(way, k, head).wait_send()
                partial(way * n_hop + k, head, nbr[1 - way]).wait_send()
    for c in puts:
        c.wait()


def copy_kernel(a, b, c, a_out, b_out, c_out, a_buf, b_buf, c_buf, in_sem, out_sem):
    ins = [pltpu.make_async_copy(x, y, in_sem.at[i]) for i, (x, y) in enumerate(((a, a_buf), (b, b_buf), (c, c_buf)))]
    outs = [pltpu.make_async_copy(x, y, out_sem.at[i]) for i, (x, y) in enumerate(((a_buf, a_out), (b_buf, b_out), (c_buf, c_out)))]
    for x in ins:
        x.start()
    for x, y in zip(ins, outs):
        x.wait()
        y.start()
    for y in outs:
        y.wait()


def solution(mesh):
    cp_size = mesh.shape['cp']
    q_spec = P(None, 'cp', 'tp', None)
    lse_spec = P(None, 'cp', 'tp')
    kv_spec = P('cp', 'tp', None)

    def local_backward(query, out_act, out_grad, row_lse, key_act, value_act, doc_ids):
        n_sub, local_len, n_heads, head_dim = query.shape
        keys_local, n_kv = key_act.shape[0], key_act.shape[1]
        group = n_heads // n_kv
        sub_start = keys_local * cp_size - n_sub * local_len * cp_size
        rows = local_len * group
        half = keys_local // 2
        n_chip = cp_size // CORES
        n_hop = n_chip - 1
        n_slot = 2 * n_hop + 2
        q5 = (n_sub, local_len, n_kv, group, head_dim)
        scale = head_dim ** -0.5
        flops = 2 * 5 * n_kv * n_sub * 2 * rows * head_dim * keys_local * n_hop
        hbm = pl.BlockSpec(memory_space=pl.ANY)
        dma = pltpu.SemaphoreType.DMA
        vmem = pltpu.VMEM
        dq, dk, dv = pl.pallas_call(
            functools.partial(ring_kernel, cp_size, sub_start, scale),
            name='ring_backward',
            out_shape=(jax.ShapeDtypeStruct(q5, BF16),) + (jax.ShapeDtypeStruct(key_act.shape, F32),) * 2,
            in_specs=[hbm] * 7,
            out_specs=(hbm,) * 3,
            scratch_shapes=[
                vmem((n_slot, n_kv, half, 2 * head_dim), BF16),
                vmem((n_slot, n_kv, half, 2 * head_dim), F32),
                vmem((2 * n_hop, n_kv, half, 2 * head_dim), F32),
                vmem((CORES,) + q5, BF16),
                vmem((CORES,) + q5, BF16),
                vmem(q5, BF16),
                vmem((n_sub, n_heads, local_len), F32),
                vmem((doc_ids.shape[0] // LANES, LANES), jnp.int32),
                vmem((n_kv, n_sub, CORES * rows, head_dim), BF16),
                vmem((n_kv, n_sub, head_dim, CORES * rows), BF16),
                vmem((n_kv, n_sub, CORES * rows, head_dim), BF16),
                vmem((n_kv, n_sub, head_dim, CORES * rows), BF16),
                vmem((n_kv, n_sub, 8, CORES * rows), F32),
                vmem((n_chip, keys_local, LANES), jnp.int32),
                vmem((n_kv, n_sub, head_dim, CORES * rows), F32),
                vmem((n_kv, n_sub, head_dim, rows), F32),
                vmem(key_act.shape, F32),
                vmem(key_act.shape, F32),
                vmem((2, half, RUNS * CORES * rows), BF16),
                vmem((2, half, RUNS * CORES * rows), BF16),
                vmem((2,) + key_act.shape, BF16),
                dma((2 * n_hop, n_kv)), dma((2 * n_hop, n_kv)), dma((2 * n_hop, n_kv)), dma((2 * n_hop, n_kv)),
                dma((4,)), dma((4,)), dma((7,)), dma((3,)),
            ],
            compiler_params=pltpu.CompilerParams(collective_id=0, has_side_effects=True, vmem_limit_bytes=62 * 1024 * 1024),
            cost_estimate=pl.CostEstimate(flops=flops, bytes_accessed=30 * 2 ** 20, transcendentals=0),
        )(key_act, value_act, query.reshape(q5), out_act.reshape(q5), out_grad.reshape(q5), jnp.swapaxes(row_lse, 1, 2), doc_ids.reshape(-1, LANES))
        dq, dk, dv = pl.pallas_call(
            copy_kernel,
            name='results',
            out_shape=tuple(jax.ShapeDtypeStruct(x.shape, x.dtype) for x in (dq, dk, dv)),
            in_specs=[hbm] * 3,
            out_specs=(hbm,) * 3,
            scratch_shapes=[vmem(x.shape, x.dtype) for x in (dq, dk, dv)] + [dma((3,)), dma((3,))],
            cost_estimate=pl.CostEstimate(flops=0, bytes_accessed=2 ** 22, transcendentals=0),
        )(dq, dk, dv)
        return dq.reshape(query.shape), dk, dv

    return jax.shard_map(local_backward, mesh=mesh, in_specs=(q_spec, q_spec, q_spec, lse_spec, kv_spec, kv_spec, P()),
                         out_specs=(q_spec, kv_spec, kv_spec), check_vma=False)
```

```python
import functools
import math

import jax
import jax.numpy as jnp
from jax import lax
from jax.experimental import pallas as pl
from jax.experimental.pallas import tpu as pltpu
from jax.sharding import PartitionSpec as P

MESH = pl.DeviceIdType.MESH
CORES = 2
LANES = 128
SPLIT = 64
PIECES = 4
RUNS = 2
UNROLL = 2
EARLY_ITEMS = 26
ORDER = ('e1 W6 e2 e3 W6 e4 W4 O W8 e5 e6 W4 E0 R60 E1 R61 R50 E2 R51 R40 R41 W10 E3 W8 R30 R31 R20 R21 E4 E5 R10 R11 W4 R00 R01 W2 E6 '
         'T60 T61 T50 T51 T40 T41 T30 T31 T20 T21 T10 T11 F T00 T01')
F32 = jnp.float32
BF16 = jnp.bfloat16


def ring_kernel(cp_size, sub_start, scale, k_in, v_in, q_in, o_in, do_in, lse_in, doc_in, dq_out, dk_out, dv_out,
                kvb, acc, rsb, raw_q, raw_do, raw_o, lse, docs, qn, qt, don, dot, lines, key_doc, dqa, dqr, dko, dvo, pbuf, dsbuf, raw_kv,
                ag_send, ag_recv, rs_send, rs_recv, x_send, x_recv, loc_sem, out_sem):
    n_chip = cp_size // CORES
    n_hop = n_chip - 1
    n_sub, local_len, n_kv, group, head_dim = q_in.shape
    rows = local_len * group
    width = CORES * rows
    key_tile = k_in.shape[0] // 2
    span = local_len * CORES
    sub_len = local_len * cp_size
    keys_local = 2 * key_tile
    own = 2 * n_hop

    me = lax.axis_index('cp')
    chip, core = me // CORES, lax.rem(me, CORES)
    right = lax.rem(me + CORES, cp_size)
    left = lax.rem(me + cp_size - CORES, cp_size)
    sibling = me + 1 - 2 * core
    nbr = (right, left)

    barrier = pltpu.get_barrier_semaphore()
    for peer in (right, left, sibling):
        pl.semaphore_signal(barrier, inc=1, device_id={'cp': peer}, device_id_type=MESH)

    own_kv = [pltpu.make_async_copy(x, raw_kv.at[i], loc_sem.at[5 + i]) for i, x in enumerate((k_in, v_in))]
    local = [pltpu.make_async_copy(a, b, loc_sem.at[i]) for i, (a, b) in enumerate((
        (doc_in, docs), (lse_in, lse), (do_in, raw_do.at[0]), (o_in, raw_o), (q_in, raw_q.at[0])))]
    for c in own_kv + local:
        c.start()

    @pl.loop(0, n_sub)
    def _(s):
        for h in range(n_kv):
            dqa[h, s] = jnp.zeros(dqa.shape[2:], F32)

    for c in own_kv:
        c.wait()

    def split(h):
        @pl.loop(0, key_tile // SPLIT)
        def _(i):
            r = pl.multiple_of(i * SPLIT, SPLIT)
            for half in range(2):
                for part in range(2):
                    x = raw_kv[part, pl.ds(half * key_tile + r, SPLIT)].astype(F32)
                    kvb[own + half, h, pl.ds(r, SPLIT), part * head_dim:(part + 1) * head_dim] = x[:, h].astype(BF16)

    split(0)
    pl.semaphore_wait(barrier, 3)

    def remote(src, dst, send, recv, peer):
        return pltpu.make_async_remote_copy(src_ref=src, dst_ref=dst, send_sem=send, recv_sem=recv,
                                            device_id={'cp': peer}, device_id_type=MESH)

    def gather(way, k, head, src=None):
        i = way * n_hop + k
        return remote(kvb.at[i, head] if src is None else src, kvb.at[i, head], ag_send.at[0], ag_recv.at[i, head], nbr[way])

    def gather_own(head):
        for j in range(2):
            for way in range(2):
                gather(way, j, head, kvb.at[own + (j + way) % 2, head]).start()

    def pass_on(k, head):
        for way in range(2):
            gather(way, k, head).wait_recv()
            i = way * n_hop + k

            @pl.when(k + 2 < n_hop)
            def _():
                gather(way, k + 2, head, kvb.at[i, head]).start()

    gather_own(0)
    for h in range(1, n_kv):
        split(h)
    share = [remote(q_in, raw_q.at[1], x_send.at[0], x_recv.at[0], sibling),
             remote(do_in, raw_do.at[1], x_send.at[1], x_recv.at[1], sibling)]
    for c in share:
        c.start()

    def mine(which):
        return lines.at[:, :, :, pl.ds(which * rows, rows)]

    share_lines = remote(mine(0), mine(1), x_send.at[2], x_recv.at[2], sibling)

    @pl.loop(0, acc.shape[0])
    def _(i):
        for h in range(n_kv):
            acc[i, h] = jnp.zeros(acc.shape[2:], F32)

    pbuf[...] = jnp.zeros(pbuf.shape, BF16)
    dsbuf[...] = jnp.zeros(dsbuf.shape, BF16)
    local[0].wait()
    tiles = keys_local // LANES

    @pl.loop(0, n_chip)
    def _(b):
        for r in range(tiles):
            row = docs[pl.ds((b * CORES + core) * tiles + r, 1), :]
            key_doc[b, r * LANES:(r + 1) * LANES, :] = jnp.broadcast_to(row, (LANES, LANES)).T

    lane = lax.broadcasted_iota(jnp.int32, (8, rows), 1)
    sub = lax.broadcasted_iota(jnp.int32, (8, rows), 0)
    for c in local[1:4]:
        c.wait()

    side = math.gcd(n_sub, 4)

    @pl.loop(0, n_sub // side)
    def _(t):
        for u in range(side):
            s = t * side + u
            rep = jnp.concatenate([lse[s]] * (LANES // local_len), axis=1)
            wide = jnp.take_along_axis(rep, lane // group, axis=1)
            for h in range(n_kv):
                line = jnp.sum(jnp.where(sub - group * h == lane % group, wide, 0.0), axis=0, keepdims=True) * math.log2(math.e)
                prod = raw_do[0, s, :, h].reshape(rows, head_dim).astype(F32) * raw_o[s, :, h].reshape(rows, head_dim).astype(F32)
                total = jnp.broadcast_to(jnp.sum(prod, axis=1, keepdims=True), (rows, LANES)).T
                first = sub_start + s * sub_len + me * local_len
                doc_row = jnp.broadcast_to(docs[pl.ds(first // LANES, 1), :], (8, LANES))
                doc = jnp.take_along_axis(doc_row, lax.rem(first, LANES) + lane // group, axis=1).astype(F32)
                lines[h, s, :, :rows] = jnp.where(sub == 0, line, jnp.where(sub == 1, total[:8, :], doc))

    share_lines.start()

    def spread(c):
        @pl.loop(0, n_sub // RUNS)
        def _(t):
            for u in range(RUNS):
                s = t * RUNS + u
                for h in range(n_kv):
                    for raw, nat, tr in ((raw_q, qn, qt), (raw_do, don, dot)):
                        x = raw[c, s, :, h].reshape(rows, head_dim)
                        nat[h, s, c * rows:(c + 1) * rows, :] = x
                        tr[h, s, :, c * rows:(c + 1) * rows] = x.T

    for c in local[4:]:
        c.wait()
    spread(0)
    pass_on(0, 0)
    for c in share:
        c.wait()
    spread(1)
    share_lines.wait()

    n_run = n_sub // RUNS
    n_early = 2 + min(8, 2 * n_hop)
    n_first = n_early + 2 * n_hop
    n_block = 2 * n_hop + 2
    n_entry = n_first + (n_kv - 1) * n_block

    def place(e):
        first, early = e < n_first, e < n_early
        past = jnp.maximum(e - n_first, 0)
        head = jnp.where(first, 0, 1 + lax.div(past, n_block))
        b = lax.rem(past, n_block)
        mine = jnp.where(first, e, b) < 2
        f = jnp.maximum(jnp.where(early, e - 2, jnp.where(first, e - n_early, b - 2)), 0)
        step = lax.div(f, 2)
        way = f - 2 * step
        k = jnp.where(early, step, n_hop - 1 - step)
        half = jnp.where(mine, jnp.where(first, e, b), lax.rem(k + way, 2))
        slot = jnp.where(mine, own + half, way * n_hop + k)
        hop = lax.div(k, 2) + 1
        key_chip = jnp.where(mine, chip, lax.rem(chip + jnp.where(way == 1, hop, n_chip - hop), n_chip))
        pos0 = (key_chip * CORES + core) * keys_local + half * key_tile
        s_lo = jnp.minimum(lax.div(jnp.maximum(pos0 - sub_start - span * chip - span + sub_len, 0), sub_len * RUNS), n_run - 1)
        return slot, head, key_chip, half, s_lo

    taken, until, n_taken = [], [], jnp.int32(0)
    total = jnp.int32(0)
    for e in range(n_entry):
        n = n_run - place(jnp.int32(e))[4]
        if e < n_early:
            fits = jnp.int32(1) if e < 2 else (total + n <= EARLY_ITEMS).astype(jnp.int32) * taken[-1]
            taken.append(fits)
            n_taken = n_taken + fits
            n = n * fits
        elif e < n_first:
            f = e - n_early
            i_early = 2 + 2 * (n_hop - 1 - f // 2) + f % 2
            if i_early < n_early:
                n = n * (1 - taken[i_early])
        total = total + n
        until.append(total)

    def following(at):
        i, e, j, n = at
        over = j + 1 >= n
        e1 = e + 1
        e1 = jnp.where(e1 == n_taken, n_early, e1)
        f = e1 - n_early
        back = n_hop - 1 - lax.div(jnp.maximum(f, 0), 2)
        odd = lax.rem(jnp.maximum(f, 0), 2)
        inside = (f >= 0) & (f < 2 * n_hop)
        gone = inside & (2 + 2 * back + odd < n_taken)
        both = (odd == 1) | (3 + 2 * back < n_taken)
        e1 = jnp.where(gone, jnp.where(both, n_first, e1 + 1), e1)
        e1 = jnp.minimum(e1, n_entry - 1)
        e, j = jnp.where(over, e1, e), jnp.where(over, 0, j + 1)
        slot, head, key_chip, half, s_lo = place(e)
        i = i + 1
        return (slot, head, (s_lo + j) * RUNS, key_chip, half, (i < total).astype(jnp.int32)), (i, e, j, n_run - s_lo)

    exp_scale = scale * math.log2(math.e)
    k_iota = lax.broadcasted_iota(jnp.int32, (key_tile, width), 0)
    col = lax.broadcasted_iota(jnp.int32, (1, width), 1)
    q_off = sub_start + jnp.where(col < rows, me, sibling) * local_len + lax.rem(col, rows) // group

    def one(now, carry):
        (slot_p, head_p, s_p), (slot, head, s, key_chip, half, live), at = carry
        then, at = following(at)
        k, v = kvb[slot, head, :, :head_dim], kvb[slot, head, :, head_dim:]
        s_t = [jnp.dot(k, qt[head, s + r], preferred_element_type=F32) for r in range(RUNS)]
        dp_t = [jnp.dot(v, dot[head, s + r], preferred_element_type=F32) for r in range(RUNS)]
        p_p, ds_p = pbuf[1 - now], dsbuf[1 - now]
        q_p = qn[head_p, pl.ds(s_p, RUNS)].reshape(RUNS * width, head_dim)
        do_p = don[head_p, pl.ds(s_p, RUNS)].reshape(RUNS * width, head_dim)
        acc[slot_p, head_p, :, head_dim:] += jnp.dot(p_p, do_p, preferred_element_type=F32)
        acc[slot_p, head_p, :, :head_dim] += jnp.dot(ds_p, q_p, preferred_element_type=F32)
        k_t = kvb[slot_p, head_p, :, :head_dim].T
        for r in range(RUNS):
            dqa[head_p, s_p + r] += jnp.dot(k_t, ds_p[:, r * width:(r + 1) * width], preferred_element_type=F32)
        docs_k = key_doc[key_chip, pl.ds(pl.multiple_of(half * key_tile, 8), key_tile), :]
        docs_k = jnp.concatenate([docs_k] * (width // LANES), axis=1)
        pos0 = (key_chip * CORES + core) * keys_local + half * key_tile
        for r in range(RUNS):
            lse_r, delta_r, doc_r = [lines[head, s + r, m:m + 1, :] for m in range(3)]
            last = jnp.where(live == 1, q_off + (s + r) * sub_len - pos0, -1)
            ok = (docs_k == doc_r.astype(jnp.int32)) & (k_iota <= last)
            p = jnp.where(ok, jnp.exp2(s_t[r] * exp_scale - lse_r), 0.0)
            pbuf[now, :, r * width:(r + 1) * width] = p.astype(BF16)
            dsbuf[now, :, r * width:(r + 1) * width] = (p * (dp_t[r] - delta_r)).astype(BF16)
        return (slot, head, s), then, at

    def advance(state, target):
        i, carry = state
        m = jnp.maximum(target - i, 0) // UNROLL

        def step(_, carry):
            for u in range(UNROLL):
                carry = one(u % 2, carry)
            return carry

        return i + m * UNROLL, lax.fori_loop(0, m, step, carry)

    def add(dst, src, head):
        cut = key_tile // 4

        @pl.loop(0, 4)
        def _(i):
            r = pl.ds(pl.multiple_of(i * cut, 8), cut)
            acc[dst, head, r, :] += rsb[src, head, r, :]

    def partial(i, head, peer):
        return remote(acc.at[i, head], rsb.at[i, head], rs_send.at[0], rs_recv.at[i, head], peer)

    half_rows = lambda which: dqa.at[:, :, :, pl.ds(which * rows, rows)]
    swap = remote(half_rows(1), dqr, x_send.at[3], x_recv.at[3], sibling)

    GATHER, SUMS, WORK, OWN, ALL = 0, 1, 2, 3, 63
    steps, arrived = [], [1, 0]
    for word in ORDER.split():
        kind, digits = word[0], word[1:]
        head = 1 if kind in 'ET' else 0
        if arrived[0] < n_hop:
            bound = min(2 * arrived[0] + 1, n_early - 1)
        else:
            bound = n_entry - 1 if arrived[1] == n_hop else n_first + 1
        k = way = items = 0
        if kind in 'eE':
            what, k = GATHER, int(digits)
            arrived[head] = k + 1
        elif kind in 'RT':
            what, k, way = SUMS, int(digits[0]), int(digits[1])
            bound = (n_first + 2 if head else n_early) + 2 * (n_hop - 1 - k) + way
        elif kind == 'O':
            what = OWN
        else:
            what, items = WORK, ALL if kind == 'F' else int(digits)
        steps.append(what + 4 * (k + 16 * (way + 2 * (head + 2 * (items + 64 * bound)))))
    def pick(table, t):
        out = jnp.int32(0)
        for j, x in enumerate(table):
            out = out + jnp.where(t == j, x, 0)
        return out

    def carry_out(t, state):
        number = pick(steps, t)
        what, number = lax.rem(number, 4), lax.div(number, 4)
        k, number = lax.rem(number, 16), lax.div(number, 16)
        way, number = lax.rem(number, 2), lax.div(number, 2)
        head, number = lax.rem(number, 2), lax.div(number, 2)
        items, bound = lax.rem(number, 64), lax.div(number, 64)
        last = pick(until, bound)
        some = jnp.where(items == ALL, last + UNROLL, jnp.minimum(state[0] + items, last))
        state = advance(state, jnp.where(what == SUMS, last + UNROLL, jnp.where(what == WORK, some, state[0])))

        @pl.when(what == GATHER)
        def _():
            pass_on(k, head)

        @pl.when(what == OWN)
        def _():
            gather_own(1)

        @pl.when(items == ALL)
        def _():
            swap.start()

        @pl.when(what == SUMS)
        def _():
            i = way * n_hop + k
            peer = jnp.where(way == 0, left, right)

            @pl.when(k + 2 < n_hop)
            def _():
                partial(i + 2, head, peer).wait_recv()
                add(i, i + 2, head)

            partial(i, head, peer).start()
        return state

    def settle(head, half):
        for k in (1, 0):
            way = (half + k) % 2
            partial(way * n_hop + k, head, nbr[1 - way]).wait_recv()
            add(own + half, way * n_hop + k, head)
        r = slice(half * key_tile, (half + 1) * key_tile)
        dko[r, head, :] = acc[own + half, head, :, :head_dim] * scale
        dvo[r, head, :] = acc[own + half, head, :, head_dim:]

    zero = jnp.int32(0)
    start, at = following((zero - 1, zero, zero - 1, zero + 1))
    lax.fori_loop(0, len(steps), carry_out, (zero, (start[:3], start, at)))
    swap.wait_recv()

    @pl.loop(0, n_sub)
    def _(s):
        for h in range(n_kv):
            x = ((dqa[h, s, :, :rows] + dqr[h, s]) * scale).astype(BF16).T
            raw_q[0, s, :, h] = x.reshape(local_len, group, head_dim)

    puts = [pltpu.make_async_copy(raw_q.at[0], dq_out, out_sem.at[0])]
    puts[0].start()
    for head in range(n_kv - 1):
        for half in range(2):
            settle(head, half)
    for half in range(2):
        settle(n_kv - 1, half)
        r = pl.ds(half * key_tile, key_tile)
        for i, (a, b) in enumerate(((dko, dk_out), (dvo, dv_out))):
            c = pltpu.make_async_copy(a.at[r], b.at[r], out_sem.at[1 + 2 * half + i])
            c.start()
            puts.append(c)
    swap.wait_send()
    moved = pl.ds(0, 2 * n_hop)
    remote(kvb.at[moved], kvb.at[moved], ag_send.at[0], ag_recv.at[0, 0], right).wait_send()
    remote(acc.at[moved], rsb.at[moved], rs_send.at[0], rs_recv.at[0, 0], right).wait_send()
    for c in puts:
        c.wait()


def copy_kernel(a, b, c, a_out, b_out, c_out, a_buf, b_buf, c_buf, in_sem, out_sem):
    moves = []
    for src, buf, dst in ((a, a_buf, a_out), (b, b_buf, b_out), (c, c_buf, c_out)):
        piece = src.shape[0] // PIECES
        for i in range(PIECES):
            r, n = pl.ds(i * piece, piece), len(moves)
            moves.append((pltpu.make_async_copy(src.at[r], buf.at[r], in_sem.at[n]),
                          pltpu.make_async_copy(buf.at[r], dst.at[r], out_sem.at[n])))
    for x, _ in moves:
        x.start()
    for x, y in moves:
        x.wait()
        y.start()
    for _, y in moves:
        y.wait()


def solution(mesh):
    cp_size = mesh.shape['cp']
    q_spec = P(None, 'cp', 'tp', None)
    lse_spec = P(None, 'cp', 'tp')
    kv_spec = P('cp', 'tp', None)

    def local_backward(query, out_act, out_grad, row_lse, key_act, value_act, doc_ids):
        n_sub, local_len, n_heads, head_dim = query.shape
        keys_local, n_kv = key_act.shape[0], key_act.shape[1]
        group = n_heads // n_kv
        sub_start = keys_local * cp_size - n_sub * local_len * cp_size
        rows = local_len * group
        half = keys_local // 2
        n_chip = cp_size // CORES
        n_hop = n_chip - 1
        n_slot = 2 * n_hop + 2
        q5 = (n_sub, local_len, n_kv, group, head_dim)
        scale = head_dim ** -0.5
        flops = 2 * 5 * n_kv * n_sub * 2 * rows * head_dim * keys_local * n_hop
        hbm = pl.BlockSpec(memory_space=pl.ANY)
        dma = pltpu.SemaphoreType.DMA
        vmem = pltpu.VMEM
        dq, dk, dv = pl.pallas_call(
            functools.partial(ring_kernel, cp_size, sub_start, scale),
            name='ring_backward',
            out_shape=(jax.ShapeDtypeStruct(q5, BF16),) + (jax.ShapeDtypeStruct(key_act.shape, F32),) * 2,
            in_specs=[hbm] * 7,
            out_specs=(hbm,) * 3,
            scratch_shapes=[
                vmem((n_slot, n_kv, half, 2 * head_dim), BF16),
                vmem((n_slot, n_kv, half, 2 * head_dim), F32),
                vmem((2 * n_hop, n_kv, half, 2 * head_dim), F32),
                vmem((CORES,) + q5, BF16),
                vmem((CORES,) + q5, BF16),
                vmem(q5, BF16),
                vmem((n_sub, n_heads, local_len), F32),
                vmem((doc_ids.shape[0] // LANES, LANES), jnp.int32),
                vmem((n_kv, n_sub, CORES * rows, head_dim), BF16),
                vmem((n_kv, n_sub, head_dim, CORES * rows), BF16),
                vmem((n_kv, n_sub, CORES * rows, head_dim), BF16),
                vmem((n_kv, n_sub, head_dim, CORES * rows), BF16),
                vmem((n_kv, n_sub, 8, CORES * rows), F32),
                vmem((n_chip, keys_local, LANES), jnp.int32),
                vmem((n_kv, n_sub, head_dim, CORES * rows), F32),
                vmem((n_kv, n_sub, head_dim, rows), F32),
                vmem(key_act.shape, F32),
                vmem(key_act.shape, F32),
                vmem((2, half, RUNS * CORES * rows), BF16),
                vmem((2, half, RUNS * CORES * rows), BF16),
                vmem((2,) + key_act.shape, BF16),
                dma((1,)), dma((2 * n_hop, n_kv)), dma((1,)), dma((2 * n_hop, n_kv)),
                dma((4,)), dma((4,)), dma((7,)), dma((5,)),
            ],
            compiler_params=pltpu.CompilerParams(collective_id=0, has_side_effects=True, vmem_limit_bytes=62 * 1024 * 1024),
            cost_estimate=pl.CostEstimate(flops=flops, bytes_accessed=30 * 2 ** 20, transcendentals=0),
        )(key_act, value_act, query.reshape(q5), out_act.reshape(q5), out_grad.reshape(q5), jnp.swapaxes(row_lse, 1, 2), doc_ids.reshape(-1, LANES))
        dq, dk, dv = pl.pallas_call(
            copy_kernel,
            name='results',
            out_shape=tuple(jax.ShapeDtypeStruct(x.shape, x.dtype) for x in (dq, dk, dv)),
            in_specs=[hbm] * 3,
            out_specs=(hbm,) * 3,
            scratch_shapes=[vmem(x.shape, x.dtype) for x in (dq, dk, dv)] + [dma((3 * PIECES,)), dma((3 * PIECES,))],
            cost_estimate=pl.CostEstimate(flops=0, bytes_accessed=2 ** 22, transcendentals=0),
        )(dq, dk, dv)
        return dq.reshape(query.shape), dk, dv

    return jax.shard_map(local_backward, mesh=mesh, in_specs=(q_spec, q_spec, q_spec, lse_spec, kv_spec, kv_spec, P()),
                         out_specs=(q_spec, kv_spec, kv_spec), check_vma=False)
```

```python
import functools
import math

import jax
import jax.numpy as jnp
from jax import lax
from jax.experimental import pallas as pl
from jax.experimental.pallas import tpu as pltpu
from jax.sharding import PartitionSpec as P

MESH = pl.DeviceIdType.MESH
CORES = 2
LANES = 128
SPLIT = 64
PIECES = 4
RUNS = 2
UNROLL = 2
EARLY_ITEMS = 26
ORDER = ('e1 W6 e2 e3 W6 e4 W4 O W8 e5 e6 W4 E0 R60 E1 R61 R50 E2 R51 R40 R41 W10 E3 W8 R30 R31 R20 R21 E4 E5 R10 R11 W4 R00 R01 W2 E6 '
         'T60 T61 T50 T51 T40 T41 T30 T31 T20 T21 T10 T11 F T00 T01')
F32 = jnp.float32
BF16 = jnp.bfloat16


def ring_kernel(cp_size, sub_start, scale, k_in, v_in, q_in, o_in, do_in, lse_in, doc_in, dq_out, dk_out, dv_out,
                kvb, acc, rsb, raw_q, raw_do, raw_o, lse, docs, qn, qt, don, dot, lines, key_doc, dqa, dqr, dko, dvo, pbuf, dsbuf, raw_kv,
                ag_send, ag_recv, rs_send, rs_recv, x_send, x_recv, loc_sem, out_sem):
    n_chip = cp_size // CORES
    n_hop = n_chip - 1
    n_sub, local_len, n_kv, group, head_dim = q_in.shape
    rows = local_len * group
    width = CORES * rows
    key_tile = k_in.shape[0] // 2
    span = local_len * CORES
    sub_len = local_len * cp_size
    keys_local = 2 * key_tile
    own = 2 * n_hop

    me = lax.axis_index('cp')
    chip, core = me // CORES, lax.rem(me, CORES)
    right = lax.rem(me + CORES, cp_size)
    left = lax.rem(me + cp_size - CORES, cp_size)
    sibling = me + 1 - 2 * core
    nbr = (right, left)

    barrier = pltpu.get_barrier_semaphore()
    for peer in (right, left, sibling):
        pl.semaphore_signal(barrier, inc=1, device_id={'cp': peer}, device_id_type=MESH)

    own_kv = [pltpu.make_async_copy(x, raw_kv.at[i], loc_sem.at[5 + i]) for i, x in enumerate((k_in, v_in))]
    local = [pltpu.make_async_copy(a, b, loc_sem.at[i]) for i, (a, b) in enumerate((
        (doc_in, docs), (lse_in, lse), (do_in, raw_do.at[0]), (o_in, raw_o), (q_in, raw_q.at[0])))]
    for c in own_kv:
        c.start()

    @pl.loop(0, n_sub)
    def _(s):
        for h in range(n_kv):
            dqa[h, s] = jnp.zeros(dqa.shape[2:], F32)

    for c in own_kv:
        c.wait()

    def split(h):
        @pl.loop(0, key_tile // SPLIT)
        def _(i):
            r = pl.multiple_of(i * SPLIT, SPLIT)
            for half in range(2):
                for part in range(2):
                    x = raw_kv[part, pl.ds(half * key_tile + r, SPLIT)].astype(F32)
                    kvb[own + half, h, pl.ds(r, SPLIT), part * head_dim:(part + 1) * head_dim] = x[:, h].astype(BF16)

    split(0)
    pl.semaphore_wait(barrier, 3)

    def remote(src, dst, send, recv, peer):
        return pltpu.make_async_remote_copy(src_ref=src, dst_ref=dst, send_sem=send, recv_sem=recv,
                                            device_id={'cp': peer}, device_id_type=MESH)

    def gather(way, k, head, src=None):
        i = way * n_hop + k
        return remote(kvb.at[i, head] if src is None else src, kvb.at[i, head], ag_send.at[0], ag_recv.at[i, head], nbr[way])

    def gather_own(head):
        for j in range(2):
            for way in range(2):
                gather(way, j, head, kvb.at[own + (j + way) % 2, head]).start()

    def pass_on(k, head):
        for way in range(2):
            gather(way, k, head).wait_recv()
            i = way * n_hop + k

            @pl.when(k + 2 < n_hop)
            def _():
                gather(way, k + 2, head, kvb.at[i, head]).start()

    gather_own(0)
    share = [remote(q_in, raw_q.at[1], x_send.at[0], x_recv.at[0], sibling),
             remote(do_in, raw_do.at[1], x_send.at[1], x_recv.at[1], sibling)]
    for c in local + share:
        c.start()
    for h in range(1, n_kv):
        split(h)

    def mine(which):
        return lines.at[:, :, :, pl.ds(which * rows, rows)]

    share_lines = remote(mine(0), mine(1), x_send.at[2], x_recv.at[2], sibling)

    @pl.loop(0, acc.shape[0])
    def _(i):
        for h in range(n_kv):
            acc[i, h] = jnp.zeros(acc.shape[2:], F32)

    pbuf[...] = jnp.zeros(pbuf.shape, BF16)
    dsbuf[...] = jnp.zeros(dsbuf.shape, BF16)
    local[0].wait()
    tiles = keys_local // LANES

    @pl.loop(0, n_chip)
    def _(b):
        for r in range(tiles):
            row = docs[pl.ds((b * CORES + core) * tiles + r, 1), :]
            key_doc[b, r * LANES:(r + 1) * LANES, :] = jnp.broadcast_to(row, (LANES, LANES)).T

    lane = lax.broadcasted_iota(jnp.int32, (8, rows), 1)
    sub = lax.broadcasted_iota(jnp.int32, (8, rows), 0)
    for c in local[1:4]:
        c.wait()

    side = math.gcd(n_sub, 4)

    @pl.loop(0, n_sub // side)
    def _(t):
        for u in range(side):
            s = t * side + u
            rep = jnp.concatenate([lse[s]] * (LANES // local_len), axis=1)
            wide = jnp.take_along_axis(rep, lane // group, axis=1)
            for h in range(n_kv):
                line = jnp.sum(jnp.where(sub - group * h == lane % group, wide, 0.0), axis=0, keepdims=True) * math.log2(math.e)
                prod = raw_do[0, s, :, h].reshape(rows, head_dim).astype(F32) * raw_o[s, :, h].reshape(rows, head_dim).astype(F32)
                total = jnp.broadcast_to(jnp.sum(prod, axis=1, keepdims=True), (rows, LANES)).T
                first = sub_start + s * sub_len + me * local_len
                doc_row = jnp.broadcast_to(docs[pl.ds(first // LANES, 1), :], (8, LANES))
                doc = jnp.take_along_axis(doc_row, lax.rem(first, LANES) + lane // group, axis=1).astype(F32)
                lines[h, s, :, :rows] = jnp.where(sub == 0, line, jnp.where(sub == 1, total[:8, :], doc))

    share_lines.start()

    def spread(c):
        @pl.loop(0, n_sub // RUNS)
        def _(t):
            for u in range(RUNS):
                s = t * RUNS + u
                for h in range(n_kv):
                    for raw, nat, tr in ((raw_q, qn, qt), (raw_do, don, dot)):
                        x = raw[c, s, :, h].reshape(rows, head_dim)
                        nat[h, s, c * rows:(c + 1) * rows, :] = x
                        tr[h, s, :, c * rows:(c + 1) * rows] = x.T

    for c in local[4:]:
        c.wait()
    spread(0)
    pass_on(0, 0)
    for c in share:
        c.wait()
    spread(1)
    share_lines.wait()

    n_run = n_sub // RUNS
    n_early = 2 + min(8, 2 * n_hop)
    n_first = n_early + 2 * n_hop
    n_block = 2 * n_hop + 2
    n_entry = n_first + (n_kv - 1) * n_block

    def place(e):
        first, early = e < n_first, e < n_early
        past = jnp.maximum(e - n_first, 0)
        head = jnp.where(first, 0, 1 + lax.div(past, n_block))
        b = lax.rem(past, n_block)
        mine = jnp.where(first, e, b) < 2
        f = jnp.maximum(jnp.where(early, e - 2, jnp.where(first, e - n_early, b - 2)), 0)
        step = lax.div(f, 2)
        way = f - 2 * step
        k = jnp.where(early, step, n_hop - 1 - step)
        half = jnp.where(mine, jnp.where(first, e, b), lax.rem(k + way, 2))
        slot = jnp.where(mine, own + half, way * n_hop + k)
        hop = lax.div(k, 2) + 1
        key_chip = jnp.where(mine, chip, lax.rem(chip + jnp.where(way == 1, hop, n_chip - hop), n_chip))
        pos0 = (key_chip * CORES + core) * keys_local + half * key_tile
        s_lo = jnp.minimum(lax.div(jnp.maximum(pos0 - sub_start - span * chip - span + sub_len, 0), sub_len * RUNS), n_run - 1)
        return slot, head, key_chip, half, s_lo

    taken, until, n_taken = [], [], jnp.int32(0)
    total = jnp.int32(0)
    for e in range(n_entry):
        n = n_run - place(jnp.int32(e))[4]
        if e < n_early:
            fits = jnp.int32(1) if e < 2 else (total + n <= EARLY_ITEMS).astype(jnp.int32) * taken[-1]
            taken.append(fits)
            n_taken = n_taken + fits
            n = n * fits
        elif e < n_first:
            f = e - n_early
            i_early = 2 + 2 * (n_hop - 1 - f // 2) + f % 2
            if i_early < n_early:
                n = n * (1 - taken[i_early])
        total = total + n
        until.append(total)

    def following(at):
        i, e, j, n = at
        over = j + 1 >= n
        e1 = e + 1
        e1 = jnp.where(e1 == n_taken, n_early, e1)
        f = e1 - n_early
        back = n_hop - 1 - lax.div(jnp.maximum(f, 0), 2)
        odd = lax.rem(jnp.maximum(f, 0), 2)
        inside = (f >= 0) & (f < 2 * n_hop)
        gone = inside & (2 + 2 * back + odd < n_taken)
        both = (odd == 1) | (3 + 2 * back < n_taken)
        e1 = jnp.where(gone, jnp.where(both, n_first, e1 + 1), e1)
        e1 = jnp.minimum(e1, n_entry - 1)
        e, j = jnp.where(over, e1, e), jnp.where(over, 0, j + 1)
        slot, head, key_chip, half, s_lo = place(e)
        i = i + 1
        return (slot, head, (s_lo + j) * RUNS, key_chip, half, (i < total).astype(jnp.int32)), (i, e, j, n_run - s_lo)

    exp_scale = scale * math.log2(math.e)
    k_iota = lax.broadcasted_iota(jnp.int32, (key_tile, width), 0)
    col = lax.broadcasted_iota(jnp.int32, (1, width), 1)
    q_off = sub_start + jnp.where(col < rows, me, sibling) * local_len + lax.rem(col, rows) // group

    def one(now, carry):
        (slot_p, head_p, s_p), (slot, head, s, key_chip, half, live), at = carry
        then, at = following(at)
        k, v = kvb[slot, head, :, :head_dim], kvb[slot, head, :, head_dim:]
        s_t = [jnp.dot(k, qt[head, s + r], preferred_element_type=F32) for r in range(RUNS)]
        dp_t = [jnp.dot(v, dot[head, s + r], preferred_element_type=F32) for r in range(RUNS)]
        p_p, ds_p = pbuf[1 - now], dsbuf[1 - now]
        q_p = qn[head_p, pl.ds(s_p, RUNS)].reshape(RUNS * width, head_dim)
        do_p = don[head_p, pl.ds(s_p, RUNS)].reshape(RUNS * width, head_dim)
        acc[slot_p, head_p, :, head_dim:] += jnp.dot(p_p, do_p, preferred_element_type=F32)
        acc[slot_p, head_p, :, :head_dim] += jnp.dot(ds_p, q_p, preferred_element_type=F32)
        k_t = kvb[slot_p, head_p, :, :head_dim].T
        for r in range(RUNS):
            dqa[head_p, s_p + r] += jnp.dot(k_t, ds_p[:, r * width:(r + 1) * width], preferred_element_type=F32)
        docs_k = key_doc[key_chip, pl.ds(pl.multiple_of(half * key_tile, 8), key_tile), :]
        docs_k = jnp.concatenate([docs_k] * (width // LANES), axis=1)
        pos0 = (key_chip * CORES + core) * keys_local + half * key_tile
        for r in range(RUNS):
            lse_r, delta_r, doc_r = [lines[head, s + r, m:m + 1, :] for m in range(3)]
            last = jnp.where(live == 1, q_off + (s + r) * sub_len - pos0, -1)
            ok = (docs_k == doc_r.astype(jnp.int32)) & (k_iota <= last)
            p = jnp.where(ok, jnp.exp2(s_t[r] * exp_scale - lse_r), 0.0)
            pbuf[now, :, r * width:(r + 1) * width] = p.astype(BF16)
            dsbuf[now, :, r * width:(r + 1) * width] = (p * (dp_t[r] - delta_r)).astype(BF16)
        return (slot, head, s), then, at

    def advance(state, target):
        i, carry = state
        m = jnp.maximum(target - i, 0) // UNROLL

        def step(_, carry):
            for u in range(UNROLL):
                carry = one(u % 2, carry)
            return carry

        return i + m * UNROLL, lax.fori_loop(0, m, step, carry)

    def add(dst, src, head):
        cut = key_tile // 4

        @pl.loop(0, 4)
        def _(i):
            r = pl.ds(pl.multiple_of(i * cut, 8), cut)
            acc[dst, head, r, :] += rsb[src, head, r, :]

    def partial(i, head, peer):
        return remote(acc.at[i, head], rsb.at[i, head], rs_send.at[0], rs_recv.at[i, head], peer)

    half_rows = lambda which: dqa.at[:, :, :, pl.ds(which * rows, rows)]
    swap = remote(half_rows(1), dqr, x_send.at[3], x_recv.at[3], sibling)

    GATHER, SUMS, WORK, OWN, ALL = 0, 1, 2, 3, 63
    steps, arrived = [], [1, 0]
    for word in ORDER.split():
        kind, digits = word[0], word[1:]
        head = 1 if kind in 'ET' else 0
        if arrived[0] < n_hop:
            bound = min(2 * arrived[0] + 1, n_early - 1)
        else:
            bound = n_entry - 1 if arrived[1] == n_hop else n_first + 1
        k = way = items = 0
        if kind in 'eE':
            what, k = GATHER, int(digits)
            arrived[head] = k + 1
        elif kind in 'RT':
            what, k, way = SUMS, int(digits[0]), int(digits[1])
            bound = (n_first + 2 if head else n_early) + 2 * (n_hop - 1 - k) + way
        elif kind == 'O':
            what = OWN
        else:
            what, items = WORK, ALL if kind == 'F' else int(digits)
        steps.append(what + 4 * (k + 16 * (way + 2 * (head + 2 * (items + 64 * bound)))))
    def pick(table, t):
        out = jnp.int32(0)
        for j, x in enumerate(table):
            out = out + jnp.where(t == j, x, 0)
        return out

    def carry_out(t, state):
        number = pick(steps, t)
        what, number = lax.rem(number, 4), lax.div(number, 4)
        k, number = lax.rem(number, 16), lax.div(number, 16)
        way, number = lax.rem(number, 2), lax.div(number, 2)
        head, number = lax.rem(number, 2), lax.div(number, 2)
        items, bound = lax.rem(number, 64), lax.div(number, 64)
        last = pick(until, bound)
        some = jnp.where(items == ALL, last + UNROLL, jnp.minimum(state[0] + items, last))
        state = advance(state, jnp.where(what == SUMS, last + UNROLL, jnp.where(what == WORK, some, state[0])))

        @pl.when(what == GATHER)
        def _():
            pass_on(k, head)

        @pl.when(what == OWN)
        def _():
            gather_own(1)

        @pl.when(items == ALL)
        def _():
            swap.start()

        @pl.when(what == SUMS)
        def _():
            i = way * n_hop + k
            peer = jnp.where(way == 0, left, right)

            @pl.when(k + 2 < n_hop)
            def _():
                partial(i + 2, head, peer).wait_recv()
                add(i, i + 2, head)

            partial(i, head, peer).start()
        return state

    def settle(head, half):
        for k in (1, 0):
            way = (half + k) % 2
            partial(way * n_hop + k, head, nbr[1 - way]).wait_recv()
            add(own + half, way * n_hop + k, head)
        r = slice(half * key_tile, (half + 1) * key_tile)
        dko[r, head, :] = acc[own + half, head, :, :head_dim] * scale
        dvo[r, head, :] = acc[own + half, head, :, head_dim:]

    zero = jnp.int32(0)
    start, at = following((zero - 1, zero, zero - 1, zero + 1))
    lax.fori_loop(0, len(steps), carry_out, (zero, (start[:3], start, at)))
    swap.wait_recv()

    @pl.loop(0, n_sub)
    def _(s):
        for h in range(n_kv):
            x = ((dqa[h, s, :, :rows] + dqr[h, s]) * scale).astype(BF16).T
            raw_q[0, s, :, h] = x.reshape(local_len, group, head_dim)

    puts = [pltpu.make_async_copy(raw_q.at[0], dq_out, out_sem.at[0])]
    puts[0].start()
    for head in range(n_kv - 1):
        for half in range(2):
            settle(head, half)
    for half in range(2):
        settle(n_kv - 1, half)
        r = pl.ds(half * key_tile, key_tile)
        for i, (a, b) in enumerate(((dko, dk_out), (dvo, dv_out))):
            c = pltpu.make_async_copy(a.at[r], b.at[r], out_sem.at[1 + 2 * half + i])
            c.start()
            puts.append(c)
    swap.wait_send()
    moved = pl.ds(0, 2 * n_hop)
    remote(kvb.at[moved], kvb.at[moved], ag_send.at[0], ag_recv.at[0, 0], right).wait_send()
    remote(acc.at[moved], rsb.at[moved], rs_send.at[0], rs_recv.at[0, 0], right).wait_send()
    for c in puts:
        c.wait()


def copy_kernel(a, b, c, a_out, b_out, c_out, a_buf, b_buf, c_buf, in_sem, out_sem):
    moves = []
    for src, buf, dst in ((a, a_buf, a_out), (b, b_buf, b_out), (c, c_buf, c_out)):
        piece = src.shape[0] // PIECES
        for i in range(PIECES):
            r, n = pl.ds(i * piece, piece), len(moves)
            moves.append((pltpu.make_async_copy(src.at[r], buf.at[r], in_sem.at[n]),
                          pltpu.make_async_copy(buf.at[r], dst.at[r], out_sem.at[n])))
    for x, _ in moves:
        x.start()
    for x, y in moves:
        x.wait()
        y.start()
    for _, y in moves:
        y.wait()


def solution(mesh):
    cp_size = mesh.shape['cp']
    q_spec = P(None, 'cp', 'tp', None)
    lse_spec = P(None, 'cp', 'tp')
    kv_spec = P('cp', 'tp', None)

    def local_backward(query, out_act, out_grad, row_lse, key_act, value_act, doc_ids):
        n_sub, local_len, n_heads, head_dim = query.shape
        keys_local, n_kv = key_act.shape[0], key_act.shape[1]
        group = n_heads // n_kv
        sub_start = keys_local * cp_size - n_sub * local_len * cp_size
        rows = local_len * group
        half = keys_local // 2
        n_chip = cp_size // CORES
        n_hop = n_chip - 1
        n_slot = 2 * n_hop + 2
        q5 = (n_sub, local_len, n_kv, group, head_dim)
        scale = head_dim ** -0.5
        flops = 2 * 5 * n_kv * n_sub * 2 * rows * head_dim * keys_local * n_hop
        hbm = pl.BlockSpec(memory_space=pl.ANY)
        dma = pltpu.SemaphoreType.DMA
        vmem = pltpu.VMEM
        dq, dk, dv = pl.pallas_call(
            functools.partial(ring_kernel, cp_size, sub_start, scale),
            name='ring_backward',
            out_shape=(jax.ShapeDtypeStruct(q5, BF16),) + (jax.ShapeDtypeStruct(key_act.shape, F32),) * 2,
            in_specs=[hbm] * 7,
            out_specs=(hbm,) * 3,
            scratch_shapes=[
                vmem((n_slot, n_kv, half, 2 * head_dim), BF16),
                vmem((n_slot, n_kv, half, 2 * head_dim), F32),
                vmem((2 * n_hop, n_kv, half, 2 * head_dim), F32),
                vmem((CORES,) + q5, BF16),
                vmem((CORES,) + q5, BF16),
                vmem(q5, BF16),
                vmem((n_sub, n_heads, local_len), F32),
                vmem((doc_ids.shape[0] // LANES, LANES), jnp.int32),
                vmem((n_kv, n_sub, CORES * rows, head_dim), BF16),
                vmem((n_kv, n_sub, head_dim, CORES * rows), BF16),
                vmem((n_kv, n_sub, CORES * rows, head_dim), BF16),
                vmem((n_kv, n_sub, head_dim, CORES * rows), BF16),
                vmem((n_kv, n_sub, 8, CORES * rows), F32),
                vmem((n_chip, keys_local, LANES), jnp.int32),
                vmem((n_kv, n_sub, head_dim, CORES * rows), F32),
                vmem((n_kv, n_sub, head_dim, rows), F32),
                vmem(key_act.shape, F32),
                vmem(key_act.shape, F32),
                vmem((2, half, RUNS * CORES * rows), BF16),
                vmem((2, half, RUNS * CORES * rows), BF16),
                vmem((2,) + key_act.shape, BF16),
                dma((1,)), dma((2 * n_hop, n_kv)), dma((1,)), dma((2 * n_hop, n_kv)),
                dma((4,)), dma((4,)), dma((7,)), dma((5,)),
            ],
            compiler_params=pltpu.CompilerParams(collective_id=0, has_side_effects=True, vmem_limit_bytes=62 * 1024 * 1024),
            cost_estimate=pl.CostEstimate(flops=flops, bytes_accessed=30 * 2 ** 20, transcendentals=0),
        )(key_act, value_act, query.reshape(q5), out_act.reshape(q5), out_grad.reshape(q5), jnp.swapaxes(row_lse, 1, 2), doc_ids.reshape(-1, LANES))
        dq, dk, dv = pl.pallas_call(
            copy_kernel,
            name='results',
            out_shape=tuple(jax.ShapeDtypeStruct(x.shape, x.dtype) for x in (dq, dk, dv)),
            in_specs=[hbm] * 3,
            out_specs=(hbm,) * 3,
            scratch_shapes=[vmem(x.shape, x.dtype) for x in (dq, dk, dv)] + [dma((3 * PIECES,)), dma((3 * PIECES,))],
            cost_estimate=pl.CostEstimate(flops=0, bytes_accessed=2 ** 22, transcendentals=0),
        )(dq, dk, dv)
        return dq.reshape(query.shape), dk, dv

    return jax.shard_map(local_backward, mesh=mesh, in_specs=(q_spec, q_spec, q_spec, lse_spec, kv_spec, kv_spec, P()),
                         out_specs=(q_spec, kv_spec, kv_spec), check_vma=False)
```

```python
import functools
import math

import jax
import jax.numpy as jnp
from jax import lax
from jax.experimental import pallas as pl
from jax.experimental.pallas import tpu as pltpu
from jax.sharding import PartitionSpec as P

MESH = pl.DeviceIdType.MESH
CORES = 2
LANES = 128
SPLIT = 64
PIECES = 8
RUNS = 2
UNROLL = 2
EARLY_ITEMS = 26
ORDER = ('e1 W6 e2 e3 W6 e4 W4 O W8 e5 e6 W4 E0 R60 E1 R61 R50 E2 R51 R40 R41 W10 E3 W8 R30 R31 R20 R21 E4 E5 R10 R11 W4 R00 R01 W2 E6 '
         'T60 T61 T50 T51 T40 T41 T30 T31 T20 T21 T10 T11 F T00 T01')
F32 = jnp.float32
BF16 = jnp.bfloat16


def ring_kernel(cp_size, sub_start, scale, k_in, v_in, q_in, o_in, do_in, lse_in, doc_in, dq_out, dk_out, dv_out,
                kvb, acc, rsb, raw_q, raw_do, raw_o, lse, docs, qn, qt, don, dot, lines, key_doc, dqa, dqr, dko, dvo, pbuf, dsbuf, raw_kv,
                ag_send, ag_recv, rs_send, rs_recv, x_send, x_recv, loc_sem, out_sem):
    n_chip = cp_size // CORES
    n_hop = n_chip - 1
    n_sub, local_len, n_kv, group, head_dim = q_in.shape
    rows = local_len * group
    width = CORES * rows
    key_tile = k_in.shape[0] // 2
    span = local_len * CORES
    sub_len = local_len * cp_size
    keys_local = 2 * key_tile
    own = 2 * n_hop

    me = lax.axis_index('cp')
    chip, core = me // CORES, lax.rem(me, CORES)
    right = lax.rem(me + CORES, cp_size)
    left = lax.rem(me + cp_size - CORES, cp_size)
    sibling = me + 1 - 2 * core
    nbr = (right, left)

    barrier = pltpu.get_barrier_semaphore()
    for peer in (right, left, sibling):
        pl.semaphore_signal(barrier, inc=1, device_id={'cp': peer}, device_id_type=MESH)

    halves = [pl.ds(half * key_tile, key_tile) for half in range(2)]
    own_kv = [[pltpu.make_async_copy(x.at[r], raw_kv.at[i, r], loc_sem.at[5 + 2 * half + i]) for i, x in enumerate((k_in, v_in))]
              for half, r in enumerate(halves)]
    local = [pltpu.make_async_copy(a, b, loc_sem.at[i]) for i, (a, b) in enumerate((
        (doc_in, docs), (lse_in, lse), (do_in, raw_do.at[0]), (o_in, raw_o), (q_in, raw_q.at[0])))]
    for c in own_kv[0] + own_kv[1]:
        c.start()

    @pl.loop(0, n_sub)
    def _(s):
        for h in range(n_kv):
            dqa[h, s] = jnp.zeros(dqa.shape[2:], F32)

    def split(h, half):
        @pl.loop(0, key_tile // SPLIT)
        def _(i):
            r = pl.multiple_of(i * SPLIT, SPLIT)
            for part in range(2):
                x = raw_kv[part, pl.ds(half * key_tile + r, SPLIT)].astype(F32)
                kvb[own + half, h, pl.ds(r, SPLIT), part * head_dim:(part + 1) * head_dim] = x[:, h].astype(BF16)

    for half in range(2):
        for c in own_kv[half]:
            c.wait()
        split(0, half)
    pl.semaphore_wait(barrier, 3)

    def remote(src, dst, send, recv, peer):
        return pltpu.make_async_remote_copy(src_ref=src, dst_ref=dst, send_sem=send, recv_sem=recv,
                                            device_id={'cp': peer}, device_id_type=MESH)

    def gather(way, k, head, src=None):
        i = way * n_hop + k
        return remote(kvb.at[i, head] if src is None else src, kvb.at[i, head], ag_send.at[0], ag_recv.at[i, head], nbr[way])

    def gather_own(head):
        for j in range(2):
            for way in range(2):
                gather(way, j, head, kvb.at[own + (j + way) % 2, head]).start()

    def pass_on(k, head):
        for way in range(2):
            gather(way, k, head).wait_recv()
            i = way * n_hop + k

            @pl.when(k + 2 < n_hop)
            def _():
                gather(way, k + 2, head, kvb.at[i, head]).start()

    gather_own(0)
    share = [remote(q_in, raw_q.at[1], x_send.at[0], x_recv.at[0], sibling),
             remote(do_in, raw_do.at[1], x_send.at[1], x_recv.at[1], sibling)]
    for c in local + share:
        c.start()
    for h in range(1, n_kv):
        for half in range(2):
            split(h, half)

    def mine(which):
        return lines.at[:, :, :, pl.ds(which * rows, rows)]

    share_lines = remote(mine(0), mine(1), x_send.at[2], x_recv.at[2], sibling)

    @pl.loop(0, acc.shape[0])
    def _(i):
        for h in range(n_kv):
            acc[i, h] = jnp.zeros(acc.shape[2:], F32)

    pbuf[...] = jnp.zeros(pbuf.shape, BF16)
    dsbuf[...] = jnp.zeros(dsbuf.shape, BF16)
    local[0].wait()
    tiles = keys_local // LANES

    @pl.loop(0, n_chip)
    def _(b):
        for r in range(tiles):
            row = docs[pl.ds((b * CORES + core) * tiles + r, 1), :]
            key_doc[b, r * LANES:(r + 1) * LANES, :] = jnp.broadcast_to(row, (LANES, LANES)).T

    lane = lax.broadcasted_iota(jnp.int32, (8, rows), 1)
    sub = lax.broadcasted_iota(jnp.int32, (8, rows), 0)
    for c in local[1:4]:
        c.wait()

    side = math.gcd(n_sub, 4)

    @pl.loop(0, n_sub // side)
    def _(t):
        for u in range(side):
            s = t * side + u
            rep = jnp.concatenate([lse[s]] * (LANES // local_len), axis=1)
            wide = jnp.take_along_axis(rep, lane // group, axis=1)
            for h in range(n_kv):
                line = jnp.sum(jnp.where(sub - group * h == lane % group, wide, 0.0), axis=0, keepdims=True) * math.log2(math.e)
                prod = raw_do[0, s, :, h].reshape(rows, head_dim).astype(F32) * raw_o[s, :, h].reshape(rows, head_dim).astype(F32)
                total = jnp.broadcast_to(jnp.sum(prod, axis=1, keepdims=True), (rows, LANES)).T
                first = sub_start + s * sub_len + me * local_len
                doc_row = jnp.broadcast_to(docs[pl.ds(first // LANES, 1), :], (8, LANES))
                doc = jnp.take_along_axis(doc_row, lax.rem(first, LANES) + lane // group, axis=1).astype(F32)
                lines[h, s, :, :rows] = jnp.where(sub == 0, line, jnp.where(sub == 1, total[:8, :], doc))

    share_lines.start()

    def spread(c):
        @pl.loop(0, n_sub // RUNS)
        def _(t):
            for u in range(RUNS):
                s = t * RUNS + u
                for h in range(n_kv):
                    for raw, nat, tr in ((raw_q, qn, qt), (raw_do, don, dot)):
                        x = raw[c, s, :, h].reshape(rows, head_dim)
                        nat[h, s, c * rows:(c + 1) * rows, :] = x
                        tr[h, s, :, c * rows:(c + 1) * rows] = x.T

    for c in local[4:]:
        c.wait()
    spread(0)
    pass_on(0, 0)
    for c in share:
        c.wait()
    spread(1)
    share_lines.wait()

    n_run = n_sub // RUNS
    n_early = 2 + min(8, 2 * n_hop)
    n_first = n_early + 2 * n_hop
    n_block = 2 * n_hop + 2
    n_entry = n_first + (n_kv - 1) * n_block

    def place(e):
        first, early = e < n_first, e < n_early
        past = jnp.maximum(e - n_first, 0)
        head = jnp.where(first, 0, 1 + lax.div(past, n_block))
        b = lax.rem(past, n_block)
        mine = jnp.where(first, e, b) < 2
        f = jnp.maximum(jnp.where(early, e - 2, jnp.where(first, e - n_early, b - 2)), 0)
        step = lax.div(f, 2)
        way = f - 2 * step
        k = jnp.where(early, step, n_hop - 1 - step)
        half = jnp.where(mine, jnp.where(first, e, b), lax.rem(k + way, 2))
        slot = jnp.where(mine, own + half, way * n_hop + k)
        hop = lax.div(k, 2) + 1
        key_chip = jnp.where(mine, chip, lax.rem(chip + jnp.where(way == 1, hop, n_chip - hop), n_chip))
        pos0 = (key_chip * CORES + core) * keys_local + half * key_tile
        s_lo = jnp.minimum(lax.div(jnp.maximum(pos0 - sub_start - span * chip - span + sub_len, 0), sub_len * RUNS), n_run - 1)
        return slot, head, key_chip, half, s_lo

    taken, until, n_taken = [], [], jnp.int32(0)
    total = jnp.int32(0)
    for e in range(n_entry):
        n = n_run - place(jnp.int32(e))[4]
        if e < n_early:
            fits = jnp.int32(1) if e < 2 else (total + n <= EARLY_ITEMS).astype(jnp.int32) * taken[-1]
            taken.append(fits)
            n_taken = n_taken + fits
            n = n * fits
        elif e < n_first:
            f = e - n_early
            i_early = 2 + 2 * (n_hop - 1 - f // 2) + f % 2
            if i_early < n_early:
                n = n * (1 - taken[i_early])
        total = total + n
        until.append(total)

    def following(at):
        i, e, j, n = at
        over = j + 1 >= n
        e1 = e + 1
        e1 = jnp.where(e1 == n_taken, n_early, e1)
        f = e1 - n_early
        back = n_hop - 1 - lax.div(jnp.maximum(f, 0), 2)
        odd = lax.rem(jnp.maximum(f, 0), 2)
        inside = (f >= 0) & (f < 2 * n_hop)
        gone = inside & (2 + 2 * back + odd < n_taken)
        both = (odd == 1) | (3 + 2 * back < n_taken)
        e1 = jnp.where(gone, jnp.where(both, n_first, e1 + 1), e1)
        e1 = jnp.minimum(e1, n_entry - 1)
        e, j = jnp.where(over, e1, e), jnp.where(over, 0, j + 1)
        slot, head, key_chip, half, s_lo = place(e)
        i = i + 1
        return (slot, head, (s_lo + j) * RUNS, key_chip, half, (i < total).astype(jnp.int32)), (i, e, j, n_run - s_lo)

    exp_scale = scale * math.log2(math.e)
    k_iota = lax.broadcasted_iota(jnp.int32, (key_tile, width), 0)
    col = lax.broadcasted_iota(jnp.int32, (1, width), 1)
    q_off = sub_start + jnp.where(col < rows, me, sibling) * local_len + lax.rem(col, rows) // group

    def one(now, carry):
        (slot_p, head_p, s_p), (slot, head, s, key_chip, half, live), at = carry
        then, at = following(at)
        k, v = kvb[slot, head, :, :head_dim], kvb[slot, head, :, head_dim:]
        s_t = [jnp.dot(k, qt[head, s + r], preferred_element_type=F32) for r in range(RUNS)]
        dp_t = [jnp.dot(v, dot[head, s + r], preferred_element_type=F32) for r in range(RUNS)]
        p_p, ds_p = pbuf[1 - now], dsbuf[1 - now]
        q_p = qn[head_p, pl.ds(s_p, RUNS)].reshape(RUNS * width, head_dim)
        do_p = don[head_p, pl.ds(s_p, RUNS)].reshape(RUNS * width, head_dim)
        acc[slot_p, head_p, :, head_dim:] += jnp.dot(p_p, do_p, preferred_element_type=F32)
        acc[slot_p, head_p, :, :head_dim] += jnp.dot(ds_p, q_p, preferred_element_type=F32)
        k_t = kvb[slot_p, head_p, :, :head_dim].T
        for r in range(RUNS):
            dqa[head_p, s_p + r] += jnp.dot(k_t, ds_p[:, r * width:(r + 1) * width], preferred_element_type=F32)
        docs_k = key_doc[key_chip, pl.ds(pl.multiple_of(half * key_tile, 8), key_tile), :]
        docs_k = jnp.concatenate([docs_k] * (width // LANES), axis=1)
        pos0 = (key_chip * CORES + core) * keys_local + half * key_tile
        for r in range(RUNS):
            lse_r, delta_r, doc_r = [lines[head, s + r, m:m + 1, :] for m in range(3)]
            last = jnp.where(live == 1, q_off + (s + r) * sub_len - pos0, -1)
            ok = (docs_k == doc_r.astype(jnp.int32)) & (k_iota <= last)
            p = jnp.where(ok, jnp.exp2(s_t[r] * exp_scale - lse_r), 0.0)
            pbuf[now, :, r * width:(r + 1) * width] = p.astype(BF16)
            dsbuf[now, :, r * width:(r + 1) * width] = (p * (dp_t[r] - delta_r)).astype(BF16)
        return (slot, head, s), then, at

    def advance(state, target):
        i, carry = state
        m = jnp.maximum(target - i, 0) // UNROLL

        def step(_, carry):
            for u in range(UNROLL):
                carry = one(u % 2, carry)
            return carry

        return i + m * UNROLL, lax.fori_loop(0, m, step, carry)

    def add(dst, src, head):
        cut = key_tile // 4

        @pl.loop(0, 4)
        def _(i):
            r = pl.ds(pl.multiple_of(i * cut, 8), cut)
            acc[dst, head, r, :] += rsb[src, head, r, :]

    def partial(i, head, peer):
        return remote(acc.at[i, head], rsb.at[i, head], rs_send.at[0], rs_recv.at[i, head], peer)

    half_rows = lambda which: dqa.at[:, :, :, pl.ds(which * rows, rows)]
    swap = remote(half_rows(1), dqr, x_send.at[3], x_recv.at[3], sibling)

    GATHER, SUMS, WORK, OWN, ALL = 0, 1, 2, 3, 63
    steps, arrived = [], [1, 0]
    for word in ORDER.split():
        kind, digits = word[0], word[1:]
        head = 1 if kind in 'ET' else 0
        if arrived[0] < n_hop:
            bound = min(2 * arrived[0] + 1, n_early - 1)
        else:
            bound = n_entry - 1 if arrived[1] == n_hop else n_first + 1
        k = way = items = 0
        if kind in 'eE':
            what, k = GATHER, int(digits)
            arrived[head] = k + 1
        elif kind in 'RT':
            what, k, way = SUMS, int(digits[0]), int(digits[1])
            bound = (n_first + 2 if head else n_early) + 2 * (n_hop - 1 - k) + way
        elif kind == 'O':
            what = OWN
        else:
            what, items = WORK, ALL if kind == 'F' else int(digits)
        steps.append(what + 4 * (k + 16 * (way + 2 * (head + 2 * (items + 64 * bound)))))
    def pick(table, t):
        out = jnp.int32(0)
        for j, x in enumerate(table):
            out = out + jnp.where(t == j, x, 0)
        return out

    def carry_out(t, state):
        number = pick(steps, t)
        what, number = lax.rem(number, 4), lax.div(number, 4)
        k, number = lax.rem(number, 16), lax.div(number, 16)
        way, number = lax.rem(number, 2), lax.div(number, 2)
        head, number = lax.rem(number, 2), lax.div(number, 2)
        items, bound = lax.rem(number, 64), lax.div(number, 64)
        last = pick(until, bound)
        some = jnp.where(items == ALL, last + UNROLL, jnp.minimum(state[0] + items, last))
        state = advance(state, jnp.where(what == SUMS, last + UNROLL, jnp.where(what == WORK, some, state[0])))

        @pl.when(what == GATHER)
        def _():
            pass_on(k, head)

        @pl.when(what == OWN)
        def _():
            gather_own(1)

        @pl.when(items == ALL)
        def _():
            swap.start()

        @pl.when(what == SUMS)
        def _():
            i = way * n_hop + k
            peer = jnp.where(way == 0, left, right)

            @pl.when(k + 2 < n_hop)
            def _():
                partial(i + 2, head, peer).wait_recv()
                add(i, i + 2, head)

            partial(i, head, peer).start()
        return state

    def settle(head, half):
        for k in (1, 0):
            way = (half + k) % 2
            partial(way * n_hop + k, head, nbr[1 - way]).wait_recv()
            add(own + half, way * n_hop + k, head)
        r = slice(half * key_tile, (half + 1) * key_tile)
        dko[r, head, :] = acc[own + half, head, :, :head_dim] * scale
        dvo[r, head, :] = acc[own + half, head, :, head_dim:]

    zero = jnp.int32(0)
    start, at = following((zero - 1, zero, zero - 1, zero + 1))
    lax.fori_loop(0, len(steps), carry_out, (zero, (start[:3], start, at)))
    swap.wait_recv()

    @pl.loop(0, n_sub)
    def _(s):
        for h in range(n_kv):
            x = ((dqa[h, s, :, :rows] + dqr[h, s]) * scale).astype(BF16).T
            raw_q[0, s, :, h] = x.reshape(local_len, group, head_dim)

    puts = [pltpu.make_async_copy(raw_q.at[0], dq_out, out_sem.at[0])]
    puts[0].start()
    for head in range(n_kv - 1):
        for half in range(2):
            settle(head, half)
    for half in range(2):
        settle(n_kv - 1, half)
        r = pl.ds(half * key_tile, key_tile)
        for i, (a, b) in enumerate(((dko, dk_out), (dvo, dv_out))):
            c = pltpu.make_async_copy(a.at[r], b.at[r], out_sem.at[1 + 2 * half + i])
            c.start()
            puts.append(c)
    swap.wait_send()
    moved = pl.ds(0, 2 * n_hop)
    remote(kvb.at[moved], kvb.at[moved], ag_send.at[0], ag_recv.at[0, 0], right).wait_send()
    remote(acc.at[moved], rsb.at[moved], rs_send.at[0], rs_recv.at[0, 0], right).wait_send()
    for c in puts:
        c.wait()


def copy_kernel(a, b, c, a_out, b_out, c_out, a_buf, b_buf, c_buf, in_sem, out_sem):
    moves = []
    for src, buf, dst in ((a, a_buf, a_out), (b, b_buf, b_out), (c, c_buf, c_out)):
        piece = src.shape[0] // PIECES
        for i in range(PIECES):
            r, n = pl.ds(i * piece, piece), len(moves)
            moves.append((pltpu.make_async_copy(src.at[r], buf.at[r], in_sem.at[n]),
                          pltpu.make_async_copy(buf.at[r], dst.at[r], out_sem.at[n])))
    for x, _ in moves:
        x.start()
    for x, y in moves:
        x.wait()
        y.start()
    for _, y in moves:
        y.wait()


def solution(mesh):
    cp_size = mesh.shape['cp']
    q_spec = P(None, 'cp', 'tp', None)
    lse_spec = P(None, 'cp', 'tp')
    kv_spec = P('cp', 'tp', None)

    def local_backward(query, out_act, out_grad, row_lse, key_act, value_act, doc_ids):
        n_sub, local_len, n_heads, head_dim = query.shape
        keys_local, n_kv = key_act.shape[0], key_act.shape[1]
        group = n_heads // n_kv
        sub_start = keys_local * cp_size - n_sub * local_len * cp_size
        rows = local_len * group
        half = keys_local // 2
        n_chip = cp_size // CORES
        n_hop = n_chip - 1
        n_slot = 2 * n_hop + 2
        q5 = (n_sub, local_len, n_kv, group, head_dim)
        scale = head_dim ** -0.5
        flops = 2 * 5 * n_kv * n_sub * 2 * rows * head_dim * keys_local * n_hop
        hbm = pl.BlockSpec(memory_space=pl.ANY)
        dma = pltpu.SemaphoreType.DMA
        vmem = pltpu.VMEM
        dq, dk, dv = pl.pallas_call(
            functools.partial(ring_kernel, cp_size, sub_start, scale),
            name='ring_backward',
            out_shape=(jax.ShapeDtypeStruct(q5, BF16),) + (jax.ShapeDtypeStruct(key_act.shape, F32),) * 2,
            in_specs=[hbm] * 7,
            out_specs=(hbm,) * 3,
            scratch_shapes=[
                vmem((n_slot, n_kv, half, 2 * head_dim), BF16),
                vmem((n_slot, n_kv, half, 2 * head_dim), F32),
                vmem((2 * n_hop, n_kv, half, 2 * head_dim), F32),
                vmem((CORES,) + q5, BF16),
                vmem((CORES,) + q5, BF16),
                vmem(q5, BF16),
                vmem((n_sub, n_heads, local_len), F32),
                vmem((doc_ids.shape[0] // LANES, LANES), jnp.int32),
                vmem((n_kv, n_sub, CORES * rows, head_dim), BF16),
                vmem((n_kv, n_sub, head_dim, CORES * rows), BF16),
                vmem((n_kv, n_sub, CORES * rows, head_dim), BF16),
                vmem((n_kv, n_sub, head_dim, CORES * rows), BF16),
                vmem((n_kv, n_sub, 8, CORES * rows), F32),
                vmem((n_chip, keys_local, LANES), jnp.int32),
                vmem((n_kv, n_sub, head_dim, CORES * rows), F32),
                vmem((n_kv, n_sub, head_dim, rows), F32),
                vmem(key_act.shape, F32),
                vmem(key_act.shape, F32),
                vmem((2, half, RUNS * CORES * rows), BF16),
                vmem((2, half, RUNS * CORES * rows), BF16),
                vmem((2,) + key_act.shape, BF16),
                dma((1,)), dma((2 * n_hop, n_kv)), dma((1,)), dma((2 * n_hop, n_kv)),
                dma((4,)), dma((4,)), dma((9,)), dma((5,)),
            ],
            compiler_params=pltpu.CompilerParams(collective_id=0, has_side_effects=True, vmem_limit_bytes=62 * 1024 * 1024),
            cost_estimate=pl.CostEstimate(flops=flops, bytes_accessed=30 * 2 ** 20, transcendentals=0),
        )(key_act, value_act, query.reshape(q5), out_act.reshape(q5), out_grad.reshape(q5), jnp.swapaxes(row_lse, 1, 2), doc_ids.reshape(-1, LANES))
        dq, dk, dv = pl.pallas_call(
            copy_kernel,
            name='results',
            out_shape=tuple(jax.ShapeDtypeStruct(x.shape, x.dtype) for x in (dq, dk, dv)),
            in_specs=[hbm] * 3,
            out_specs=(hbm,) * 3,
            scratch_shapes=[vmem(x.shape, x.dtype) for x in (dq, dk, dv)] + [dma((3 * PIECES,)), dma((3 * PIECES,))],
            cost_estimate=pl.CostEstimate(flops=0, bytes_accessed=2 ** 22, transcendentals=0),
        )(dq, dk, dv)
        return dq.reshape(query.shape), dk, dv

    return jax.shard_map(local_backward, mesh=mesh, in_specs=(q_spec, q_spec, q_spec, lse_spec, kv_spec, kv_spec, P()),
                         out_specs=(q_spec, kv_spec, kv_spec), check_vma=False)
```

```python
import functools
import math

import jax
import jax.numpy as jnp
from jax import lax
from jax.experimental import pallas as pl
from jax.experimental.pallas import tpu as pltpu
from jax.sharding import PartitionSpec as P

MESH = pl.DeviceIdType.MESH
CORES = 2
LANES = 128
SPLIT = 64
PIECES = 4
RUNS = 2
UNROLL = 2
EARLY_ITEMS = 26
ORDER = ('e1 W6 e2 e3 W6 e4 W4 O W8 e5 e6 W4 E0 R60 E1 R61 R50 E2 R51 R40 R41 W10 E3 W8 R30 R31 R20 R21 E4 E5 R10 R11 W4 R00 R01 W2 E6 '
         'T60 T61 T50 T51 T40 T41 T30 T31 T20 T21 T10 T11 F T00 T01')
F32 = jnp.float32
BF16 = jnp.bfloat16


def ring_kernel(cp_size, sub_start, scale, k_in, v_in, q_in, o_in, do_in, lse_in, doc_in, dq_out, dk_out, dv_out,
                kvb, acc, rsb, raw_q, raw_do, raw_o, lse, docs, qn, qt, don, dot, lines, key_doc, dqa, dqr, dko, dvo, pbuf, dsbuf, raw_kv,
                ag_send, ag_recv, rs_send, rs_recv, x_send, x_recv, loc_sem, out_sem):
    n_chip = cp_size // CORES
    n_hop = n_chip - 1
    n_sub, local_len, n_kv, group, head_dim = q_in.shape
    rows = local_len * group
    width = CORES * rows
    key_tile = k_in.shape[0] // 2
    span = local_len * CORES
    sub_len = local_len * cp_size
    keys_local = 2 * key_tile
    own = 2 * n_hop

    me = lax.axis_index('cp')
    chip, core = me // CORES, lax.rem(me, CORES)
    right = lax.rem(me + CORES, cp_size)
    left = lax.rem(me + cp_size - CORES, cp_size)
    sibling = me + 1 - 2 * core
    nbr = (right, left)

    barrier = pltpu.get_barrier_semaphore()
    for peer in (right, left, sibling):
        pl.semaphore_signal(barrier, inc=1, device_id={'cp': peer}, device_id_type=MESH)

    own_kv = [pltpu.make_async_copy(x, raw_kv.at[i], loc_sem.at[5 + i]) for i, x in enumerate((k_in, v_in))]
    local = [pltpu.make_async_copy(a, b, loc_sem.at[i]) for i, (a, b) in enumerate((
        (doc_in, docs), (lse_in, lse), (do_in, raw_do.at[0]), (o_in, raw_o), (q_in, raw_q.at[0])))]
    for c in own_kv:
        c.start()

    @pl.loop(0, n_sub)
    def _(s):
        for h in range(n_kv):
            dqa[h, s] = jnp.zeros(dqa.shape[2:], F32)

    for c in own_kv:
        c.wait()

    def split(h):
        @pl.loop(0, key_tile // SPLIT)
        def _(i):
            r = pl.multiple_of(i * SPLIT, SPLIT)
            for half in range(2):
                for part in range(2):
                    x = raw_kv[part, pl.ds(half * key_tile + r, SPLIT)].astype(F32)
                    kvb[own + half, h, pl.ds(r, SPLIT), part * head_dim:(part + 1) * head_dim] = x[:, h].astype(BF16)

    split(0)
    pl.semaphore_wait(barrier, 3)

    def remote(src, dst, send, recv, peer):
        return pltpu.make_async_remote_copy(src_ref=src, dst_ref=dst, send_sem=send, recv_sem=recv,
                                            device_id={'cp': peer}, device_id_type=MESH)

    def gather(way, k, head, src=None):
        i = way * n_hop + k
        return remote(kvb.at[i, head] if src is None else src, kvb.at[i, head], ag_send.at[0], ag_recv.at[i, head], nbr[way])

    def gather_own(head):
        for j in range(2):
            for way in range(2):
                gather(way, j, head, kvb.at[own + (j + way) % 2, head]).start()

    def pass_on(k, head):
        for way in range(2):
            gather(way, k, head).wait_recv()
            i = way * n_hop + k

            @pl.when(k + 2 < n_hop)
            def _():
                gather(way, k + 2, head, kvb.at[i, head]).start()

    gather_own(0)
    share = [remote(q_in, raw_q.at[1], x_send.at[0], x_recv.at[0], sibling),
             remote(do_in, raw_do.at[1], x_send.at[1], x_recv.at[1], sibling)]
    for c in local + share:
        c.start()
    for h in range(1, n_kv):
        split(h)

    def mine(which):
        return lines.at[:, :, :, pl.ds(which * rows, rows)]

    share_lines = remote(mine(0), mine(1), x_send.at[2], x_recv.at[2], sibling)

    @pl.loop(0, acc.shape[0])
    def _(i):
        for h in range(n_kv):
            acc[i, h] = jnp.zeros(acc.shape[2:], F32)

    pbuf[...] = jnp.zeros(pbuf.shape, BF16)
    dsbuf[...] = jnp.zeros(dsbuf.shape, BF16)
    local[0].wait()
    tiles = keys_local // LANES

    @pl.loop(0, n_chip)
    def _(b):
        for r in range(tiles):
            row = docs[pl.ds((b * CORES + core) * tiles + r, 1), :]
            key_doc[b, r * LANES:(r + 1) * LANES, :] = jnp.broadcast_to(row, (LANES, LANES)).T

    lane = lax.broadcasted_iota(jnp.int32, (8, rows), 1)
    sub = lax.broadcasted_iota(jnp.int32, (8, rows), 0)
    for c in local[1:4]:
        c.wait()

    side = math.gcd(n_sub, 4)

    @pl.loop(0, n_sub // side)
    def _(t):
        for u in range(side):
            s = t * side + u
            rep = jnp.concatenate([lse[s]] * (LANES // local_len), axis=1)
            wide = jnp.take_along_axis(rep, lane // group, axis=1)
            for h in range(n_kv):
                line = jnp.sum(jnp.where(sub - group * h == lane % group, wide, 0.0), axis=0, keepdims=True) * math.log2(math.e)
                prod = raw_do[0, s, :, h].reshape(rows, head_dim).astype(F32) * raw_o[s, :, h].reshape(rows, head_dim).astype(F32)
                total = jnp.broadcast_to(jnp.sum(prod, axis=1, keepdims=True), (rows, LANES)).T
                first = sub_start + s * sub_len + me * local_len
                doc_row = jnp.broadcast_to(docs[pl.ds(first // LANES, 1), :], (8, LANES))
                doc = jnp.take_along_axis(doc_row, lax.rem(first, LANES) + lane // group, axis=1).astype(F32)
                lines[h, s, :, :rows] = jnp.where(sub == 0, line, jnp.where(sub == 1, total[:8, :], doc))

    share_lines.start()

    def spread(c):
        @pl.loop(0, n_sub // RUNS)
        def _(t):
            for u in range(RUNS):
                s = t * RUNS + u
                for h in range(n_kv):
                    for raw, nat, tr in ((raw_q, qn, qt), (raw_do, don, dot)):
                        x = raw[c, s, :, h].reshape(rows, head_dim)
                        nat[h, s, c * rows:(c + 1) * rows, :] = x
                        tr[h, s, :, c * rows:(c + 1) * rows] = x.T

    for c in local[4:]:
        c.wait()
    spread(0)
    pass_on(0, 0)
    for c in share:
        c.wait()
    spread(1)
    share_lines.wait()

    n_run = n_sub // RUNS
    n_early = 2 + min(8, 2 * n_hop)
    n_first = n_early + 2 * n_hop
    n_block = 2 * n_hop + 2
    n_entry = n_first + (n_kv - 1) * n_block

    def place(e):
        first, early = e < n_first, e < n_early
        past = jnp.maximum(e - n_first, 0)
        head = jnp.where(first, 0, 1 + lax.div(past, n_block))
        b = lax.rem(past, n_block)
        mine = jnp.where(first, e, b) < 2
        f = jnp.maximum(jnp.where(early, e - 2, jnp.where(first, e - n_early, b - 2)), 0)
        step = lax.div(f, 2)
        way = f - 2 * step
        k = jnp.where(early, step, n_hop - 1 - step)
        half = jnp.where(mine, jnp.where(first, e, b), lax.rem(k + way, 2))
        slot = jnp.where(mine, own + half, way * n_hop + k)
        hop = lax.div(k, 2) + 1
        key_chip = jnp.where(mine, chip, lax.rem(chip + jnp.where(way == 1, hop, n_chip - hop), n_chip))
        pos0 = (key_chip * CORES + core) * keys_local + half * key_tile
        s_lo = jnp.minimum(lax.div(jnp.maximum(pos0 - sub_start - span * chip - span + sub_len, 0), sub_len * RUNS), n_run - 1)
        return slot, head, key_chip, half, s_lo

    taken, until, n_taken = [], [], jnp.int32(0)
    total = jnp.int32(0)
    for e in range(n_entry):
        n = n_run - place(jnp.int32(e))[4]
        if e < n_early:
            fits = jnp.int32(1) if e < 2 else (total + n <= EARLY_ITEMS).astype(jnp.int32) * taken[-1]
            taken.append(fits)
            n_taken = n_taken + fits
            n = n * fits
        elif e < n_first:
            f = e - n_early
            i_early = 2 + 2 * (n_hop - 1 - f // 2) + f % 2
            if i_early < n_early:
                n = n * (1 - taken[i_early])
        total = total + n
        until.append(total)

    def following(at):
        i, e, j, n = at
        over = j + 1 >= n
        e1 = e + 1
        e1 = jnp.where(e1 == n_taken, n_early, e1)
        f = e1 - n_early
        back = n_hop - 1 - lax.div(jnp.maximum(f, 0), 2)
        odd = lax.rem(jnp.maximum(f, 0), 2)
        inside = (f >= 0) & (f < 2 * n_hop)
        gone = inside & (2 + 2 * back + odd < n_taken)
        both = (odd == 1) | (3 + 2 * back < n_taken)
        e1 = jnp.where(gone, jnp.where(both, n_first, e1 + 1), e1)
        e1 = jnp.minimum(e1, n_entry - 1)
        e, j = jnp.where(over, e1, e), jnp.where(over, 0, j + 1)
        slot, head, key_chip, half, s_lo = place(e)
        i = i + 1
        return (slot, head, (s_lo + j) * RUNS, key_chip, half, (i < total).astype(jnp.int32)), (i, e, j, n_run - s_lo)

    exp_scale = scale * math.log2(math.e)
    k_iota = lax.broadcasted_iota(jnp.int32, (key_tile, width), 0)
    col = lax.broadcasted_iota(jnp.int32, (1, width), 1)
    q_off = sub_start + jnp.where(col < rows, me, sibling) * local_len + lax.rem(col, rows) // group

    def one(now, carry):
        (slot_p, head_p, s_p), (slot, head, s, key_chip, half, live), at = carry
        then, at = following(at)
        k, v = kvb[slot, head, :, :head_dim], kvb[slot, head, :, head_dim:]
        s_t = [jnp.dot(k, qt[head, s + r], preferred_element_type=F32) for r in range(RUNS)]
        dp_t = [jnp.dot(v, dot[head, s + r], preferred_element_type=F32) for r in range(RUNS)]
        p_p, ds_p = pbuf[1 - now], dsbuf[1 - now]
        q_p = qn[head_p, pl.ds(s_p, RUNS)].reshape(RUNS * width, head_dim)
        do_p = don[head_p, pl.ds(s_p, RUNS)].reshape(RUNS * width, head_dim)
        acc[slot_p, head_p, :, head_dim:] += jnp.dot(p_p, do_p, preferred_element_type=F32)
        acc[slot_p, head_p, :, :head_dim] += jnp.dot(ds_p, q_p, preferred_element_type=F32)
        k_t = kvb[slot_p, head_p, :, :head_dim].T
        for r in range(RUNS):
            dqa[head_p, s_p + r] += jnp.dot(k_t, ds_p[:, r * width:(r + 1) * width], preferred_element_type=F32)
        docs_k = key_doc[key_chip, pl.ds(pl.multiple_of(half * key_tile, 8), key_tile), :]
        docs_k = jnp.concatenate([docs_k] * (width // LANES), axis=1)
        pos0 = (key_chip * CORES + core) * keys_local + half * key_tile
        for r in range(RUNS):
            lse_r, delta_r, doc_r = [lines[head, s + r, m:m + 1, :] for m in range(3)]
            last = jnp.where(live == 1, q_off + (s + r) * sub_len - pos0, -1)
            ok = (docs_k == doc_r.astype(jnp.int32)) & (k_iota <= last)
            p = jnp.where(ok, jnp.exp2(s_t[r] * exp_scale - lse_r), 0.0)
            pbuf[now, :, r * width:(r + 1) * width] = p.astype(BF16)
            dsbuf[now, :, r * width:(r + 1) * width] = (p * (dp_t[r] - delta_r)).astype(BF16)
        return (slot, head, s), then, at

    def advance(state, target):
        i, carry = state
        m = jnp.maximum(target - i, 0) // UNROLL

        def step(_, carry):
            for u in range(UNROLL):
                carry = one(u % 2, carry)
            return carry

        return i + m * UNROLL, lax.fori_loop(0, m, step, carry)

    def add(dst, src, head):
        cut = key_tile // 4

        @pl.loop(0, 4)
        def _(i):
            r = pl.ds(pl.multiple_of(i * cut, 8), cut)
            acc[dst, head, r, :] += rsb[src, head, r, :]

    def partial(i, head, peer):
        return remote(acc.at[i, head], rsb.at[i, head], rs_send.at[0], rs_recv.at[i, head], peer)

    half_rows = lambda which: dqa.at[:, :, :, pl.ds(which * rows, rows)]
    swap = remote(half_rows(1), dqr, x_send.at[3], x_recv.at[3], sibling)

    GATHER, SUMS, WORK, OWN, ALL = 0, 1, 2, 3, 63
    steps, arrived = [], [1, 0]
    for word in ORDER.split():
        kind, digits = word[0], word[1:]
        head = 1 if kind in 'ET' else 0
        if arrived[0] < n_hop:
            bound = min(2 * arrived[0] + 1, n_early - 1)
        else:
            bound = n_entry - 1 if arrived[1] == n_hop else n_first + 1
        k = way = items = 0
        if kind in 'eE':
            what, k = GATHER, int(digits)
            arrived[head] = k + 1
        elif kind in 'RT':
            what, k, way = SUMS, int(digits[0]), int(digits[1])
            bound = (n_first + 2 if head else n_early) + 2 * (n_hop - 1 - k) + way
        elif kind == 'O':
            what = OWN
        else:
            what, items = WORK, ALL if kind == 'F' else int(digits)
        steps.append(what + 4 * (k + 16 * (way + 2 * (head + 2 * (items + 64 * bound)))))
    def pick(table, t):
        out = jnp.int32(0)
        for j, x in enumerate(table):
            out = out + jnp.where(t == j, x, 0)
        return out

    def carry_out(t, state):
        number = pick(steps, t)
        what, number = lax.rem(number, 4), lax.div(number, 4)
        k, number = lax.rem(number, 16), lax.div(number, 16)
        way, number = lax.rem(number, 2), lax.div(number, 2)
        head, number = lax.rem(number, 2), lax.div(number, 2)
        items, bound = lax.rem(number, 64), lax.div(number, 64)
        last = pick(until, bound)
        some = jnp.where(items == ALL, last + UNROLL, jnp.minimum(state[0] + items, last))
        state = advance(state, jnp.where(what == SUMS, last + UNROLL, jnp.where(what == WORK, some, state[0])))

        @pl.when(what == GATHER)
        def _():
            pass_on(k, head)

        @pl.when(what == OWN)
        def _():
            gather_own(1)

        @pl.when(items == ALL)
        def _():
            swap.start()

        @pl.when(what == SUMS)
        def _():
            i = way * n_hop + k
            peer = jnp.where(way == 0, left, right)

            @pl.when(k + 2 < n_hop)
            def _():
                partial(i + 2, head, peer).wait_recv()
                add(i, i + 2, head)

            partial(i, head, peer).start()
        return state

    def settle(head, half):
        for k in (1, 0):
            way = (half + k) % 2
            partial(way * n_hop + k, head, nbr[1 - way]).wait_recv()
            add(own + half, way * n_hop + k, head)
        r = slice(half * key_tile, (half + 1) * key_tile)
        dko[r, head, :] = acc[own + half, head, :, :head_dim] * scale
        dvo[r, head, :] = acc[own + half, head, :, head_dim:]

    zero = jnp.int32(0)
    start, at = following((zero - 1, zero, zero - 1, zero + 1))
    lax.fori_loop(0, len(steps), carry_out, (zero, (start[:3], start, at)))
    swap.wait_recv()

    @pl.loop(0, n_sub)
    def _(s):
        for h in range(n_kv):
            x = ((dqa[h, s, :, :rows] + dqr[h, s]) * scale).astype(BF16).T
            raw_q[0, s, :, h] = x.reshape(local_len, group, head_dim)

    puts = [pltpu.make_async_copy(raw_q.at[0], dq_out, out_sem.at[0])]
    puts[0].start()
    for head in range(n_kv - 1):
        for half in range(2):
            settle(head, half)
    for half in range(2):
        settle(n_kv - 1, half)
        r = pl.ds(half * key_tile, key_tile)
        for i, (a, b) in enumerate(((dko, dk_out), (dvo, dv_out))):
            c = pltpu.make_async_copy(a.at[r], b.at[r], out_sem.at[1 + 2 * half + i])
            c.start()
            puts.append(c)
    swap.wait_send()
    moved = pl.ds(0, 2 * n_hop)
    remote(kvb.at[moved], kvb.at[moved], ag_send.at[0], ag_recv.at[0, 0], right).wait_send()
    remote(acc.at[moved], rsb.at[moved], rs_send.at[0], rs_recv.at[0, 0], right).wait_send()
    for c in puts:
        c.wait()


def copy_kernel(a, b, c, a_out, b_out, c_out, a_buf, b_buf, c_buf, in_sem, out_sem):
    moves = []
    for src, buf, dst in ((a, a_buf, a_out), (b, b_buf, b_out), (c, c_buf, c_out)):
        piece = src.shape[0] // PIECES
        for i in range(PIECES):
            r, n = pl.ds(i * piece, piece), len(moves)
            moves.append((pltpu.make_async_copy(src.at[r], buf.at[r], in_sem.at[n]),
                          pltpu.make_async_copy(buf.at[r], dst.at[r], out_sem.at[n])))
    for n, (x, _) in enumerate(moves):
        x.start(priority=n % 2)
    for n, (x, y) in enumerate(moves):
        x.wait()
        y.start(priority=n % 2)
    for _, y in moves:
        y.wait()


def solution(mesh):
    cp_size = mesh.shape['cp']
    q_spec = P(None, 'cp', 'tp', None)
    lse_spec = P(None, 'cp', 'tp')
    kv_spec = P('cp', 'tp', None)

    def local_backward(query, out_act, out_grad, row_lse, key_act, value_act, doc_ids):
        n_sub, local_len, n_heads, head_dim = query.shape
        keys_local, n_kv = key_act.shape[0], key_act.shape[1]
        group = n_heads // n_kv
        sub_start = keys_local * cp_size - n_sub * local_len * cp_size
        rows = local_len * group
        half = keys_local // 2
        n_chip = cp_size // CORES
        n_hop = n_chip - 1
        n_slot = 2 * n_hop + 2
        q5 = (n_sub, local_len, n_kv, group, head_dim)
        scale = head_dim ** -0.5
        flops = 2 * 5 * n_kv * n_sub * 2 * rows * head_dim * keys_local * n_hop
        hbm = pl.BlockSpec(memory_space=pl.ANY)
        dma = pltpu.SemaphoreType.DMA
        vmem = pltpu.VMEM
        dq, dk, dv = pl.pallas_call(
            functools.partial(ring_kernel, cp_size, sub_start, scale),
            name='ring_backward',
            out_shape=(jax.ShapeDtypeStruct(q5, BF16),) + (jax.ShapeDtypeStruct(key_act.shape, F32),) * 2,
            in_specs=[hbm] * 7,
            out_specs=(hbm,) * 3,
            scratch_shapes=[
                vmem((n_slot, n_kv, half, 2 * head_dim), BF16),
                vmem((n_slot, n_kv, half, 2 * head_dim), F32),
                vmem((2 * n_hop, n_kv, half, 2 * head_dim), F32),
                vmem((CORES,) + q5, BF16),
                vmem((CORES,) + q5, BF16),
                vmem(q5, BF16),
                vmem((n_sub, n_heads, local_len), F32),
                vmem((doc_ids.shape[0] // LANES, LANES), jnp.int32),
                vmem((n_kv, n_sub, CORES * rows, head_dim), BF16),
                vmem((n_kv, n_sub, head_dim, CORES * rows), BF16),
                vmem((n_kv, n_sub, CORES * rows, head_dim), BF16),
                vmem((n_kv, n_sub, head_dim, CORES * rows), BF16),
                vmem((n_kv, n_sub, 8, CORES * rows), F32),
                vmem((n_chip, keys_local, LANES), jnp.int32),
                vmem((n_kv, n_sub, head_dim, CORES * rows), F32),
                vmem((n_kv, n_sub, head_dim, rows), F32),
                vmem(key_act.shape, F32),
                vmem(key_act.shape, F32),
                vmem((2, half, RUNS * CORES * rows), BF16),
                vmem((2, half, RUNS * CORES * rows), BF16),
                vmem((2,) + key_act.shape, BF16),
                dma((1,)), dma((2 * n_hop, n_kv)), dma((1,)), dma((2 * n_hop, n_kv)),
                dma((4,)), dma((4,)), dma((7,)), dma((5,)),
            ],
            compiler_params=pltpu.CompilerParams(collective_id=0, has_side_effects=True, vmem_limit_bytes=62 * 1024 * 1024),
            cost_estimate=pl.CostEstimate(flops=flops, bytes_accessed=30 * 2 ** 20, transcendentals=0),
        )(key_act, value_act, query.reshape(q5), out_act.reshape(q5), out_grad.reshape(q5), jnp.swapaxes(row_lse, 1, 2), doc_ids.reshape(-1, LANES))
        dq, dk, dv = pl.pallas_call(
            copy_kernel,
            name='results',
            out_shape=tuple(jax.ShapeDtypeStruct(x.shape, x.dtype) for x in (dq, dk, dv)),
            in_specs=[hbm] * 3,
            out_specs=(hbm,) * 3,
            scratch_shapes=[vmem(x.shape, x.dtype) for x in (dq, dk, dv)] + [dma((3 * PIECES,)), dma((3 * PIECES,))],
            cost_estimate=pl.CostEstimate(flops=0, bytes_accessed=2 ** 22, transcendentals=0),
        )(dq, dk, dv)
        return dq.reshape(query.shape), dk, dv

    return jax.shard_map(local_backward, mesh=mesh, in_specs=(q_spec, q_spec, q_spec, lse_spec, kv_spec, kv_spec, P()),
                         out_specs=(q_spec, kv_spec, kv_spec), check_vma=False)
```

```python
import functools
import math

import jax
import jax.numpy as jnp
from jax import lax
from jax.experimental import pallas as pl
from jax.experimental.pallas import tpu as pltpu
from jax.sharding import PartitionSpec as P

MESH = pl.DeviceIdType.MESH
CORES = 2
LANES = 128
SPLIT = 64
PIECES = 4
RUNS = 2
UNROLL = 2
EARLY_ITEMS = 26
ORDER = ('e1 W6 e2 e3 W6 e4 W4 O W8 e5 e6 W4 E0 R60 E1 R61 R50 E2 R51 R40 R41 W10 E3 W8 R30 R31 R20 R21 E4 E5 R10 R11 W4 R00 R01 W2 E6 '
         'T60 T61 T50 T51 T40 T41 T30 T31 T20 T21 T10 T11 F T00 T01')
F32 = jnp.float32
BF16 = jnp.bfloat16


def ring_kernel(cp_size, sub_start, scale, k_in, v_in, q_in, o_in, do_in, lse_in, doc_in, dq_out, dk_out, dv_out,
                kvb, acc, rsb, raw_q, raw_do, raw_o, lse, docs, qn, qt, don, dot, lines, key_doc, dqa, dqr, dko, dvo, pbuf, dsbuf, raw_kv,
                ag_send, ag_recv, rs_send, rs_recv, x_send, x_recv, loc_sem, out_sem):
    n_chip = cp_size // CORES
    n_hop = n_chip - 1
    n_sub, local_len, n_kv, group, head_dim = q_in.shape
    rows = local_len * group
    width = CORES * rows
    key_tile = k_in.shape[0] // 2
    span = local_len * CORES
    sub_len = local_len * cp_size
    keys_local = 2 * key_tile
    own = 2 * n_hop

    me = lax.axis_index('cp')
    chip, core = me // CORES, lax.rem(me, CORES)
    right = lax.rem(me + CORES, cp_size)
    left = lax.rem(me + cp_size - CORES, cp_size)
    sibling = me + 1 - 2 * core
    nbr = (right, left)

    barrier = pltpu.get_barrier_semaphore()
    for peer in (right, left, sibling):
        pl.semaphore_signal(barrier, inc=1, device_id={'cp': peer}, device_id_type=MESH)

    own_kv = [pltpu.make_async_copy(x, raw_kv.at[i], loc_sem.at[5 + i]) for i, x in enumerate((k_in, v_in))]
    local = [pltpu.make_async_copy(a, b, loc_sem.at[i]) for i, (a, b) in enumerate((
        (doc_in, docs), (lse_in, lse), (do_in, raw_do.at[0]), (o_in, raw_o), (q_in, raw_q.at[0])))]
    for c in own_kv + local:
        c.start()

    @pl.loop(0, n_sub)
    def _(s):
        for h in range(n_kv):
            dqa[h, s] = jnp.zeros(dqa.shape[2:], F32)

    for c in own_kv:
        c.wait()

    def split(h):
        @pl.loop(0, key_tile // SPLIT)
        def _(i):
            r = pl.multiple_of(i * SPLIT, SPLIT)
            for half in range(2):
                for part in range(2):
                    x = raw_kv[part, pl.ds(half * key_tile + r, SPLIT)].astype(F32)
                    kvb[own + half, h, pl.ds(r, SPLIT), part * head_dim:(part + 1) * head_dim] = x[:, h].astype(BF16)

    split(0)
    pl.semaphore_wait(barrier, 3)

    def remote(src, dst, send, recv, peer):
        return pltpu.make_async_remote_copy(src_ref=src, dst_ref=dst, send_sem=send, recv_sem=recv,
                                            device_id={'cp': peer}, device_id_type=MESH)

    def gather(way, k, head, src=None):
        i = way * n_hop + k
        return remote(kvb.at[i, head] if src is None else src, kvb.at[i, head], ag_send.at[0], ag_recv.at[k, head], nbr[way])

    def gather_own(head):
        for j in range(2):
            for way in range(2):
                gather(way, j, head, kvb.at[own + (j + way) % 2, head]).start()

    def pass_on(k, head):
        two = kvb.at[pl.ds(0, 2), head]
        remote(two, two, ag_send.at[0], ag_recv.at[k, head], right).wait_recv()
        for way in range(2):
            i = way * n_hop + k

            @pl.when(k + 2 < n_hop)
            def _():
                gather(way, k + 2, head, kvb.at[i, head]).start()

    gather_own(0)
    for h in range(1, n_kv):
        split(h)
    share = [remote(q_in, raw_q.at[1], x_send.at[0], x_recv.at[0], sibling),
             remote(do_in, raw_do.at[1], x_send.at[1], x_recv.at[1], sibling)]
    for c in share:
        c.start()

    def mine(which):
        return lines.at[:, :, :, pl.ds(which * rows, rows)]

    share_lines = remote(mine(0), mine(1), x_send.at[2], x_recv.at[2], sibling)

    @pl.loop(0, acc.shape[0])
    def _(i):
        for h in range(n_kv):
            acc[i, h] = jnp.zeros(acc.shape[2:], F32)

    pbuf[...] = jnp.zeros(pbuf.shape, BF16)
    dsbuf[...] = jnp.zeros(dsbuf.shape, BF16)
    local[0].wait()
    tiles = keys_local // LANES

    @pl.loop(0, n_chip)
    def _(b):
        for r in range(tiles):
            row = docs[pl.ds((b * CORES + core) * tiles + r, 1), :]
            key_doc[b, r * LANES:(r + 1) * LANES, :] = jnp.broadcast_to(row, (LANES, LANES)).T

    lane = lax.broadcasted_iota(jnp.int32, (8, rows), 1)
    sub = lax.broadcasted_iota(jnp.int32, (8, rows), 0)
    for c in local[1:4]:
        c.wait()

    side = math.gcd(n_sub, 4)

    @pl.loop(0, n_sub // side)
    def _(t):
        for u in range(side):
            s = t * side + u
            rep = jnp.concatenate([lse[s]] * (LANES // local_len), axis=1)
            wide = jnp.take_along_axis(rep, lane // group, axis=1)
            for h in range(n_kv):
                line = jnp.sum(jnp.where(sub - group * h == lane % group, wide, 0.0), axis=0, keepdims=True) * math.log2(math.e)
                prod = raw_do[0, s, :, h].reshape(rows, head_dim).astype(F32) * raw_o[s, :, h].reshape(rows, head_dim).astype(F32)
                total = jnp.broadcast_to(jnp.sum(prod, axis=1, keepdims=True), (rows, LANES)).T
                first = sub_start + s * sub_len + me * local_len
                doc_row = jnp.broadcast_to(docs[pl.ds(first // LANES, 1), :], (8, LANES))
                doc = jnp.take_along_axis(doc_row, lax.rem(first, LANES) + lane // group, axis=1).astype(F32)
                lines[h, s, :, :rows] = jnp.where(sub == 0, line, jnp.where(sub == 1, total[:8, :], doc))

    share_lines.start()

    def spread(c):
        @pl.loop(0, n_sub // RUNS)
        def _(t):
            for u in range(RUNS):
                s = t * RUNS + u
                for h in range(n_kv):
                    for raw, nat, tr in ((raw_q, qn, qt), (raw_do, don, dot)):
                        x = raw[c, s, :, h].reshape(rows, head_dim)
                        nat[h, s, c * rows:(c + 1) * rows, :] = x
                        tr[h, s, :, c * rows:(c + 1) * rows] = x.T

    for c in local[4:]:
        c.wait()
    spread(0)
    pass_on(0, 0)
    for c in share:
        c.wait()
    spread(1)
    share_lines.wait()

    n_run = n_sub // RUNS
    n_early = 2 + min(8, 2 * n_hop)
    n_first = n_early + 2 * n_hop
    n_block = 2 * n_hop + 2
    n_entry = n_first + (n_kv - 1) * n_block

    def place(e):
        first, early = e < n_first, e < n_early
        past = jnp.maximum(e - n_first, 0)
        head = jnp.where(first, 0, 1 + lax.div(past, n_block))
        b = lax.rem(past, n_block)
        mine = jnp.where(first, e, b) < 2
        f = jnp.maximum(jnp.where(early, e - 2, jnp.where(first, e - n_early, b - 2)), 0)
        step = lax.div(f, 2)
        way = f - 2 * step
        k = jnp.where(early, step, n_hop - 1 - step)
        half = jnp.where(mine, jnp.where(first, e, b), lax.rem(k + way, 2))
        slot = jnp.where(mine, own + half, way * n_hop + k)
        hop = lax.div(k, 2) + 1
        key_chip = jnp.where(mine, chip, lax.rem(chip + jnp.where(way == 1, hop, n_chip - hop), n_chip))
        pos0 = (key_chip * CORES + core) * keys_local + half * key_tile
        s_lo = jnp.minimum(lax.div(jnp.maximum(pos0 - sub_start - span * chip - span + sub_len, 0), sub_len * RUNS), n_run - 1)
        return slot, head, key_chip, half, s_lo

    taken, until, n_taken = [], [], jnp.int32(0)
    total = jnp.int32(0)
    for e in range(n_entry):
        n = n_run - place(jnp.int32(e))[4]
        if e < n_early:
            fits = jnp.int32(1) if e < 2 else (total + n <= EARLY_ITEMS).astype(jnp.int32) * taken[-1]
            taken.append(fits)
            n_taken = n_taken + fits
            n = n * fits
        elif e < n_first:
            f = e - n_early
            i_early = 2 + 2 * (n_hop - 1 - f // 2) + f % 2
            if i_early < n_early:
                n = n * (1 - taken[i_early])
        total = total + n
        until.append(total)

    def following(at):
        i, e, j, n = at
        over = j + 1 >= n
        e1 = e + 1
        e1 = jnp.where(e1 == n_taken, n_early, e1)
        f = e1 - n_early
        back = n_hop - 1 - lax.div(jnp.maximum(f, 0), 2)
        odd = lax.rem(jnp.maximum(f, 0), 2)
        inside = (f >= 0) & (f < 2 * n_hop)
        gone = inside & (2 + 2 * back + odd < n_taken)
        both = (odd == 1) | (3 + 2 * back < n_taken)
        e1 = jnp.where(gone, jnp.where(both, n_first, e1 + 1), e1)
        e1 = jnp.minimum(e1, n_entry - 1)
        e, j = jnp.where(over, e1, e), jnp.where(over, 0, j + 1)
        slot, head, key_chip, half, s_lo = place(e)
        i = i + 1
        return (slot, head, (s_lo + j) * RUNS, key_chip, half, (i < total).astype(jnp.int32)), (i, e, j, n_run - s_lo)

    exp_scale = scale * math.log2(math.e)
    k_iota = lax.broadcasted_iota(jnp.int32, (key_tile, width), 0)
    col = lax.broadcasted_iota(jnp.int32, (1, width), 1)
    q_off = sub_start + jnp.where(col < rows, me, sibling) * local_len + lax.rem(col, rows) // group

    def one(now, carry):
        (slot_p, head_p, s_p), (slot, head, s, key_chip, half, live), at = carry
        then, at = following(at)
        k, v = kvb[slot, head, :, :head_dim], kvb[slot, head, :, head_dim:]
        s_t = [jnp.dot(k, qt[head, s + r], preferred_element_type=F32) for r in range(RUNS)]
        dp_t = [jnp.dot(v, dot[head, s + r], preferred_element_type=F32) for r in range(RUNS)]
        p_p, ds_p = pbuf[1 - now], dsbuf[1 - now]
        q_p = qn[head_p, pl.ds(s_p, RUNS)].reshape(RUNS * width, head_dim)
        do_p = don[head_p, pl.ds(s_p, RUNS)].reshape(RUNS * width, head_dim)
        acc[slot_p, head_p, :, head_dim:] += jnp.dot(p_p, do_p, preferred_element_type=F32)
        acc[slot_p, head_p, :, :head_dim] += jnp.dot(ds_p, q_p, preferred_element_type=F32)
        k_t = kvb[slot_p, head_p, :, :head_dim].T
        for r in range(RUNS):
            dqa[head_p, s_p + r] += jnp.dot(k_t, ds_p[:, r * width:(r + 1) * width], preferred_element_type=F32)
        docs_k = key_doc[key_chip, pl.ds(pl.multiple_of(half * key_tile, 8), key_tile), :]
        docs_k = jnp.concatenate([docs_k] * (width // LANES), axis=1)
        pos0 = (key_chip * CORES + core) * keys_local + half * key_tile
        for r in range(RUNS):
            lse_r, delta_r, doc_r = [lines[head, s + r, m:m + 1, :] for m in range(3)]
            last = jnp.where(live == 1, q_off + (s + r) * sub_len - pos0, -1)
            ok = (docs_k == doc_r.astype(jnp.int32)) & (k_iota <= last)
            p = jnp.where(ok, jnp.exp2(s_t[r] * exp_scale - lse_r), 0.0)
            pbuf[now, :, r * width:(r + 1) * width] = p.astype(BF16)
            dsbuf[now, :, r * width:(r + 1) * width] = (p * (dp_t[r] - delta_r)).astype(BF16)
        return (slot, head, s), then, at

    def advance(state, target):
        i, carry = state
        m = jnp.maximum(target - i, 0) // UNROLL

        def step(_, carry):
            for u in range(UNROLL):
                carry = one(u % 2, carry)
            return carry

        return i + m * UNROLL, lax.fori_loop(0, m, step, carry)

    def add(dst, src, head):
        cut = key_tile // 4

        @pl.loop(0, 4)
        def _(i):
            r = pl.ds(pl.multiple_of(i * cut, 8), cut)
            acc[dst, head, r, :] += rsb[src, head, r, :]

    def partial(way, k, head, peer):
        i = way * n_hop + k
        sem = rs_recv.at[jnp.where(k < 2, way * n_hop + k, k), head]
        return remote(acc.at[i, head], rsb.at[i, head], rs_send.at[0], sem, peer)

    half_rows = lambda which: dqa.at[:, :, :, pl.ds(which * rows, rows)]
    swap = remote(half_rows(1), dqr, x_send.at[3], x_recv.at[3], sibling)

    GATHER, SUMS, WORK, OWN, ALL = 0, 1, 2, 3, 63
    steps, arrived = [], [1, 0]
    for word in ORDER.split():
        kind, digits = word[0], word[1:]
        head = 1 if kind in 'ET' else 0
        if arrived[0] < n_hop:
            bound = min(2 * arrived[0] + 1, n_early - 1)
        else:
            bound = n_entry - 1 if arrived[1] == n_hop else n_first + 1
        k = way = items = 0
        if kind in 'eE':
            what, k = GATHER, int(digits)
            arrived[head] = k + 1
        elif kind in 'RT':
            what, k, way = SUMS, int(digits[0]), int(digits[1])
            bound = (n_first + 2 if head else n_early) + 2 * (n_hop - 1 - k) + way
        elif kind == 'O':
            what = OWN
        else:
            what, items = WORK, ALL if kind == 'F' else int(digits)
        steps.append(what + 4 * (k + 16 * (way + 2 * (head + 2 * (items + 64 * bound)))))
    def pick(table, t):
        out = jnp.int32(0)
        for j, x in enumerate(table):
            out = out + jnp.where(t == j, x, 0)
        return out

    def carry_out(t, state):
        number = pick(steps, t)
        what, number = lax.rem(number, 4), lax.div(number, 4)
        k, number = lax.rem(number, 16), lax.div(number, 16)
        way, number = lax.rem(number, 2), lax.div(number, 2)
        head, number = lax.rem(number, 2), lax.div(number, 2)
        items, bound = lax.rem(number, 64), lax.div(number, 64)
        last = pick(until, bound)
        some = jnp.where(items == ALL, last + UNROLL, jnp.minimum(state[0] + items, last))
        state = advance(state, jnp.where(what == SUMS, last + UNROLL, jnp.where(what == WORK, some, state[0])))

        @pl.when(what == GATHER)
        def _():
            pass_on(k, head)

        @pl.when(what == OWN)
        def _():
            gather_own(1)

        @pl.when(items == ALL)
        def _():
            swap.start()

        @pl.when(what == SUMS)
        def _():
            i = way * n_hop + k
            peer = jnp.where(way == 0, left, right)

            @pl.when((k + 2 < n_hop) & (way == 0))
            def _():
                two = pl.ds(0, 2)
                remote(acc.at[two, head], rsb.at[two, head], rs_send.at[0], rs_recv.at[k + 2, head], peer).wait_recv()

            @pl.when(k + 2 < n_hop)
            def _():
                add(i, i + 2, head)

            partial(way, k, head, peer).start()
        return state

    def settle(head, half):
        for k in (1, 0):
            way = (half + k) % 2
            partial(way, k, head, nbr[1 - way]).wait_recv()
            add(own + half, way * n_hop + k, head)
        r = slice(half * key_tile, (half + 1) * key_tile)
        dko[r, head, :] = acc[own + half, head, :, :head_dim] * scale
        dvo[r, head, :] = acc[own + half, head, :, head_dim:]

    zero = jnp.int32(0)
    start, at = following((zero - 1, zero, zero - 1, zero + 1))
    lax.fori_loop(0, len(steps), carry_out, (zero, (start[:3], start, at)))
    swap.wait_recv()

    @pl.loop(0, n_sub)
    def _(s):
        for h in range(n_kv):
            x = ((dqa[h, s, :, :rows] + dqr[h, s]) * scale).astype(BF16).T
            raw_q[0, s, :, h] = x.reshape(local_len, group, head_dim)

    puts = [pltpu.make_async_copy(raw_q.at[0], dq_out, out_sem.at[0])]
    puts[0].start()
    for head in range(n_kv - 1):
        for half in range(2):
            settle(head, half)
    for half in range(2):
        settle(n_kv - 1, half)
        r = pl.ds(half * key_tile, key_tile)
        for i, (a, b) in enumerate(((dko, dk_out), (dvo, dv_out))):
            c = pltpu.make_async_copy(a.at[r], b.at[r], out_sem.at[1 + 2 * half + i])
            c.start()
            puts.append(c)
    swap.wait_send()
    moved = pl.ds(0, 2 * n_hop)
    remote(kvb.at[moved], kvb.at[moved], ag_send.at[0], ag_recv.at[0, 0], right).wait_send()
    remote(acc.at[moved], rsb.at[moved], rs_send.at[0], rs_recv.at[0, 0], right).wait_send()
    for c in puts:
        c.wait()


def copy_kernel(a, b, c, a_out, b_out, c_out, a_buf, b_buf, c_buf, in_sem, out_sem):
    moves = []
    for src, buf, dst in ((a, a_buf, a_out), (b, b_buf, b_out), (c, c_buf, c_out)):
        piece = src.shape[0] // PIECES
        for i in range(PIECES):
            r, n = pl.ds(i * piece, piece), len(moves)
            moves.append((pltpu.make_async_copy(src.at[r], buf.at[r], in_sem.at[n]),
                          pltpu.make_async_copy(buf.at[r], dst.at[r], out_sem.at[n])))
    for x, _ in moves:
        x.start()
    for x, y in moves:
        x.wait()
        y.start()
    for _, y in moves:
        y.wait()


def solution(mesh):
    cp_size = mesh.shape['cp']
    q_spec = P(None, 'cp', 'tp', None)
    lse_spec = P(None, 'cp', 'tp')
    kv_spec = P('cp', 'tp', None)

    def local_backward(query, out_act, out_grad, row_lse, key_act, value_act, doc_ids):
        n_sub, local_len, n_heads, head_dim = query.shape
        keys_local, n_kv = key_act.shape[0], key_act.shape[1]
        group = n_heads // n_kv
        sub_start = keys_local * cp_size - n_sub * local_len * cp_size
        rows = local_len * group
        half = keys_local // 2
        n_chip = cp_size // CORES
        n_hop = n_chip - 1
        n_slot = 2 * n_hop + 2
        q5 = (n_sub, local_len, n_kv, group, head_dim)
        scale = head_dim ** -0.5
        flops = 2 * 5 * n_kv * n_sub * 2 * rows * head_dim * keys_local * n_hop
        hbm = pl.BlockSpec(memory_space=pl.ANY)
        dma = pltpu.SemaphoreType.DMA
        vmem = pltpu.VMEM
        dq, dk, dv = pl.pallas_call(
            functools.partial(ring_kernel, cp_size, sub_start, scale),
            name='ring_backward',
            out_shape=(jax.ShapeDtypeStruct(q5, BF16),) + (jax.ShapeDtypeStruct(key_act.shape, F32),) * 2,
            in_specs=[hbm] * 7,
            out_specs=(hbm,) * 3,
            scratch_shapes=[
                vmem((n_slot, n_kv, half, 2 * head_dim), BF16),
                vmem((n_slot, n_kv, half, 2 * head_dim), F32),
                vmem((2 * n_hop, n_kv, half, 2 * head_dim), F32),
                vmem((CORES,) + q5, BF16),
                vmem((CORES,) + q5, BF16),
                vmem(q5, BF16),
                vmem((n_sub, n_heads, local_len), F32),
                vmem((doc_ids.shape[0] // LANES, LANES), jnp.int32),
                vmem((n_kv, n_sub, CORES * rows, head_dim), BF16),
                vmem((n_kv, n_sub, head_dim, CORES * rows), BF16),
                vmem((n_kv, n_sub, CORES * rows, head_dim), BF16),
                vmem((n_kv, n_sub, head_dim, CORES * rows), BF16),
                vmem((n_kv, n_sub, 8, CORES * rows), F32),
                vmem((n_chip, keys_local, LANES), jnp.int32),
                vmem((n_kv, n_sub, head_dim, CORES * rows), F32),
                vmem((n_kv, n_sub, head_dim, rows), F32),
                vmem(key_act.shape, F32),
                vmem(key_act.shape, F32),
                vmem((2, half, RUNS * CORES * rows), BF16),
                vmem((2, half, RUNS * CORES * rows), BF16),
                vmem((2,) + key_act.shape, BF16),
                dma((1,)), dma((n_hop, n_kv)), dma((1,)), dma((n_hop + 2, n_kv)),
                dma((4,)), dma((4,)), dma((7,)), dma((5,)),
            ],
            compiler_params=pltpu.CompilerParams(collective_id=0, has_side_effects=True, vmem_limit_bytes=62 * 1024 * 1024),
            cost_estimate=pl.CostEstimate(flops=flops, bytes_accessed=30 * 2 ** 20, transcendentals=0),
        )(key_act, value_act, query.reshape(q5), out_act.reshape(q5), out_grad.reshape(q5), jnp.swapaxes(row_lse, 1, 2), doc_ids.reshape(-1, LANES))
        dq, dk, dv = pl.pallas_call(
            copy_kernel,
            name='results',
            out_shape=tuple(jax.ShapeDtypeStruct(x.shape, x.dtype) for x in (dq, dk, dv)),
            in_specs=[hbm] * 3,
            out_specs=(hbm,) * 3,
            scratch_shapes=[vmem(x.shape, x.dtype) for x in (dq, dk, dv)] + [dma((3 * PIECES,)), dma((3 * PIECES,))],
            cost_estimate=pl.CostEstimate(flops=0, bytes_accessed=2 ** 22, transcendentals=0),
        )(dq, dk, dv)
        return dq.reshape(query.shape), dk, dv

    return jax.shard_map(local_backward, mesh=mesh, in_specs=(q_spec, q_spec, q_spec, lse_spec, kv_spec, kv_spec, P()),
                         out_specs=(q_spec, kv_spec, kv_spec), check_vma=False)
```

```python
import functools
import math

import jax
import jax.numpy as jnp
from jax import lax
from jax.experimental import pallas as pl
from jax.experimental.pallas import tpu as pltpu
from jax.sharding import PartitionSpec as P

MESH = pl.DeviceIdType.MESH
CORES = 2
LANES = 128
SPLIT = 64
PIECES = 4
RUNS = 2
UNROLL = 2
EARLY_ITEMS = 26
ORDER = ('e1 W6 e2 e3 W6 e4 W4 O W8 e5 e6 W4 E0 R60 E1 R61 R50 E2 R51 R40 R41 W10 E3 W8 R30 R31 R20 R21 E4 E5 R10 R11 W4 R00 R01 W2 E6 '
         'T60 T61 T50 T51 T40 T41 T30 T31 T20 T21 T10 T11 F T00 T01')
F32 = jnp.float32
BF16 = jnp.bfloat16


def ring_kernel(cp_size, sub_start, scale, k_in, v_in, q_in, o_in, do_in, lse_in, doc_in, dq_out, dk_out, dv_out,
                kvb, acc, rsb, raw_q, raw_do, raw_o, lse, docs, qn, qt, don, dot, lines, key_doc, dqa, dqr, dko, dvo, pbuf, dsbuf, raw_kv,
                ag_send, ag_recv, rs_send, rs_recv, x_send, x_recv, loc_sem, out_sem):
    n_chip = cp_size // CORES
    n_hop = n_chip - 1
    n_sub, local_len, n_kv, group, head_dim = q_in.shape
    rows = local_len * group
    width = CORES * rows
    key_tile = k_in.shape[0] // 2
    span = local_len * CORES
    sub_len = local_len * cp_size
    keys_local = 2 * key_tile
    own = 2 * n_hop

    me = lax.axis_index('cp')
    chip, core = me // CORES, lax.rem(me, CORES)
    right = lax.rem(me + CORES, cp_size)
    left = lax.rem(me + cp_size - CORES, cp_size)
    sibling = me + 1 - 2 * core
    nbr = (right, left)

    barrier = pltpu.get_barrier_semaphore()
    for peer in (right, left, sibling):
        pl.semaphore_signal(barrier, inc=1, device_id={'cp': peer}, device_id_type=MESH)

    own_kv = [pltpu.make_async_copy(x, raw_kv.at[i], loc_sem.at[5 + i]) for i, x in enumerate((k_in, v_in))]
    local = [pltpu.make_async_copy(a, b, loc_sem.at[i]) for i, (a, b) in enumerate((
        (doc_in, docs), (lse_in, lse), (do_in, raw_do.at[0]), (o_in, raw_o), (q_in, raw_q.at[0])))]
    for c in own_kv + local:
        c.start()

    @pl.loop(0, n_sub)
    def _(s):
        for h in range(n_kv):
            dqa[h, s] = jnp.zeros(dqa.shape[2:], F32)

    for c in own_kv:
        c.wait()

    def split(h):
        @pl.loop(0, key_tile // SPLIT)
        def _(i):
            r = pl.multiple_of(i * SPLIT, SPLIT)
            for half in range(2):
                for part in range(2):
                    x = raw_kv[part, pl.ds(half * key_tile + r, SPLIT)].astype(F32)
                    kvb[own + half, h, pl.ds(r, SPLIT), part * head_dim:(part + 1) * head_dim] = x[:, h].astype(BF16)

    split(0)
    pl.semaphore_wait(barrier, 3)

    def remote(src, dst, send, recv, peer):
        return pltpu.make_async_remote_copy(src_ref=src, dst_ref=dst, send_sem=send, recv_sem=recv,
                                            device_id={'cp': peer}, device_id_type=MESH)

    def gather(way, k, head, src=None):
        i = way * n_hop + k
        return remote(kvb.at[i, head] if src is None else src, kvb.at[i, head], ag_send.at[0], ag_recv.at[k, head], nbr[way])

    def gather_own(head):
        for j in range(2):
            for way in range(2):
                gather(way, j, head, kvb.at[own + (j + way) % 2, head]).start()

    def pass_on(k, head):
        two = kvb.at[pl.ds(0, 2), head]
        remote(two, two, ag_send.at[0], ag_recv.at[k, head], right).wait_recv()
        for way in range(2):
            i = way * n_hop + k

            @pl.when(k + 2 < n_hop)
            def _():
                gather(way, k + 2, head, kvb.at[i, head]).start()

    gather_own(0)
    for h in range(1, n_kv):
        split(h)
    share = [remote(q_in, raw_q.at[1], x_send.at[0], x_recv.at[0], sibling),
             remote(do_in, raw_do.at[1], x_send.at[1], x_recv.at[1], sibling)]
    for c in share:
        c.start()

    def mine(which):
        return lines.at[:, :, :, pl.ds(which * rows, rows)]

    share_lines = remote(mine(0), mine(1), x_send.at[2], x_recv.at[2], sibling)

    @pl.loop(0, acc.shape[0])
    def _(i):
        for h in range(n_kv):
            acc[i, h] = jnp.zeros(acc.shape[2:], F32)

    pbuf[...] = jnp.zeros(pbuf.shape, BF16)
    dsbuf[...] = jnp.zeros(dsbuf.shape, BF16)
    local[0].wait()
    tiles = keys_local // LANES

    @pl.loop(0, n_chip)
    def _(b):
        for r in range(tiles):
            row = docs[pl.ds((b * CORES + core) * tiles + r, 1), :]
            key_doc[b, r * LANES:(r + 1) * LANES, :] = jnp.broadcast_to(row, (LANES, LANES)).T

    lane = lax.broadcasted_iota(jnp.int32, (8, rows), 1)
    sub = lax.broadcasted_iota(jnp.int32, (8, rows), 0)
    for c in local[1:4]:
        c.wait()

    side = math.gcd(n_sub, 4)

    @pl.loop(0, n_sub // side)
    def _(t):
        for u in range(side):
            s = t * side + u
            rep = jnp.concatenate([lse[s]] * (LANES // local_len), axis=1)
            wide = jnp.take_along_axis(rep, lane // group, axis=1)
            for h in range(n_kv):
                line = jnp.sum(jnp.where(sub - group * h == lane % group, wide, 0.0), axis=0, keepdims=True) * math.log2(math.e)
                prod = raw_do[0, s, :, h].reshape(rows, head_dim).astype(F32) * raw_o[s, :, h].reshape(rows, head_dim).astype(F32)
                total = jnp.broadcast_to(jnp.sum(prod, axis=1, keepdims=True), (rows, LANES)).T
                first = sub_start + s * sub_len + me * local_len
                doc_row = jnp.broadcast_to(docs[pl.ds(first // LANES, 1), :], (8, LANES))
                doc = jnp.take_along_axis(doc_row, lax.rem(first, LANES) + lane // group, axis=1).astype(F32)
                lines[h, s, :, :rows] = jnp.where(sub == 0, line, jnp.where(sub == 1, total[:8, :], doc))

    share_lines.start()

    def spread(c):
        @pl.loop(0, n_sub // RUNS)
        def _(t):
            for u in range(RUNS):
                s = t * RUNS + u
                for h in range(n_kv):
                    for raw, nat, tr in ((raw_q, qn, qt), (raw_do, don, dot)):
                        x = raw[c, s, :, h].reshape(rows, head_dim)
                        nat[h, s, c * rows:(c + 1) * rows, :] = x
                        tr[h, s, :, c * rows:(c + 1) * rows] = x.T

    for c in local[4:]:
        c.wait()
    spread(0)
    pass_on(0, 0)
    for c in share:
        c.wait()
    spread(1)
    share_lines.wait()

    n_run = n_sub // RUNS
    n_early = 2 + min(8, 2 * n_hop)
    n_first = n_early + 2 * n_hop
    n_block = 2 * n_hop + 2
    n_entry = n_first + (n_kv - 1) * n_block

    def place(e):
        first, early = e < n_first, e < n_early
        past = jnp.maximum(e - n_first, 0)
        head = jnp.where(first, 0, 1 + lax.div(past, n_block))
        b = lax.rem(past, n_block)
        mine = jnp.where(first, e, b) < 2
        f = jnp.maximum(jnp.where(early, e - 2, jnp.where(first, e - n_early, b - 2)), 0)
        step = lax.div(f, 2)
        way = f - 2 * step
        k = jnp.where(early, step, n_hop - 1 - step)
        half = jnp.where(mine, jnp.where(first, e, b), lax.rem(k + way, 2))
        slot = jnp.where(mine, own + half, way * n_hop + k)
        hop = lax.div(k, 2) + 1
        key_chip = jnp.where(mine, chip, lax.rem(chip + jnp.where(way == 1, hop, n_chip - hop), n_chip))
        pos0 = (key_chip * CORES + core) * keys_local + half * key_tile
        s_lo = jnp.minimum(lax.div(jnp.maximum(pos0 - sub_start - span * chip - span + sub_len, 0), sub_len * RUNS), n_run - 1)
        return slot, head, key_chip, half, s_lo

    taken, until, n_taken = [], [], jnp.int32(0)
    total = jnp.int32(0)
    for e in range(n_entry):
        n = n_run - place(jnp.int32(e))[4]
        if e < n_early:
            fits = jnp.int32(1) if e < 2 else (total + n <= EARLY_ITEMS).astype(jnp.int32) * taken[-1]
            taken.append(fits)
            n_taken = n_taken + fits
            n = n * fits
        elif e < n_first:
            f = e - n_early
            i_early = 2 + 2 * (n_hop - 1 - f // 2) + f % 2
            if i_early < n_early:
                n = n * (1 - taken[i_early])
        total = total + n
        until.append(total)

    def following(at):
        i, e, j, n = at
        over = j + 1 >= n
        e1 = e + 1
        e1 = jnp.where(e1 == n_taken, n_early, e1)
        f = e1 - n_early
        back = n_hop - 1 - lax.div(jnp.maximum(f, 0), 2)
        odd = lax.rem(jnp.maximum(f, 0), 2)
        inside = (f >= 0) & (f < 2 * n_hop)
        gone = inside & (2 + 2 * back + odd < n_taken)
        both = (odd == 1) | (3 + 2 * back < n_taken)
        e1 = jnp.where(gone, jnp.where(both, n_first, e1 + 1), e1)
        e1 = jnp.minimum(e1, n_entry - 1)
        e, j = jnp.where(over, e1, e), jnp.where(over, 0, j + 1)
        slot, head, key_chip, half, s_lo = place(e)
        i = i + 1
        return (slot, head, (s_lo + j) * RUNS, key_chip, half, (i < total).astype(jnp.int32)), (i, e, j, n_run - s_lo)

    exp_scale = scale * math.log2(math.e)
    k_iota = lax.broadcasted_iota(jnp.int32, (key_tile, width), 0)
    col = lax.broadcasted_iota(jnp.int32, (1, width), 1)
    q_off = sub_start + jnp.where(col < rows, me, sibling) * local_len + lax.rem(col, rows) // group

    def one(now, carry):
        (slot_p, head_p, s_p), (slot, head, s, key_chip, half, live), at = carry
        then, at = following(at)
        k, v = kvb[slot, head, :, :head_dim], kvb[slot, head, :, head_dim:]
        s_t = [jnp.dot(k, qt[head, s + r], preferred_element_type=F32) for r in range(RUNS)]
        dp_t = [jnp.dot(v, dot[head, s + r], preferred_element_type=F32) for r in range(RUNS)]
        p_p, ds_p = pbuf[1 - now], dsbuf[1 - now]
        q_p = qn[head_p, pl.ds(s_p, RUNS)].reshape(RUNS * width, head_dim)
        do_p = don[head_p, pl.ds(s_p, RUNS)].reshape(RUNS * width, head_dim)
        acc[slot_p, head_p, :, head_dim:] += jnp.dot(p_p, do_p, preferred_element_type=F32)
        acc[slot_p, head_p, :, :head_dim] += jnp.dot(ds_p, q_p, preferred_element_type=F32)
        k_t = kvb[slot_p, head_p, :, :head_dim].T
        for r in range(RUNS):
            dqa[head_p, s_p + r] += jnp.dot(k_t, ds_p[:, r * width:(r + 1) * width], preferred_element_type=F32)
        docs_k = key_doc[key_chip, pl.ds(pl.multiple_of(half * key_tile, 8), key_tile), :]
        docs_k = jnp.concatenate([docs_k] * (width // LANES), axis=1)
        pos0 = (key_chip * CORES + core) * keys_local + half * key_tile
        for r in range(RUNS):
            lse_r, delta_r, doc_r = [lines[head, s + r, m:m + 1, :] for m in range(3)]
            last = jnp.where(live == 1, q_off + (s + r) * sub_len - pos0, -1)
            ok = (docs_k == doc_r.astype(jnp.int32)) & (k_iota <= last)
            p = jnp.where(ok, jnp.exp2(s_t[r] * exp_scale - lse_r), 0.0)
            pbuf[now, :, r * width:(r + 1) * width] = p.astype(BF16)
            dsbuf[now, :, r * width:(r + 1) * width] = (p * (dp_t[r] - delta_r)).astype(BF16)
        return (slot, head, s), then, at

    def advance(state, target):
        i, carry = state
        m = jnp.maximum(target - i, 0) // UNROLL

        def step(_, carry):
            for u in range(UNROLL):
                carry = one(u % 2, carry)
            return carry

        return i + m * UNROLL, lax.fori_loop(0, m, step, carry)

    def add(dst, src, head):
        cut = key_tile // 4

        @pl.loop(0, 4)
        def _(i):
            r = pl.ds(pl.multiple_of(i * cut, 8), cut)
            acc[dst, head, r, :] += rsb[src, head, r, :]

    def partial(way, k, head, peer):
        i = way * n_hop + k
        sem = rs_recv.at[jnp.where(k < 2, way * n_hop + k, k), head]
        return remote(acc.at[i, head], rsb.at[i, head], rs_send.at[0], sem, peer)

    half_rows = lambda which: dqa.at[:, :, :, pl.ds(which * rows, rows)]
    swap = remote(half_rows(1), dqr, x_send.at[3], x_recv.at[3], sibling)

    GATHER, SUMS, WORK, OWN, ALL = 0, 1, 2, 3, 63
    steps, arrived = [], [1, 0]
    for word in ORDER.split():
        kind, digits = word[0], word[1:]
        head = 1 if kind in 'ET' else 0
        if arrived[0] < n_hop:
            bound = min(2 * arrived[0] + 1, n_early - 1)
        else:
            bound = n_entry - 1 if arrived[1] == n_hop else n_first + 1
        k = way = items = 0
        if kind in 'eE':
            what, k = GATHER, int(digits)
            arrived[head] = k + 1
        elif kind in 'RT':
            what, k, way = SUMS, int(digits[0]), int(digits[1])
            bound = (n_first + 2 if head else n_early) + 2 * (n_hop - 1 - k) + way
        elif kind == 'O':
            what = OWN
        else:
            what, items = WORK, ALL if kind == 'F' else int(digits)
        steps.append(what + 4 * (k + 16 * (way + 2 * (head + 2 * (items + 64 * bound)))))
    def pick(table, t):
        out = jnp.int32(0)
        for j, x in enumerate(table):
            out = out + jnp.where(t == j, x, 0)
        return out

    def carry_out(t, state):
        number = pick(steps, t)
        what, number = lax.rem(number, 4), lax.div(number, 4)
        k, number = lax.rem(number, 16), lax.div(number, 16)
        way, number = lax.rem(number, 2), lax.div(number, 2)
        head, number = lax.rem(number, 2), lax.div(number, 2)
        items, bound = lax.rem(number, 64), lax.div(number, 64)
        last = pick(until, bound)
        some = jnp.where(items == ALL, last + UNROLL, jnp.minimum(state[0] + items, last))
        state = advance(state, jnp.where(what == SUMS, last + UNROLL, jnp.where(what == WORK, some, state[0])))

        @pl.when(what == GATHER)
        def _():
            pass_on(k, head)

        @pl.when(what == OWN)
        def _():
            gather_own(1)

        @pl.when(items == ALL)
        def _():
            swap.start()

        @pl.when(what == SUMS)
        def _():
            i = way * n_hop + k
            peer = jnp.where(way == 0, left, right)

            @pl.when((k + 2 < n_hop) & (way == 0))
            def _():
                two = pl.ds(0, 2)
                remote(acc.at[two, head], rsb.at[two, head], rs_send.at[0], rs_recv.at[k + 2, head], peer).wait_recv()

            @pl.when(k + 2 < n_hop)
            def _():
                add(i, i + 2, head)

            partial(way, k, head, peer).start()
        return state

    def settle(head, half):
        near, far = half * n_hop, (1 - half) * n_hop + 1
        partial(1 - half, 1, head, nbr[half]).wait_recv()
        add(own + half, far, head)
        partial(half, 0, head, nbr[1 - half]).wait_recv()
        r = slice(half * key_tile, (half + 1) * key_tile)
        dko[r, head, :] = (acc[own + half, head, :, :head_dim] + rsb[near, head, :, :head_dim]) * scale
        dvo[r, head, :] = acc[own + half, head, :, head_dim:] + rsb[near, head, :, head_dim:]

    zero = jnp.int32(0)
    start, at = following((zero - 1, zero, zero - 1, zero + 1))
    lax.fori_loop(0, len(steps), carry_out, (zero, (start[:3], start, at)))
    swap.wait_recv()

    @pl.loop(0, n_sub)
    def _(s):
        for h in range(n_kv):
            x = ((dqa[h, s, :, :rows] + dqr[h, s]) * scale).astype(BF16).T
            raw_q[0, s, :, h] = x.reshape(local_len, group, head_dim)

    puts = [pltpu.make_async_copy(raw_q.at[0], dq_out, out_sem.at[0])]
    puts[0].start()
    for head in range(n_kv - 1):
        for half in range(2):
            settle(head, half)
    for half in range(2):
        settle(n_kv - 1, half)
        r = pl.ds(half * key_tile, key_tile)
        for i, (a, b) in enumerate(((dko, dk_out), (dvo, dv_out))):
            c = pltpu.make_async_copy(a.at[r], b.at[r], out_sem.at[1 + 2 * half + i])
            c.start()
            puts.append(c)
    swap.wait_send()
    moved = pl.ds(0, 2 * n_hop)
    remote(kvb.at[moved], kvb.at[moved], ag_send.at[0], ag_recv.at[0, 0], right).wait_send()
    remote(acc.at[moved], rsb.at[moved], rs_send.at[0], rs_recv.at[0, 0], right).wait_send()
    for c in puts:
        c.wait()


def copy_kernel(a, b, c, a_out, b_out, c_out, a_buf, b_buf, c_buf, in_sem, out_sem):
    moves = []
    for src, buf, dst in ((a, a_buf, a_out), (b, b_buf, b_out), (c, c_buf, c_out)):
        piece = src.shape[0] // PIECES
        for i in range(PIECES):
            r, n = pl.ds(i * piece, piece), len(moves)
            moves.append((pltpu.make_async_copy(src.at[r], buf.at[r], in_sem.at[n]),
                          pltpu.make_async_copy(buf.at[r], dst.at[r], out_sem.at[n])))
    for x, _ in moves:
        x.start()
    for x, y in moves:
        x.wait()
        y.start()
    for _, y in moves:
        y.wait()


def solution(mesh):
    cp_size = mesh.shape['cp']
    q_spec = P(None, 'cp', 'tp', None)
    lse_spec = P(None, 'cp', 'tp')
    kv_spec = P('cp', 'tp', None)

    def local_backward(query, out_act, out_grad, row_lse, key_act, value_act, doc_ids):
        n_sub, local_len, n_heads, head_dim = query.shape
        keys_local, n_kv = key_act.shape[0], key_act.shape[1]
        group = n_heads // n_kv
        sub_start = keys_local * cp_size - n_sub * local_len * cp_size
        rows = local_len * group
        half = keys_local // 2
        n_chip = cp_size // CORES
        n_hop = n_chip - 1
        n_slot = 2 * n_hop + 2
        q5 = (n_sub, local_len, n_kv, group, head_dim)
        scale = head_dim ** -0.5
        flops = 2 * 5 * n_kv * n_sub * 2 * rows * head_dim * keys_local * n_hop
        hbm = pl.BlockSpec(memory_space=pl.ANY)
        dma = pltpu.SemaphoreType.DMA
        vmem = pltpu.VMEM
        dq, dk, dv = pl.pallas_call(
            functools.partial(ring_kernel, cp_size, sub_start, scale),
            name='ring_backward',
            out_shape=(jax.ShapeDtypeStruct(q5, BF16),) + (jax.ShapeDtypeStruct(key_act.shape, F32),) * 2,
            in_specs=[hbm] * 7,
            out_specs=(hbm,) * 3,
            scratch_shapes=[
                vmem((n_slot, n_kv, half, 2 * head_dim), BF16),
                vmem((n_slot, n_kv, half, 2 * head_dim), F32),
                vmem((2 * n_hop, n_kv, half, 2 * head_dim), F32),
                vmem((CORES,) + q5, BF16),
                vmem((CORES,) + q5, BF16),
                vmem(q5, BF16),
                vmem((n_sub, n_heads, local_len), F32),
                vmem((doc_ids.shape[0] // LANES, LANES), jnp.int32),
                vmem((n_kv, n_sub, CORES * rows, head_dim), BF16),
                vmem((n_kv, n_sub, head_dim, CORES * rows), BF16),
                vmem((n_kv, n_sub, CORES * rows, head_dim), BF16),
                vmem((n_kv, n_sub, head_dim, CORES * rows), BF16),
                vmem((n_kv, n_sub, 8, CORES * rows), F32),
                vmem((n_chip, keys_local, LANES), jnp.int32),
                vmem((n_kv, n_sub, head_dim, CORES * rows), F32),
                vmem((n_kv, n_sub, head_dim, rows), F32),
                vmem(key_act.shape, F32),
                vmem(key_act.shape, F32),
                vmem((2, half, RUNS * CORES * rows), BF16),
                vmem((2, half, RUNS * CORES * rows), BF16),
                vmem((2,) + key_act.shape, BF16),
                dma((1,)), dma((n_hop, n_kv)), dma((1,)), dma((n_hop + 2, n_kv)),
                dma((4,)), dma((4,)), dma((7,)), dma((5,)),
            ],
            compiler_params=pltpu.CompilerParams(collective_id=0, has_side_effects=True, vmem_limit_bytes=62 * 1024 * 1024),
            cost_estimate=pl.CostEstimate(flops=flops, bytes_accessed=30 * 2 ** 20, transcendentals=0),
        )(key_act, value_act, query.reshape(q5), out_act.reshape(q5), out_grad.reshape(q5), jnp.swapaxes(row_lse, 1, 2), doc_ids.reshape(-1, LANES))
        dq, dk, dv = pl.pallas_call(
            copy_kernel,
            name='results',
            out_shape=tuple(jax.ShapeDtypeStruct(x.shape, x.dtype) for x in (dq, dk, dv)),
            in_specs=[hbm] * 3,
            out_specs=(hbm,) * 3,
            scratch_shapes=[vmem(x.shape, x.dtype) for x in (dq, dk, dv)] + [dma((3 * PIECES,)), dma((3 * PIECES,))],
            cost_estimate=pl.CostEstimate(flops=0, bytes_accessed=2 ** 22, transcendentals=0),
        )(dq, dk, dv)
        return dq.reshape(query.shape), dk, dv

    return jax.shard_map(local_backward, mesh=mesh, in_specs=(q_spec, q_spec, q_spec, lse_spec, kv_spec, kv_spec, P()),
                         out_specs=(q_spec, kv_spec, kv_spec), check_vma=False)
```

```python
import functools
import math

import jax
import jax.numpy as jnp
from jax import lax
from jax.experimental import pallas as pl
from jax.experimental.pallas import tpu as pltpu
from jax.sharding import PartitionSpec as P

MESH = pl.DeviceIdType.MESH
CORES = 2
LANES = 128
SPLIT = 64
PIECES = 2
RUNS = 2
UNROLL = 2
EARLY_ITEMS = 26
ORDER = ('e1 W6 e2 e3 W6 e4 W4 O W8 e5 e6 W4 E0 R60 E1 R61 R50 E2 R51 R40 R41 W10 E3 W8 R30 R31 R20 R21 E4 E5 R10 R11 W4 R00 R01 W2 E6 '
         'T60 T61 T50 T51 T40 T41 T30 T31 T20 T21 T10 T11 F T00 T01')
F32 = jnp.float32
BF16 = jnp.bfloat16


def ring_kernel(cp_size, sub_start, scale, k_in, v_in, q_in, o_in, do_in, lse_in, doc_in, dq_out, dk_out, dv_out,
                kvb, acc, rsb, raw_q, raw_do, raw_o, lse, docs, qn, qt, don, dot, lines, key_doc, dqa, dqr, dko, dvo, pbuf, dsbuf, raw_kv,
                ag_send, ag_recv, rs_send, rs_recv, x_send, x_recv, loc_sem, out_sem):
    n_chip = cp_size // CORES
    n_hop = n_chip - 1
    n_sub, local_len, n_kv, group, head_dim = q_in.shape
    rows = local_len * group
    width = CORES * rows
    key_tile = k_in.shape[0] // 2
    span = local_len * CORES
    sub_len = local_len * cp_size
    keys_local = 2 * key_tile
    own = 2 * n_hop

    me = lax.axis_index('cp')
    chip, core = me // CORES, lax.rem(me, CORES)
    right = lax.rem(me + CORES, cp_size)
    left = lax.rem(me + cp_size - CORES, cp_size)
    sibling = me + 1 - 2 * core
    nbr = (right, left)

    barrier = pltpu.get_barrier_semaphore()
    for peer in (right, left, sibling):
        pl.semaphore_signal(barrier, inc=1, device_id={'cp': peer}, device_id_type=MESH)

    own_kv = [pltpu.make_async_copy(x, raw_kv.at[i], loc_sem.at[5 + i]) for i, x in enumerate((k_in, v_in))]
    local = [pltpu.make_async_copy(a, b, loc_sem.at[i]) for i, (a, b) in enumerate((
        (doc_in, docs), (lse_in, lse), (do_in, raw_do.at[0]), (o_in, raw_o), (q_in, raw_q.at[0])))]
    for c in own_kv + local:
        c.start()

    @pl.loop(0, n_sub)
    def _(s):
        for h in range(n_kv):
            dqa[h, s] = jnp.zeros(dqa.shape[2:], F32)

    for c in own_kv:
        c.wait()

    def split(h):
        @pl.loop(0, key_tile // SPLIT)
        def _(i):
            r = pl.multiple_of(i * SPLIT, SPLIT)
            for half in range(2):
                for part in range(2):
                    x = raw_kv[part, pl.ds(half * key_tile + r, SPLIT)].astype(F32)
                    kvb[own + half, h, pl.ds(r, SPLIT), part * head_dim:(part + 1) * head_dim] = x[:, h].astype(BF16)

    split(0)
    pl.semaphore_wait(barrier, 3)

    def remote(src, dst, send, recv, peer):
        return pltpu.make_async_remote_copy(src_ref=src, dst_ref=dst, send_sem=send, recv_sem=recv,
                                            device_id={'cp': peer}, device_id_type=MESH)

    def gather(way, k, head, src=None):
        i = way * n_hop + k
        return remote(kvb.at[i, head] if src is None else src, kvb.at[i, head], ag_send.at[0], ag_recv.at[k, head], nbr[way])

    def gather_own(head):
        for j in range(2):
            for way in range(2):
                gather(way, j, head, kvb.at[own + (j + way) % 2, head]).start()

    def pass_on(k, head):
        two = kvb.at[pl.ds(0, 2), head]
        remote(two, two, ag_send.at[0], ag_recv.at[k, head], right).wait_recv()
        for way in range(2):
            i = way * n_hop + k

            @pl.when(k + 2 < n_hop)
            def _():
                gather(way, k + 2, head, kvb.at[i, head]).start()

    gather_own(0)
    for h in range(1, n_kv):
        split(h)
    share = [remote(q_in, raw_q.at[1], x_send.at[0], x_recv.at[0], sibling),
             remote(do_in, raw_do.at[1], x_send.at[1], x_recv.at[1], sibling)]
    for c in share:
        c.start()

    def mine(which):
        return lines.at[:, :, :, pl.ds(which * rows, rows)]

    share_lines = remote(mine(0), mine(1), x_send.at[2], x_recv.at[2], sibling)

    @pl.loop(0, acc.shape[0])
    def _(i):
        for h in range(n_kv):
            acc[i, h] = jnp.zeros(acc.shape[2:], F32)

    pbuf[...] = jnp.zeros(pbuf.shape, BF16)
    dsbuf[...] = jnp.zeros(dsbuf.shape, BF16)
    local[0].wait()
    tiles = keys_local // LANES

    @pl.loop(0, n_chip)
    def _(b):
        for r in range(tiles):
            row = docs[pl.ds((b * CORES + core) * tiles + r, 1), :]
            key_doc[b, r * LANES:(r + 1) * LANES, :] = jnp.broadcast_to(row, (LANES, LANES)).T

    lane = lax.broadcasted_iota(jnp.int32, (8, rows), 1)
    sub = lax.broadcasted_iota(jnp.int32, (8, rows), 0)
    for c in local[1:4]:
        c.wait()

    side = math.gcd(n_sub, 4)

    @pl.loop(0, n_sub // side)
    def _(t):
        for u in range(side):
            s = t * side + u
            rep = jnp.concatenate([lse[s]] * (LANES // local_len), axis=1)
            wide = jnp.take_along_axis(rep, lane // group, axis=1)
            for h in range(n_kv):
                line = jnp.sum(jnp.where(sub - group * h == lane % group, wide, 0.0), axis=0, keepdims=True) * math.log2(math.e)
                prod = raw_do[0, s, :, h].reshape(rows, head_dim).astype(F32) * raw_o[s, :, h].reshape(rows, head_dim).astype(F32)
                total = jnp.broadcast_to(jnp.sum(prod, axis=1, keepdims=True), (rows, LANES)).T
                first = sub_start + s * sub_len + me * local_len
                doc_row = jnp.broadcast_to(docs[pl.ds(first // LANES, 1), :], (8, LANES))
                doc = jnp.take_along_axis(doc_row, lax.rem(first, LANES) + lane // group, axis=1).astype(F32)
                lines[h, s, :, :rows] = jnp.where(sub == 0, line, jnp.where(sub == 1, total[:8, :], doc))

    share_lines.start()

    def spread(c):
        @pl.loop(0, n_sub // RUNS)
        def _(t):
            for u in range(RUNS):
                s = t * RUNS + u
                for h in range(n_kv):
                    for raw, nat, tr in ((raw_q, qn, qt), (raw_do, don, dot)):
                        x = raw[c, s, :, h].reshape(rows, head_dim)
                        nat[h, s, c * rows:(c + 1) * rows, :] = x
                        tr[h, s, :, c * rows:(c + 1) * rows] = x.T

    for c in local[4:]:
        c.wait()
    spread(0)
    pass_on(0, 0)
    for c in share:
        c.wait()
    spread(1)
    share_lines.wait()

    n_run = n_sub // RUNS
    n_early = 2 + min(8, 2 * n_hop)
    n_first = n_early + 2 * n_hop
    n_block = 2 * n_hop + 2
    n_entry = n_first + (n_kv - 1) * n_block

    def place(e):
        first, early = e < n_first, e < n_early
        past = jnp.maximum(e - n_first, 0)
        head = jnp.where(first, 0, 1 + lax.div(past, n_block))
        b = lax.rem(past, n_block)
        mine = jnp.where(first, e, b) < 2
        f = jnp.maximum(jnp.where(early, e - 2, jnp.where(first, e - n_early, b - 2)), 0)
        step = lax.div(f, 2)
        way = f - 2 * step
        k = jnp.where(early, step, n_hop - 1 - step)
        half = jnp.where(mine, jnp.where(first, e, b), lax.rem(k + way, 2))
        slot = jnp.where(mine, own + half, way * n_hop + k)
        hop = lax.div(k, 2) + 1
        key_chip = jnp.where(mine, chip, lax.rem(chip + jnp.where(way == 1, hop, n_chip - hop), n_chip))
        pos0 = (key_chip * CORES + core) * keys_local + half * key_tile
        s_lo = jnp.minimum(lax.div(jnp.maximum(pos0 - sub_start - span * chip - span + sub_len, 0), sub_len * RUNS), n_run - 1)
        return slot, head, key_chip, half, s_lo

    taken, until, n_taken = [], [], jnp.int32(0)
    total = jnp.int32(0)
    for e in range(n_entry):
        n = n_run - place(jnp.int32(e))[4]
        if e < n_early:
            fits = jnp.int32(1) if e < 2 else (total + n <= EARLY_ITEMS).astype(jnp.int32) * taken[-1]
            taken.append(fits)
            n_taken = n_taken + fits
            n = n * fits
        elif e < n_first:
            f = e - n_early
            i_early = 2 + 2 * (n_hop - 1 - f // 2) + f % 2
            if i_early < n_early:
                n = n * (1 - taken[i_early])
        total = total + n
        until.append(total)

    def following(at):
        i, e, j, n = at
        over = j + 1 >= n
        e1 = e + 1
        e1 = jnp.where(e1 == n_taken, n_early, e1)
        f = e1 - n_early
        back = n_hop - 1 - lax.div(jnp.maximum(f, 0), 2)
        odd = lax.rem(jnp.maximum(f, 0), 2)
        inside = (f >= 0) & (f < 2 * n_hop)
        gone = inside & (2 + 2 * back + odd < n_taken)
        both = (odd == 1) | (3 + 2 * back < n_taken)
        e1 = jnp.where(gone, jnp.where(both, n_first, e1 + 1), e1)
        e1 = jnp.minimum(e1, n_entry - 1)
        e, j = jnp.where(over, e1, e), jnp.where(over, 0, j + 1)
        slot, head, key_chip, half, s_lo = place(e)
        i = i + 1
        return (slot, head, (s_lo + j) * RUNS, key_chip, half, (i < total).astype(jnp.int32)), (i, e, j, n_run - s_lo)

    exp_scale = scale * math.log2(math.e)
    k_iota = lax.broadcasted_iota(jnp.int32, (key_tile, width), 0)
    col = lax.broadcasted_iota(jnp.int32, (1, width), 1)
    q_off = sub_start + jnp.where(col < rows, me, sibling) * local_len + lax.rem(col, rows) // group

    def one(now, carry):
        (slot_p, head_p, s_p), (slot, head, s, key_chip, half, live), at = carry
        then, at = following(at)
        k, v = kvb[slot, head, :, :head_dim], kvb[slot, head, :, head_dim:]
        s_t = [jnp.dot(k, qt[head, s + r], preferred_element_type=F32) for r in range(RUNS)]
        dp_t = [jnp.dot(v, dot[head, s + r], preferred_element_type=F32) for r in range(RUNS)]
        p_p, ds_p = pbuf[1 - now], dsbuf[1 - now]
        q_p = qn[head_p, pl.ds(s_p, RUNS)].reshape(RUNS * width, head_dim)
        do_p = don[head_p, pl.ds(s_p, RUNS)].reshape(RUNS * width, head_dim)
        acc[slot_p, head_p, :, head_dim:] += jnp.dot(p_p, do_p, preferred_element_type=F32)
        acc[slot_p, head_p, :, :head_dim] += jnp.dot(ds_p, q_p, preferred_element_type=F32)
        k_t = kvb[slot_p, head_p, :, :head_dim].T
        for r in range(RUNS):
            dqa[head_p, s_p + r] += jnp.dot(k_t, ds_p[:, r * width:(r + 1) * width], preferred_element_type=F32)
        docs_k = key_doc[key_chip, pl.ds(pl.multiple_of(half * key_tile, 8), key_tile), :]
        docs_k = jnp.concatenate([docs_k] * (width // LANES), axis=1)
        pos0 = (key_chip * CORES + core) * keys_local + half * key_tile
        for r in range(RUNS):
            lse_r, delta_r, doc_r = [lines[head, s + r, m:m + 1, :] for m in range(3)]
            last = jnp.where(live == 1, q_off + (s + r) * sub_len - pos0, -1)
            ok = (docs_k == doc_r.astype(jnp.int32)) & (k_iota <= last)
            p = jnp.where(ok, jnp.exp2(s_t[r] * exp_scale - lse_r), 0.0)
            pbuf[now, :, r * width:(r + 1) * width] = p.astype(BF16)
            dsbuf[now, :, r * width:(r + 1) * width] = (p * (dp_t[r] - delta_r)).astype(BF16)
        return (slot, head, s), then, at

    def advance(state, target):
        i, carry = state
        m = jnp.maximum(target - i, 0) // UNROLL

        def step(_, carry):
            for u in range(UNROLL):
                carry = one(u % 2, carry)
            return carry

        return i + m * UNROLL, lax.fori_loop(0, m, step, carry)

    def add(dst, src, head):
        cut = key_tile // 4

        @pl.loop(0, 4)
        def _(i):
            r = pl.ds(pl.multiple_of(i * cut, 8), cut)
            acc[dst, head, r, :] += rsb[src, head, r, :]

    def partial(way, k, head, peer):
        i = way * n_hop + k
        sem = rs_recv.at[jnp.where(k < 2, way * n_hop + k, k), head]
        return remote(acc.at[i, head], rsb.at[i, head], rs_send.at[0], sem, peer)

    half_rows = lambda which: dqa.at[:, :, :, pl.ds(which * rows, rows)]
    swap = remote(half_rows(1), dqr, x_send.at[3], x_recv.at[3], sibling)

    GATHER, SUMS, WORK, OWN, ALL = 0, 1, 2, 3, 63
    steps, arrived = [], [1, 0]
    for word in ORDER.split():
        kind, digits = word[0], word[1:]
        head = 1 if kind in 'ET' else 0
        if arrived[0] < n_hop:
            bound = min(2 * arrived[0] + 1, n_early - 1)
        else:
            bound = n_entry - 1 if arrived[1] == n_hop else n_first + 1
        k = way = items = 0
        if kind in 'eE':
            what, k = GATHER, int(digits)
            arrived[head] = k + 1
        elif kind in 'RT':
            what, k, way = SUMS, int(digits[0]), int(digits[1])
            bound = (n_first + 2 if head else n_early) + 2 * (n_hop - 1 - k) + way
        elif kind == 'O':
            what = OWN
        else:
            what, items = WORK, ALL if kind == 'F' else int(digits)
        steps.append(what + 4 * (k + 16 * (way + 2 * (head + 2 * (items + 64 * bound)))))
    def pick(table, t):
        out = jnp.int32(0)
        for j, x in enumerate(table):
            out = out + jnp.where(t == j, x, 0)
        return out

    def carry_out(t, state):
        number = pick(steps, t)
        what, number = lax.rem(number, 4), lax.div(number, 4)
        k, number = lax.rem(number, 16), lax.div(number, 16)
        way, number = lax.rem(number, 2), lax.div(number, 2)
        head, number = lax.rem(number, 2), lax.div(number, 2)
        items, bound = lax.rem(number, 64), lax.div(number, 64)
        last = pick(until, bound)
        some = jnp.where(items == ALL, last + UNROLL, jnp.minimum(state[0] + items, last))
        state = advance(state, jnp.where(what == SUMS, last + UNROLL, jnp.where(what == WORK, some, state[0])))

        @pl.when(what == GATHER)
        def _():
            pass_on(k, head)

        @pl.when(what == OWN)
        def _():
            gather_own(1)

        @pl.when(items == ALL)
        def _():
            swap.start()

        @pl.when(what == SUMS)
        def _():
            i = way * n_hop + k
            peer = jnp.where(way == 0, left, right)

            @pl.when((k + 2 < n_hop) & (way == 0))
            def _():
                two = pl.ds(0, 2)
                remote(acc.at[two, head], rsb.at[two, head], rs_send.at[0], rs_recv.at[k + 2, head], peer).wait_recv()

            @pl.when(k + 2 < n_hop)
            def _():
                add(i, i + 2, head)

            partial(way, k, head, peer).start()
        return state

    def settle(head, half):
        near, far = half * n_hop, (1 - half) * n_hop + 1
        partial(1 - half, 1, head, nbr[half]).wait_recv()
        add(own + half, far, head)
        partial(half, 0, head, nbr[1 - half]).wait_recv()
        r = slice(half * key_tile, (half + 1) * key_tile)
        dko[r, head, :] = (acc[own + half, head, :, :head_dim] + rsb[near, head, :, :head_dim]) * scale
        dvo[r, head, :] = acc[own + half, head, :, head_dim:] + rsb[near, head, :, head_dim:]

    zero = jnp.int32(0)
    start, at = following((zero - 1, zero, zero - 1, zero + 1))
    lax.fori_loop(0, len(steps), carry_out, (zero, (start[:3], start, at)))
    swap.wait_recv()

    @pl.loop(0, n_sub)
    def _(s):
        for h in range(n_kv):
            x = ((dqa[h, s, :, :rows] + dqr[h, s]) * scale).astype(BF16).T
            raw_q[0, s, :, h] = x.reshape(local_len, group, head_dim)

    puts = [pltpu.make_async_copy(raw_q.at[0], dq_out, out_sem.at[0])]
    puts[0].start()
    for head in range(n_kv - 1):
        for half in range(2):
            settle(head, half)
    for half in range(2):
        settle(n_kv - 1, half)
        r = pl.ds(half * key_tile, key_tile)
        for i, (a, b) in enumerate(((dko, dk_out), (dvo, dv_out))):
            c = pltpu.make_async_copy(a.at[r], b.at[r], out_sem.at[1 + 2 * half + i])
            c.start()
            puts.append(c)
    swap.wait_send()
    moved = pl.ds(0, 2 * n_hop)
    remote(kvb.at[moved], kvb.at[moved], ag_send.at[0], ag_recv.at[0, 0], right).wait_send()
    remote(acc.at[moved], rsb.at[moved], rs_send.at[0], rs_recv.at[0, 0], right).wait_send()
    for c in puts:
        c.wait()


def copy_kernel(a, b, c, a_out, b_out, c_out, a_buf, b_buf, c_buf, in_sem, out_sem):
    moves = []
    for src, buf, dst in ((a, a_buf, a_out), (b, b_buf, b_out), (c, c_buf, c_out)):
        piece = src.shape[0] // PIECES
        for i in range(PIECES):
            r, n = pl.ds(i * piece, piece), len(moves)
            moves.append((pltpu.make_async_copy(src.at[r], buf.at[r], in_sem.at[n]),
                          pltpu.make_async_copy(buf.at[r], dst.at[r], out_sem.at[n])))
    for x, _ in moves:
        x.start()
    for x, y in moves:
        x.wait()
        y.start()
    for _, y in moves:
        y.wait()


def solution(mesh):
    cp_size = mesh.shape['cp']
    q_spec = P(None, 'cp', 'tp', None)
    lse_spec = P(None, 'cp', 'tp')
    kv_spec = P('cp', 'tp', None)

    def local_backward(query, out_act, out_grad, row_lse, key_act, value_act, doc_ids):
        n_sub, local_len, n_heads, head_dim = query.shape
        keys_local, n_kv = key_act.shape[0], key_act.shape[1]
        group = n_heads // n_kv
        sub_start = keys_local * cp_size - n_sub * local_len * cp_size
        rows = local_len * group
        half = keys_local // 2
        n_chip = cp_size // CORES
        n_hop = n_chip - 1
        n_slot = 2 * n_hop + 2
        q5 = (n_sub, local_len, n_kv, group, head_dim)
        scale = head_dim ** -0.5
        flops = 2 * 5 * n_kv * n_sub * 2 * rows * head_dim * keys_local * n_hop
        hbm = pl.BlockSpec(memory_space=pl.ANY)
        dma = pltpu.SemaphoreType.DMA
        vmem = pltpu.VMEM
        dq, dk, dv = pl.pallas_call(
            functools.partial(ring_kernel, cp_size, sub_start, scale),
            name='ring_backward',
            out_shape=(jax.ShapeDtypeStruct(q5, BF16),) + (jax.ShapeDtypeStruct(key_act.shape, F32),) * 2,
            in_specs=[hbm] * 7,
            out_specs=(hbm,) * 3,
            scratch_shapes=[
                vmem((n_slot, n_kv, half, 2 * head_dim), BF16),
                vmem((n_slot, n_kv, half, 2 * head_dim), F32),
                vmem((2 * n_hop, n_kv, half, 2 * head_dim), F32),
                vmem((CORES,) + q5, BF16),
                vmem((CORES,) + q5, BF16),
                vmem(q5, BF16),
                vmem((n_sub, n_heads, local_len), F32),
                vmem((doc_ids.shape[0] // LANES, LANES), jnp.int32),
                vmem((n_kv, n_sub, CORES * rows, head_dim), BF16),
                vmem((n_kv, n_sub, head_dim, CORES * rows), BF16),
                vmem((n_kv, n_sub, CORES * rows, head_dim), BF16),
                vmem((n_kv, n_sub, head_dim, CORES * rows), BF16),
                vmem((n_kv, n_sub, 8, CORES * rows), F32),
                vmem((n_chip, keys_local, LANES), jnp.int32),
                vmem((n_kv, n_sub, head_dim, CORES * rows), F32),
                vmem((n_kv, n_sub, head_dim, rows), F32),
                vmem(key_act.shape, F32),
                vmem(key_act.shape, F32),
                vmem((2, half, RUNS * CORES * rows), BF16),
                vmem((2, half, RUNS * CORES * rows), BF16),
                vmem((2,) + key_act.shape, BF16),
                dma((1,)), dma((n_hop, n_kv)), dma((1,)), dma((n_hop + 2, n_kv)),
                dma((4,)), dma((4,)), dma((7,)), dma((5,)),
            ],
            compiler_params=pltpu.CompilerParams(collective_id=0, has_side_effects=True, vmem_limit_bytes=62 * 1024 * 1024),
            cost_estimate=pl.CostEstimate(flops=flops, bytes_accessed=30 * 2 ** 20, transcendentals=0),
        )(key_act, value_act, query.reshape(q5), out_act.reshape(q5), out_grad.reshape(q5), jnp.swapaxes(row_lse, 1, 2), doc_ids.reshape(-1, LANES))
        dq, dk, dv = pl.pallas_call(
            copy_kernel,
            name='results',
            out_shape=tuple(jax.ShapeDtypeStruct(x.shape, x.dtype) for x in (dq, dk, dv)),
            in_specs=[hbm] * 3,
            out_specs=(hbm,) * 3,
            scratch_shapes=[vmem(x.shape, x.dtype) for x in (dq, dk, dv)] + [dma((3 * PIECES,)), dma((3 * PIECES,))],
            cost_estimate=pl.CostEstimate(flops=0, bytes_accessed=2 ** 22, transcendentals=0),
        )(dq, dk, dv)
        return dq.reshape(query.shape), dk, dv

    return jax.shard_map(local_backward, mesh=mesh, in_specs=(q_spec, q_spec, q_spec, lse_spec, kv_spec, kv_spec, P()),
                         out_specs=(q_spec, kv_spec, kv_spec), check_vma=False)
```

```python
import functools
import math

import jax
import jax.numpy as jnp
from jax import lax
from jax.experimental import pallas as pl
from jax.experimental.pallas import tpu as pltpu
from jax.sharding import PartitionSpec as P

MESH = pl.DeviceIdType.MESH
CORES = 2
LANES = 128
SPLIT = 64
PIECES = 2
RUNS = 2
UNROLL = 2
EARLY_ITEMS = 26
ORDER = (
    'e1', 'W6', 'e2', 'e3', 'W6', 'e4', 'W4', 'O', 'W8', 'e5', 'e6', 'W4', 'E0', 'R60', 'E1', 'R61', 'R50', 'E2',
    'R51', 'R40', 'R41', 'W10', 'E3', 'W8', 'R30', 'R31', 'R20', 'R21', 'E4', 'E5', 'R10', 'R11', 'W4', 'R00', 'R01',
    'W2', 'E6', 'T60', 'T61', 'T50', 'T51', 'T40', 'T41', 'T30', 'T31', 'T20', 'T21', 'T10', 'T11', 'F', 'T00', 'T01',
)
F32 = jnp.float32
BF16 = jnp.bfloat16


def ring_kernel(cp_size, sub_start, scale, k_in, v_in, q_in, o_in, do_in, lse_in, doc_in, dq_out, dk_out, dv_out,
                kvb, acc, rsb, raw_q, raw_do, raw_o, lse, docs, qn, qt, don, dot, lines, key_doc, dqa, dqr, dko, dvo, pbuf, dsbuf, raw_kv,
                ag_send, ag_recv, rs_send, rs_recv, x_send, x_recv, loc_sem, out_sem):
    n_chip = cp_size // CORES
    n_hop = n_chip - 1
    n_sub, local_len, n_kv, group, head_dim = q_in.shape
    rows = local_len * group
    width = CORES * rows
    key_tile = k_in.shape[0] // 2
    span = local_len * CORES
    sub_len = local_len * cp_size
    keys_local = 2 * key_tile
    own = 2 * n_hop

    me = lax.axis_index('cp')
    chip, core = me // CORES, lax.rem(me, CORES)
    right = lax.rem(me + CORES, cp_size)
    left = lax.rem(me + cp_size - CORES, cp_size)
    sibling = me + 1 - 2 * core
    nbr = (right, left)

    barrier = pltpu.get_barrier_semaphore()
    for peer in (right, left, sibling):
        pl.semaphore_signal(barrier, inc=1, device_id={'cp': peer}, device_id_type=MESH)

    own_kv = [pltpu.make_async_copy(x, raw_kv.at[i], loc_sem.at[5 + i]) for i, x in enumerate((k_in, v_in))]
    local = [pltpu.make_async_copy(a, b, loc_sem.at[i]) for i, (a, b) in enumerate((
        (doc_in, docs), (lse_in, lse), (do_in, raw_do.at[0]), (o_in, raw_o), (q_in, raw_q.at[0])))]
    for c in own_kv + local:
        c.start()

    @pl.loop(0, n_sub)
    def _(s):
        for h in range(n_kv):
            dqa[h, s] = jnp.zeros(dqa.shape[2:], F32)

    for c in own_kv:
        c.wait()

    def split(h):
        @pl.loop(0, key_tile // SPLIT)
        def _(i):
            r = pl.multiple_of(i * SPLIT, SPLIT)
            for half in range(2):
                for part in range(2):
                    x = raw_kv[part, pl.ds(half * key_tile + r, SPLIT)].astype(F32)
                    kvb[own + half, h, pl.ds(r, SPLIT), part * head_dim:(part + 1) * head_dim] = x[:, h].astype(BF16)

    split(0)
    pl.semaphore_wait(barrier, 3)

    def remote(src, dst, send, recv, peer):
        return pltpu.make_async_remote_copy(src_ref=src, dst_ref=dst, send_sem=send, recv_sem=recv,
                                            device_id={'cp': peer}, device_id_type=MESH)

    def gather(way, k, head, src=None):
        i = way * n_hop + k
        return remote(kvb.at[i, head] if src is None else src, kvb.at[i, head], ag_send.at[0], ag_recv.at[k, head], nbr[way])

    def gather_own(head):
        for j in range(2):
            for way in range(2):
                gather(way, j, head, kvb.at[own + (j + way) % 2, head]).start()

    def pass_on(k, head):
        two = kvb.at[pl.ds(0, 2), head]
        remote(two, two, ag_send.at[0], ag_recv.at[k, head], right).wait_recv()
        for way in range(2):
            i = way * n_hop + k

            @pl.when(k + 2 < n_hop)
            def _():
                gather(way, k + 2, head, kvb.at[i, head]).start()

    gather_own(0)
    for h in range(1, n_kv):
        split(h)
    share = [remote(q_in, raw_q.at[1], x_send.at[0], x_recv.at[0], sibling),
             remote(do_in, raw_do.at[1], x_send.at[1], x_recv.at[1], sibling)]
    for c in share:
        c.start()

    def mine(which):
        return lines.at[:, :, :, pl.ds(which * rows, rows)]

    share_lines = remote(mine(0), mine(1), x_send.at[2], x_recv.at[2], sibling)

    @pl.loop(0, acc.shape[0])
    def _(i):
        for h in range(n_kv):
            acc[i, h] = jnp.zeros(acc.shape[2:], F32)

    pbuf[...] = jnp.zeros(pbuf.shape, BF16)
    dsbuf[...] = jnp.zeros(dsbuf.shape, BF16)
    local[0].wait()
    tiles = keys_local // LANES

    @pl.loop(0, n_chip)
    def _(b):
        for r in range(tiles):
            row = docs[pl.ds((b * CORES + core) * tiles + r, 1), :]
            key_doc[b, r * LANES:(r + 1) * LANES, :] = jnp.broadcast_to(row, (LANES, LANES)).T

    lane = lax.broadcasted_iota(jnp.int32, (8, rows), 1)
    sub = lax.broadcasted_iota(jnp.int32, (8, rows), 0)
    for c in local[1:4]:
        c.wait()

    side = math.gcd(n_sub, 4)

    @pl.loop(0, n_sub // side)
    def _(t):
        for u in range(side):
            s = t * side + u
            rep = jnp.concatenate([lse[s]] * (LANES // local_len), axis=1)
            wide = jnp.take_along_axis(rep, lane // group, axis=1)
            for h in range(n_kv):
                line = jnp.sum(jnp.where(sub - group * h == lane % group, wide, 0.0), axis=0, keepdims=True) * math.log2(math.e)
                prod = raw_do[0, s, :, h].reshape(rows, head_dim).astype(F32) * raw_o[s, :, h].reshape(rows, head_dim).astype(F32)
                total = jnp.broadcast_to(jnp.sum(prod, axis=1, keepdims=True), (rows, LANES)).T
                first = sub_start + s * sub_len + me * local_len
                doc_row = jnp.broadcast_to(docs[pl.ds(first // LANES, 1), :], (8, LANES))
                doc = jnp.take_along_axis(doc_row, lax.rem(first, LANES) + lane // group, axis=1).astype(F32)
                lines[h, s, :, :rows] = jnp.where(sub == 0, line, jnp.where(sub == 1, total[:8, :], doc))

    share_lines.start()

    def spread(c):
        @pl.loop(0, n_sub // RUNS)
        def _(t):
            for u in range(RUNS):
                s = t * RUNS + u
                for h in range(n_kv):
                    for raw, nat, tr in ((raw_q, qn, qt), (raw_do, don, dot)):
                        x = raw[c, s, :, h].reshape(rows, head_dim)
                        nat[h, s, c * rows:(c + 1) * rows, :] = x
                        tr[h, s, :, c * rows:(c + 1) * rows] = x.T

    for c in local[4:]:
        c.wait()
    spread(0)
    pass_on(0, 0)
    for c in share:
        c.wait()
    spread(1)
    share_lines.wait()

    n_run = n_sub // RUNS
    n_early = 2 + min(8, 2 * n_hop)
    n_first = n_early + 2 * n_hop
    n_block = 2 * n_hop + 2
    n_entry = n_first + (n_kv - 1) * n_block

    def place(e):
        first, early = e < n_first, e < n_early
        past = jnp.maximum(e - n_first, 0)
        head = jnp.where(first, 0, 1 + lax.div(past, n_block))
        b = lax.rem(past, n_block)
        mine = jnp.where(first, e, b) < 2
        f = jnp.maximum(jnp.where(early, e - 2, jnp.where(first, e - n_early, b - 2)), 0)
        step = lax.div(f, 2)
        way = f - 2 * step
        k = jnp.where(early, step, n_hop - 1 - step)
        half = jnp.where(mine, jnp.where(first, e, b), lax.rem(k + way, 2))
        slot = jnp.where(mine, own + half, way * n_hop + k)
        hop = lax.div(k, 2) + 1
        key_chip = jnp.where(mine, chip, lax.rem(chip + jnp.where(way == 1, hop, n_chip - hop), n_chip))
        pos0 = (key_chip * CORES + core) * keys_local + half * key_tile
        s_lo = jnp.minimum(lax.div(jnp.maximum(pos0 - sub_start - span * chip - span + sub_len, 0), sub_len * RUNS), n_run - 1)
        return slot, head, key_chip, half, s_lo

    taken, until, n_taken = [], [], jnp.int32(0)
    total = jnp.int32(0)
    for e in range(n_entry):
        n = n_run - place(jnp.int32(e))[4]
        if e < n_early:
            fits = jnp.int32(1) if e < 2 else (total + n <= EARLY_ITEMS).astype(jnp.int32) * taken[-1]
            taken.append(fits)
            n_taken = n_taken + fits
            n = n * fits
        elif e < n_first:
            f = e - n_early
            i_early = 2 + 2 * (n_hop - 1 - f // 2) + f % 2
            if i_early < n_early:
                n = n * (1 - taken[i_early])
        total = total + n
        until.append(total)

    def following(at):
        i, e, j, n = at
        over = j + 1 >= n
        e1 = e + 1
        e1 = jnp.where(e1 == n_taken, n_early, e1)
        f = e1 - n_early
        back = n_hop - 1 - lax.div(jnp.maximum(f, 0), 2)
        odd = lax.rem(jnp.maximum(f, 0), 2)
        inside = (f >= 0) & (f < 2 * n_hop)
        gone = inside & (2 + 2 * back + odd < n_taken)
        both = (odd == 1) | (3 + 2 * back < n_taken)
        e1 = jnp.where(gone, jnp.where(both, n_first, e1 + 1), e1)
        e1 = jnp.minimum(e1, n_entry - 1)
        e, j = jnp.where(over, e1, e), jnp.where(over, 0, j + 1)
        slot, head, key_chip, half, s_lo = place(e)
        i = i + 1
        return (slot, head, (s_lo + j) * RUNS, key_chip, half, (i < total).astype(jnp.int32)), (i, e, j, n_run - s_lo)

    exp_scale = scale * math.log2(math.e)
    k_iota = lax.broadcasted_iota(jnp.int32, (key_tile, width), 0)
    col = lax.broadcasted_iota(jnp.int32, (1, width), 1)
    q_off = sub_start + jnp.where(col < rows, me, sibling) * local_len + lax.rem(col, rows) // group

    def one(now, carry):
        (slot_p, head_p, s_p), (slot, head, s, key_chip, half, live), at = carry
        then, at = following(at)
        k, v = kvb[slot, head, :, :head_dim], kvb[slot, head, :, head_dim:]
        s_t = [jnp.dot(k, qt[head, s + r], preferred_element_type=F32) for r in range(RUNS)]
        dp_t = [jnp.dot(v, dot[head, s + r], preferred_element_type=F32) for r in range(RUNS)]
        p_p, ds_p = pbuf[1 - now], dsbuf[1 - now]
        q_p = qn[head_p, pl.ds(s_p, RUNS)].reshape(RUNS * width, head_dim)
        do_p = don[head_p, pl.ds(s_p, RUNS)].reshape(RUNS * width, head_dim)
        acc[slot_p, head_p, :, head_dim:] += jnp.dot(p_p, do_p, preferred_element_type=F32)
        acc[slot_p, head_p, :, :head_dim] += jnp.dot(ds_p, q_p, preferred_element_type=F32)
        k_t = kvb[slot_p, head_p, :, :head_dim].T
        for r in range(RUNS):
            dqa[head_p, s_p + r] += jnp.dot(k_t, ds_p[:, r * width:(r + 1) * width], preferred_element_type=F32)
        docs_k = key_doc[key_chip, pl.ds(pl.multiple_of(half * key_tile, 8), key_tile), :]
        docs_k = jnp.concatenate([docs_k] * (width // LANES), axis=1)
        pos0 = (key_chip * CORES + core) * keys_local + half * key_tile
        for r in range(RUNS):
            lse_r, delta_r, doc_r = [lines[head, s + r, m:m + 1, :] for m in range(3)]
            last = jnp.where(live == 1, q_off + (s + r) * sub_len - pos0, -1)
            ok = (docs_k == doc_r.astype(jnp.int32)) & (k_iota <= last)
            p = jnp.where(ok, jnp.exp2(s_t[r] * exp_scale - lse_r), 0.0)
            pbuf[now, :, r * width:(r + 1) * width] = p.astype(BF16)
            dsbuf[now, :, r * width:(r + 1) * width] = (p * (dp_t[r] - delta_r)).astype(BF16)
        return (slot, head, s), then, at

    def advance(state, target):
        i, carry = state
        m = jnp.maximum(target - i, 0) // UNROLL

        def step(_, carry):
            for u in range(UNROLL):
                carry = one(u % 2, carry)
            return carry

        return i + m * UNROLL, lax.fori_loop(0, m, step, carry)

    def add(dst, src, head):
        cut = key_tile // 4

        @pl.loop(0, 4)
        def _(i):
            r = pl.ds(pl.multiple_of(i * cut, 8), cut)
            acc[dst, head, r, :] += rsb[src, head, r, :]

    def partial(way, k, head, peer):
        i = way * n_hop + k
        sem = rs_recv.at[jnp.where(k < 2, way * n_hop + k, k), head]
        return remote(acc.at[i, head], rsb.at[i, head], rs_send.at[0], sem, peer)

    half_rows = lambda which: dqa.at[:, :, :, pl.ds(which * rows, rows)]
    swap = remote(half_rows(1), dqr, x_send.at[3], x_recv.at[3], sibling)

    GATHER, SUMS, WORK, OWN, ALL = 0, 1, 2, 3, 63
    steps, arrived = [], [1, 0]
    for word in ORDER:
        kind, digits = word[0], word[1:]
        head = 1 if kind in 'ET' else 0
        if arrived[0] < n_hop:
            bound = min(2 * arrived[0] + 1, n_early - 1)
        else:
            bound = n_entry - 1 if arrived[1] == n_hop else n_first + 1
        k = way = items = 0
        if kind in 'eE':
            what, k = GATHER, int(digits)
            arrived[head] = k + 1
        elif kind in 'RT':
            what, k, way = SUMS, int(digits[0]), int(digits[1])
            bound = (n_first + 2 if head else n_early) + 2 * (n_hop - 1 - k) + way
        elif kind == 'O':
            what = OWN
        else:
            what, items = WORK, ALL if kind == 'F' else int(digits)
        steps.append(what + 4 * (k + 16 * (way + 2 * (head + 2 * (items + 64 * bound)))))
    def pick(table, t):
        out = jnp.int32(0)
        for j, x in enumerate(table):
            out = out + jnp.where(t == j, x, 0)
        return out

    def carry_out(t, state):
        number = pick(steps, t)
        what, number = lax.rem(number, 4), lax.div(number, 4)
        k, number = lax.rem(number, 16), lax.div(number, 16)
        way, number = lax.rem(number, 2), lax.div(number, 2)
        head, number = lax.rem(number, 2), lax.div(number, 2)
        items, bound = lax.rem(number, 64), lax.div(number, 64)
        last = pick(until, bound)
        some = jnp.where(items == ALL, last + UNROLL, jnp.minimum(state[0] + items, last))
        state = advance(state, jnp.where(what == SUMS, last + UNROLL, jnp.where(what == WORK, some, state[0])))

        @pl.when(what == GATHER)
        def _():
            pass_on(k, head)

        @pl.when(what == OWN)
        def _():
            gather_own(1)

        @pl.when(items == ALL)
        def _():
            swap.start()

        @pl.when(what == SUMS)
        def _():
            i = way * n_hop + k
            peer = jnp.where(way == 0, left, right)

            @pl.when((k + 2 < n_hop) & (way == 0))
            def _():
                two = pl.ds(0, 2)
                remote(acc.at[two, head], rsb.at[two, head], rs_send.at[0], rs_recv.at[k + 2, head], peer).wait_recv()

            @pl.when(k + 2 < n_hop)
            def _():
                add(i, i + 2, head)

            partial(way, k, head, peer).start()
        return state

    def settle(head, half):
        near, far = half * n_hop, (1 - half) * n_hop + 1
        partial(1 - half, 1, head, nbr[half]).wait_recv()
        add(own + half, far, head)
        partial(half, 0, head, nbr[1 - half]).wait_recv()
        r = slice(half * key_tile, (half + 1) * key_tile)
        dko[r, head, :] = (acc[own + half, head, :, :head_dim] + rsb[near, head, :, :head_dim]) * scale
        dvo[r, head, :] = acc[own + half, head, :, head_dim:] + rsb[near, head, :, head_dim:]

    zero = jnp.int32(0)
    start, at = following((zero - 1, zero, zero - 1, zero + 1))
    lax.fori_loop(0, len(steps), carry_out, (zero, (start[:3], start, at)))
    swap.wait_recv()

    @pl.loop(0, n_sub)
    def _(s):
        for h in range(n_kv):
            x = ((dqa[h, s, :, :rows] + dqr[h, s]) * scale).astype(BF16).T
            raw_q[0, s, :, h] = x.reshape(local_len, group, head_dim)

    puts = [pltpu.make_async_copy(raw_q.at[0], dq_out, out_sem.at[0])]
    puts[0].start()
    for head in range(n_kv - 1):
        for half in range(2):
            settle(head, half)
    for half in range(2):
        settle(n_kv - 1, half)
        r = pl.ds(half * key_tile, key_tile)
        for i, (a, b) in enumerate(((dko, dk_out), (dvo, dv_out))):
            c = pltpu.make_async_copy(a.at[r], b.at[r], out_sem.at[1 + 2 * half + i])
            c.start()
            puts.append(c)
    swap.wait_send()
    moved = pl.ds(0, 2 * n_hop)
    remote(kvb.at[moved], kvb.at[moved], ag_send.at[0], ag_recv.at[0, 0], right).wait_send()
    remote(acc.at[moved], rsb.at[moved], rs_send.at[0], rs_recv.at[0, 0], right).wait_send()
    for c in puts:
        c.wait()


def copy_kernel(a, b, c, a_out, b_out, c_out, a_buf, b_buf, c_buf, in_sem, out_sem):
    moves = []
    for src, buf, dst in ((a, a_buf, a_out), (b, b_buf, b_out), (c, c_buf, c_out)):
        piece = src.shape[0] // PIECES
        for i in range(PIECES):
            r, n = pl.ds(i * piece, piece), len(moves)
            moves.append((pltpu.make_async_copy(src.at[r], buf.at[r], in_sem.at[n]),
                          pltpu.make_async_copy(buf.at[r], dst.at[r], out_sem.at[n])))
    for x, _ in moves:
        x.start()
    for x, y in moves:
        x.wait()
        y.start()
    for _, y in moves:
        y.wait()


def solution(mesh):
    cp_size = mesh.shape['cp']
    q_spec = P(None, 'cp', 'tp', None)
    lse_spec = P(None, 'cp', 'tp')
    kv_spec = P('cp', 'tp', None)

    def local_backward(query, out_act, out_grad, row_lse, key_act, value_act, doc_ids):
        n_sub, local_len, n_heads, head_dim = query.shape
        keys_local, n_kv = key_act.shape[0], key_act.shape[1]
        group = n_heads // n_kv
        sub_start = keys_local * cp_size - n_sub * local_len * cp_size
        rows = local_len * group
        half = keys_local // 2
        n_chip = cp_size // CORES
        n_hop = n_chip - 1
        n_slot = 2 * n_hop + 2
        q5 = (n_sub, local_len, n_kv, group, head_dim)
        scale = head_dim ** -0.5
        flops = 2 * 5 * n_kv * n_sub * 2 * rows * head_dim * keys_local * n_hop
        hbm = pl.BlockSpec(memory_space=pl.ANY)
        dma = pltpu.SemaphoreType.DMA
        vmem = pltpu.VMEM
        dq, dk, dv = pl.pallas_call(
            functools.partial(ring_kernel, cp_size, sub_start, scale),
            name='ring_backward',
            out_shape=(jax.ShapeDtypeStruct(q5, BF16),) + (jax.ShapeDtypeStruct(key_act.shape, F32),) * 2,
            in_specs=[hbm] * 7,
            out_specs=(hbm,) * 3,
            scratch_shapes=[
                vmem((n_slot, n_kv, half, 2 * head_dim), BF16),
                vmem((n_slot, n_kv, half, 2 * head_dim), F32),
                vmem((2 * n_hop, n_kv, half, 2 * head_dim), F32),
                vmem((CORES,) + q5, BF16),
                vmem((CORES,) + q5, BF16),
                vmem(q5, BF16),
                vmem((n_sub, n_heads, local_len), F32),
                vmem((doc_ids.shape[0] // LANES, LANES), jnp.int32),
                vmem((n_kv, n_sub, CORES * rows, head_dim), BF16),
                vmem((n_kv, n_sub, head_dim, CORES * rows), BF16),
                vmem((n_kv, n_sub, CORES * rows, head_dim), BF16),
                vmem((n_kv, n_sub, head_dim, CORES * rows), BF16),
                vmem((n_kv, n_sub, 8, CORES * rows), F32),
                vmem((n_chip, keys_local, LANES), jnp.int32),
                vmem((n_kv, n_sub, head_dim, CORES * rows), F32),
                vmem((n_kv, n_sub, head_dim, rows), F32),
                vmem(key_act.shape, F32),
                vmem(key_act.shape, F32),
                vmem((2, half, RUNS * CORES * rows), BF16),
                vmem((2, half, RUNS * CORES * rows), BF16),
                vmem((2,) + key_act.shape, BF16),
                dma((1,)), dma((n_hop, n_kv)), dma((1,)), dma((n_hop + 2, n_kv)),
                dma((4,)), dma((4,)), dma((7,)), dma((5,)),
            ],
            compiler_params=pltpu.CompilerParams(collective_id=0, has_side_effects=True, vmem_limit_bytes=62 * 1024 * 1024),
            cost_estimate=pl.CostEstimate(flops=flops, bytes_accessed=30 * 2 ** 20, transcendentals=0),
        )(key_act, value_act, query.reshape(q5), out_act.reshape(q5), out_grad.reshape(q5), jnp.swapaxes(row_lse, 1, 2), doc_ids.reshape(-1, LANES))
        dq, dk, dv = pl.pallas_call(
            copy_kernel,
            name='results',
            out_shape=tuple(jax.ShapeDtypeStruct(x.shape, x.dtype) for x in (dq, dk, dv)),
            in_specs=[hbm] * 3,
            out_specs=(hbm,) * 3,
            scratch_shapes=[vmem(x.shape, x.dtype) for x in (dq, dk, dv)] + [dma((3 * PIECES,)), dma((3 * PIECES,))],
            cost_estimate=pl.CostEstimate(flops=0, bytes_accessed=2 ** 22, transcendentals=0),
        )(dq, dk, dv)
        return dq.reshape(query.shape), dk, dv

    return jax.shard_map(local_backward, mesh=mesh, in_specs=(q_spec, q_spec, q_spec, lse_spec, kv_spec, kv_spec, P()),
                         out_specs=(q_spec, kv_spec, kv_spec), check_vma=False)
```
